32 devices in a mesh: group: 2 (over y), temp: 4 (over x, core), gz: 4 (over z).
Axes of the slice: x: 2, y: 2, z: 4, core: 2. Of those that a mesh axis runs over, the one named last changes fastest.
Arguments:
- spin_state: float32 [16, 3, 16, 128, 128], P(('group', 'temp'), None, 'gz'), parts along dimension 0, may hold values from -1 to 1, as said below
- couplings: float32 [3, 32, 128, 128], P(None, ('group', 'gz')), parts along dimension 1, may hold values from -12 to 12
- inverse_temps: float32 [16], P(('group', 'temp')), parts along dimension 0, may hold values from 0.3 to 3
- colour_order: int32 [16], P(('group', 'temp')), parts along dimension 0, may hold values 0 or 1
- heat_level: float32 [16, 16, 128, 128], P(('group', 'temp'), 'gz'), parts along dimension 0, may hold values from 0.001 to 0.999
- heat_height: float32 [16, 16, 128, 128], P(('group', 'temp'), 'gz'), parts along dimension 0, may hold values from -1 to 1
- heat_angle: float32 [16, 16, 128, 128], P(('group', 'temp'), 'gz'), parts along dimension 0, may hold values from -3.140625 to 3.140625
- swap_bits: int32 [16], P(('group', 'temp')), parts along dimension 0, may hold values 0 or 1
Outputs:
- spin_final: float32 [16, 3, 16, 128, 128], P(('group', 'temp'), None, 'gz'), parts along dimension 0
- energies: float32 [16], P(('group', 'temp')), parts along dimension 0
The draws below stay inside these ranges and needn't reach their ends.
There are 2 independent parts, one for each index of `group`. The reference program is written for one: setup_inputs(seed, part) draws one part's arguments, and reference() takes and returns one part's arrays. A program takes and returns all parts, laid end to end along the dimension named above; each array names one. Nothing has to cross between parts.
Inputs may be any that keep to these rules, and one draw needn't show every extreme that they name: `spin_state`: every site's three components form a vector of unit length.
All inputs are finite; a program needn't handle non-finite values. No bound on the sum of `colour_order` or of `swap_bits` on one device may be relied on, other than what follows from the above.
Results may differ from the reference program's by a relative error of at most 0.0003.
Values sent between devices are 32-bit elements; how exact they have to be, the bound alone decides.
A program may use at most 64 MiB of HBM per device.

```python
import math
import jax
import jax.numpy as jnp
from jax import lax

LX = 128
LY = 128
OR_SWEEPS = 2
REPLICAS = 8
NZ = 16


def draw_spin_state(key, part):
    first_key, second_key = jax.random.split(jax.random.fold_in(key, 11))
    array_shape = (REPLICAS, NZ, LY, LX)
    height = jax.random.uniform(first_key, array_shape, jnp.float32, -1.0, 1.0)
    azimuth = jax.random.uniform(second_key, array_shape, jnp.float32, -math.pi, math.pi)
    side = jnp.sqrt(jnp.maximum(1.0 - height * height, 0.0))
    return jnp.stack([side * jnp.cos(azimuth), side * jnp.sin(azimuth), height], axis=1)


def draw_couplings(key, part):
    first_key = jax.random.fold_in(key, 23)
    array_shape = (3, NZ, LY, LX)
    position = jnp.arange(NZ, dtype=jnp.float32) / max(NZ - 1, 1)
    values = jnp.clip(jax.random.normal(first_key, array_shape, jnp.float32), -4.0, 4.0)
    factor = 1.0 + 2.0 * position
    return values * factor[None, :, None, None]


def place_ends(array, rng, smallest, largest):
    longest = array.shape.index(max(array.shape))
    spots = []
    for shift in (0, 1):
        where = [jax.random.randint(jax.random.fold_in(rng, axis), (), 0, length) for axis, length in enumerate(array.shape)]
        where[longest] = (where[longest] + shift) % array.shape[longest]
        spots.append(tuple(where))
    return array.at[spots[0]].set(smallest).at[spots[1]].set(largest)


def steps_of(rng, dims, shards, low, largest):
    level = 1.0
    for dim, blocks in shards:
        draws = jax.random.uniform(jax.random.fold_in(jax.random.fold_in(rng, 6), dim), (blocks,), jnp.float32, low / len(shards), largest / len(shards))
        level = level * jnp.repeat(jnp.exp(draws), dims[dim] // blocks).reshape((-1,) + (1,) * (len(dims) - 1 - dim))
    return level


def setup_inputs(seed: int = 0, part: int = 0) -> dict:
    streams_of = jax.random.split(jax.random.key(seed), 9)
    part_splits = jax.random.split(jax.random.fold_in(streams_of[8], part), 9)
    return {
        "spin_state": draw_spin_state(jax.random.fold_in(jax.random.fold_in(streams_of[8], part), 71), part),
        "couplings": draw_couplings(jax.random.fold_in(jax.random.fold_in(streams_of[8], part), 71), part),
        "inverse_temps": jnp.clip(jnp.exp(math.log(3.0) - 2.3025851 * jax.random.uniform(part_splits[2], (REPLICAS,), jnp.float32) ** steps_of(part_splits[2], (REPLICAS,), ((0, 4),), -0.2, 0.2)), 0.3, 3.0),
        "colour_order": place_ends((jax.random.randint(part_splits[3], (REPLICAS,), 0, 2) < 1).astype(jnp.int32), jax.random.fold_in(part_splits[3], 1), 0, 1),
        "heat_level": jnp.clip(0.001 + 0.998 * jax.random.uniform(part_splits[4], (REPLICAS, NZ, LY, LX), jnp.float32) ** steps_of(part_splits[4], (REPLICAS, NZ, LY, LX), ((0, 4), (1, 4)), -0.2, 0.2), 0.001, 0.999),
        "heat_height": jnp.clip(jax.random.uniform(part_splits[5], (REPLICAS, NZ, LY, LX), jnp.float32, -1.0, 1.0) * steps_of(part_splits[5], (REPLICAS, NZ, LY, LX), ((0, 4), (1, 4)), -0.4, 0.0), -1.0, 1.0),
        "heat_angle": jnp.clip(jax.random.uniform(part_splits[6], (REPLICAS, NZ, LY, LX), jnp.float32, -3.140625, 3.140625), -3.140625, 3.140625),
        "swap_bits": place_ends((jax.random.randint(part_splits[7], (REPLICAS,), 0, 4) < 3).astype(jnp.int32), jax.random.fold_in(part_splits[7], 1), 0, 1),
    }


def neighbour_sum(current, bonds):
    east_bond, north_bond, upper_bond = (bonds[0], bonds[1], bonds[2])
    summed = east_bond * jnp.roll(current, -1, 3) + jnp.roll(east_bond, 1, 2) * jnp.roll(current, 1, 3)
    summed = summed + north_bond * jnp.roll(current, -1, 2) + jnp.roll(north_bond, 1, 1) * jnp.roll(current, 1, 2)
    summed = summed + upper_bond * jnp.roll(current, -1, 1) + jnp.roll(upper_bond, 1, 0) * jnp.roll(current, 1, 1)
    return summed

def reflect(current, pulled, component_axis):
    projection = lax.optimization_barrier(jnp.sum(current * pulled, axis=component_axis, keepdims=True))
    square = lax.optimization_barrier(jnp.sum(pulled * pulled, axis=component_axis, keepdims=True))
    return 2.0 * projection / jnp.maximum(square, 0.01) * pulled - current

def heat_bath(pulled, beta_value, uniform_level, cosine_draw, angle_draw, component_axis):
    square = lax.optimization_barrier(jnp.sum(pulled * pulled, axis=component_axis, keepdims=True))
    strength = jnp.sqrt(jnp.maximum(square, 0.01))
    unit_axis = pulled / strength
    reach = beta_value * strength
    cosine = 1.0 + jnp.log1p(uniform_level * jnp.expm1(-2.0 * reach)) / reach
    side = jnp.sqrt(jnp.maximum(1.0 - cosine_draw * cosine_draw, 0.0))
    proposal = jnp.concatenate([side * jnp.cos(angle_draw), side * jnp.sin(angle_draw), cosine_draw], axis=component_axis)
    along_axis = lax.optimization_barrier(jnp.sum(proposal * unit_axis, axis=component_axis, keepdims=True))
    tangent = proposal - along_axis * unit_axis
    tangent = tangent / jnp.sqrt(jnp.maximum(lax.optimization_barrier(jnp.sum(tangent * tangent, axis=component_axis, keepdims=True)), 0.0001))
    return cosine * unit_axis + jnp.sqrt(jnp.maximum(1.0 - cosine * cosine, 0.0)) * tangent

def pair_swap(stacked, decisions):
    flipped = stacked[:, ::-1]
    taking = (decisions != 0).reshape((-1,) + (1,) * (stacked.ndim - 1))
    return jnp.where(taking, flipped, stacked)

def reference(spin_state, couplings, inverse_temps, colour_order, heat_level, heat_height, heat_angle, swap_bits):
    plane_index = jnp.arange(NZ, dtype=jnp.int32)
    row_index = jnp.arange(LY, dtype=jnp.int32)
    column_index = jnp.arange(LX, dtype=jnp.int32)
    site_sum = plane_index[:, None, None] + row_index[None, :, None] + column_index[None, None, :]

    def one_replica(packed):
        current, beta_value, start_colour, uniform_level, cosine_draw, angle_draw = packed
        parity = (site_sum + start_colour) % 2
        colours = ((parity == 0)[None], (parity == 1)[None])
        for sweep_index in range(OR_SWEEPS):
            for chosen in colours:
                pulled = neighbour_sum(current, couplings)
                current = jnp.where(chosen, reflect(current, pulled, 0), current)
        for chosen in colours:
            pulled = neighbour_sum(current, couplings)
            renewed = heat_bath(pulled, beta_value, uniform_level[None], cosine_draw[None], angle_draw[None], 0)
            current = jnp.where(chosen, renewed, current)
        bond_sum = couplings[0] * jnp.roll(current, -1, 3) + couplings[1] * jnp.roll(current, -1, 2) + couplings[2] * jnp.roll(current, -1, 1)
        energy = -jnp.sum(current * bond_sum) / (LX * LY * NZ)
        return (current, energy)
    swept, energy_all = lax.map(one_replica, (spin_state, inverse_temps, colour_order, heat_level, heat_height, heat_angle))
    count = REPLICAS
    tail_shape = swept.shape[1:]
    swept = pair_swap(swept.reshape((count // 2, 2) + tail_shape), swap_bits[0::2]).reshape(swept.shape)
    energy_all = pair_swap(energy_all.reshape((count // 2, 2)), swap_bits[0::2]).reshape((count,))
    middle = pair_swap(swept[1:count - 1].reshape(((count - 2) // 2, 2) + tail_shape), swap_bits[1:count - 1:2])
    swept = jnp.concatenate([swept[:1], middle.reshape((count - 2,) + tail_shape), swept[count - 1:]], axis=0)
    middle_energy = pair_swap(energy_all[1:count - 1].reshape(((count - 2) // 2, 2)), swap_bits[1:count - 1:2])
    energy_all = jnp.concatenate([energy_all[:1], middle_energy.reshape((count - 2,)), energy_all[count - 1:]], axis=0)
    return (swept, energy_all)
```

```python
import functools
import math

import jax
import jax.numpy as jnp
from jax import lax
from jax.experimental import pallas as pl
from jax.experimental.pallas import tpu as pltpu
from jax.sharding import PartitionSpec as P

OR_SWEEPS = 2
HALVES = 2 * OR_SWEEPS + 2
PAD = 8
MESH = pl.DeviceIdType.MESH
SIN_TERMS = [(-1.0) ** i / math.factorial(2 * i + 1) for i in range(8)]
COS_TERMS = [(-1.0) ** i / math.factorial(2 * i) for i in range(9)]


def horner(terms, value):
    total = jnp.full_like(value, terms[-1])
    for term in terms[-2::-1]:
        total = total * value + term
    return total


def cos_sin(angle):
    half = 0.5 * angle
    square = half * half
    sine = half * horner(SIN_TERMS, square)
    cosine = horner(COS_TERMS, square)
    return 1.0 - 2.0 * sine * sine, 2.0 * sine * cosine


def dot3(a, b):
    return a[0] * b[0] + a[1] * b[1] + a[2] * b[2]


def reflect(current, pulled):
    factor = 2.0 * dot3(current, pulled) / jnp.maximum(dot3(pulled, pulled), 0.01)
    return [factor * p - s for p, s in zip(pulled, current)]


def heat_bath(pulled, beta, level, trial):
    strength = jnp.sqrt(jnp.maximum(dot3(pulled, pulled), 0.01))
    inverse = 1.0 / strength
    axis = [p * inverse for p in pulled]
    reach = beta * strength
    shrink = -jnp.tanh(reach) * (jnp.exp(-2.0 * reach) + 1.0)
    cosine = 1.0 + jnp.log1p(level * shrink) / reach
    along = dot3(trial, axis)
    tangent = [t - along * a for t, a in zip(trial, axis)]
    scale = jnp.sqrt(jnp.maximum(1.0 - cosine * cosine, 0.0)) * (
        1.0 / jnp.sqrt(jnp.maximum(dot3(tangent, tangent), 0.0001))
    )
    return [cosine * a + scale * t for a, t in zip(axis, tangent)]


def flag(bits_ref, j, size, width):
    return jnp.full((size, width), bits_ref[j], jnp.int32) != 0


def sweep_kernel(
    dims,
    spin_hbm,
    coup_hbm,
    beta_ref,
    order_ref,
    level_hbm,
    height_hbm,
    angle_hbm,
    bits_ref,
    evened,
    rbuf,
    trecv,
    ebuf,
    spin_in,
    coup_in,
    level_in,
    height_in,
    angle_in,
    lifted,
    sp,
    xo,
    xr,
    yi,
    yo,
    zu,
    zd,
    lv,
    ut,
    eacc,
    tsend,
    in_sem,
    hsend,
    hrecv,
    esend,
    erecv,
    tssem,
    trsem,
    xsend,
    xrecv,
    wrap_sem,
):
    count, planes, rows, width, n, m = dims
    k = rows // 2
    chunk = 32 if k % 32 == 0 else 8
    last = planes - 1
    g = lax.axis_index("gz")
    t = lax.axis_index("temp")
    up, down = lax.rem(g + 1, n), lax.rem(g + n - 1, n)
    has_below, has_above = t > 0, t < m - 1
    near = 2 < n <= 2 * HALVES - 2

    loads = [
        pltpu.make_async_copy(src, dst, in_sem.at[i])
        for i, (src, dst) in enumerate(
            (
                (spin_hbm.at[:, :, pl.ds(0, 1)], spin_in.at[:, :, pl.ds(0, 1)]),
                (spin_hbm.at[:, :, pl.ds(last, 1)], spin_in.at[:, :, pl.ds(last, 1)]),
                (coup_hbm.at[2, last], coup_in.at[2, last]),
                (coup_hbm.at[pl.ds(0, 2)], coup_in.at[pl.ds(0, 2)]),
                (coup_hbm.at[2, pl.ds(0, last)], coup_in.at[2, pl.ds(0, last)]),
                (
                    spin_hbm.at[:, :, pl.ds(1, planes - 2)],
                    spin_in.at[:, :, pl.ds(1, planes - 2)],
                ),
                (level_hbm, level_in),
                (height_hbm, height_in),
                (angle_hbm, angle_in),
            )
        )
    ]

    def peer(dt, there):
        return {"gz": there} if dt == 0 else {"temp": t + dt, "gz": there}

    def along(dt, action):
        if dt == 0:
            action()
        else:
            pl.when(has_below if dt < 0 else has_above)(action)

    barrier = pltpu.get_barrier_semaphore()

    def greet(dt, there):
        pl.semaphore_signal(barrier, inc=1, device_id=peer(dt, there), device_id_type=MESH)

    sides = has_below.astype(jnp.int32) + has_above.astype(jnp.int32)
    if near:

        @pl.when(g < n - 1)
        def _():
            greet(0, up)

        greet(0, down)
        along(-1, lambda: greet(-1, g))
        along(1, lambda: greet(1, g))
        expected = sides + jnp.where(g == 0, 1, 2)
    else:
        for dt in (-1, 0, 1):

            def greet_all(dt=dt):
                for d in range(1 if dt == 0 else 0, n):
                    greet(dt, lax.rem(g + d, n))

            along(dt, greet_all)
        expected = n - 1 + n * sides

    for load in loads:
        load.start()

    def parity(r, z, size):
        lane = lax.broadcasted_iota(jnp.int32, (size, width), 1)
        return ((lane + (g * planes + z + order_ref[r])) & 1) != 0

    def halves(ref, index, start, size):
        even = ref[index + (pl.ds(2 * start, size, stride=2), slice(None))]
        odd = ref[index + (pl.ds(2 * start + 1, size, stride=2), slice(None))]
        return even, odd

    def put_spin(c, r, d, z, start, value):
        size = value.shape[0]
        sp[c, r, d, z + 1, pl.ds(PAD + start, size), :] = value
        if start == 0:
            sp[c, r, d, z + 1, pl.ds(PAD + k, 1), :] = value[0:1]
        if start + size == k:
            sp[c, r, d, z + 1, pl.ds(PAD - 1, 1), :] = value[size - 1 : size]

    def pack_spin(r, z):
        e = parity(r, z, k)
        for d in range(3):
            even, odd = halves(spin_in, (r, d, z), 0, k)
            put_spin(0, r, d, z, 0, jnp.where(e, odd, even))
            put_spin(1, r, d, z, 0, jnp.where(e, even, odd))

    def halo(x, r, side):
        c = 1 - x % 2
        plain = sp.at[c, r, :, 1, pl.ds(PAD, k), :]
        return pltpu.make_async_remote_copy(
            src_ref=plain if side == 0 else lifted.at[c, r],
            dst_ref=sp.at[c, r, :, planes + 1 if side == 0 else 0, pl.ds(PAD, k), :],
            send_sem=hsend.at[x, r, side],
            recv_sem=hrecv.at[x, r, side],
            device_id={"gz": down if side == 0 else up},
            device_id_type=MESH,
        )

    def lift(c, r, d, start, value):
        part = pl.ds(start, value.shape[0])
        lifted[c, r, d, part, :] = zu[c, r, last, part, :] * value

    def inner(r, action):
        if planes > 2:
            lax.fori_loop(1, last, lambda z, carry: (action(r, z), carry)[1], 0)

    for load in loads[:3]:
        load.wait()
    for r in range(count):
        e = parity(r, last, k)
        even, odd = halves(coup_in, (2, last), 0, k)
        zu[0, r, last] = jnp.where(e, odd, even)
        zu[1, r, last] = jnp.where(e, even, odd)
        pack_spin(r, last)
        for d in range(3):
            lift(1, r, d, 0, sp[1, r, d, planes, pl.ds(PAD, k), :])
        pack_spin(r, 0)

    def slot_order(r):
        other = order_ref[r ^ 1]
        return jnp.where(bits_ref[r - r % 2] != 0, other, order_ref[r])

    def wide(value):
        return jnp.full((1, width), value, jnp.int32).astype(jnp.float32)

    tsend[0, 0:1] = wide(slot_order(count - 1))
    tsend[0, 1:2] = wide(bits_ref[count - 1])
    tsend[0, 2:3] = wide(bits_ref[count - 2])
    tsend[1, 0:1] = wide(slot_order(0))
    tsend[1, 1:2] = wide(0)
    tsend[1, 2:3] = wide(bits_ref[0])
    for r in range(count):
        trecv[2, r : r + 1] = wide(slot_order(r))
        trecv[2, count + r : count + r + 1] = wide(bits_ref[r])

    pl.semaphore_wait(barrier, expected)
    if near:

        @pl.when(g == n - 1)
        def _():
            pl.semaphore_signal(wrap_sem, inc=1, device_id={"gz": up}, device_id_type=MESH)

    for r in range(count):
        halo(0, r, 1).start()
        if r == 0 and near:

            @pl.when(g == 0)
            def _():
                pl.semaphore_wait(wrap_sem, 1)

        halo(0, r, 0).start()

    def tell(side):
        return pltpu.make_async_remote_copy(
            src_ref=tsend.at[side],
            dst_ref=trecv.at[side],
            send_sem=tssem.at[side],
            recv_sem=trsem.at[side],
            device_id={"temp": t + 1 if side == 0 else t - 1},
            device_id_type=MESH,
        )

    along(1, lambda: tell(0).start())
    along(-1, lambda: tell(1).start())

    for load in loads[3:6]:
        load.wait()

    def pack_bonds(i, carry):
        r, z = i // planes, i % planes
        e = parity(r, z, k)
        even, odd = halves(coup_in, (0, z), 0, k)
        first, second = jnp.where(e, odd, even), jnp.where(e, even, odd)
        xo[0, r, z] = first
        xo[1, r, z] = second
        xr[0, r, z] = pltpu.roll(second, 1, 1)
        xr[1, r, z] = pltpu.roll(first, 1, 1)
        even, odd = halves(coup_in, (1, z), 0, k)
        before = pltpu.roll(odd, 1, 0)
        yi[r, z] = even
        yo[0, r, z] = jnp.where(e, odd, before)
        yo[1, r, z] = jnp.where(e, before, odd)
        return carry

    def pack_lower(i, carry):
        r, z = i // last, 1 + i % last
        e = parity(r, z, k)
        even, odd = halves(coup_in, (2, z - 1), 0, k)
        zd[0, r, z] = jnp.where(e, odd, even)
        zd[1, r, z] = jnp.where(e, even, odd)
        zu[0, r, z - 1] = jnp.where(e, even, odd)
        zu[1, r, z - 1] = jnp.where(e, odd, even)
        return carry

    for r in range(count):
        inner(r, pack_spin)
    lax.fori_loop(0, count * planes, pack_bonds, 0)
    lax.fori_loop(0, count * last, pack_lower, 0)
    for r in range(count):
        for c in (0, 1):
            zd[c, r, 0] = jnp.ones((k, width), jnp.float32)

    def pull(c, r, z, start):
        o = 1 - c
        part = pl.ds(start, chunk)
        e = parity(r, z, chunk)
        bx, br, by = xo[c, r, z, part, :], xr[c, r, z, part, :], yi[r, z, part, :]
        bo, bu, bd = yo[c, r, z, part, :], zu[c, r, z, part, :], zd[c, r, z, part, :]
        pulled = []
        for d in range(3):
            mid = sp[o, r, d, z + 1, pl.ds(PAD + start, chunk), :]
            nxt = sp[o, r, d, z + 1, pl.ds(PAD + start + 1, chunk), :]
            prv = sp[o, r, d, z + 1, pl.ds(PAD + start - 1, chunk), :]
            outer = jnp.where(e, nxt, prv) if c == 0 else jnp.where(e, prv, nxt)
            total = bx * pltpu.roll(mid, width - 1, 1) + br * pltpu.roll(mid, 1, 1)
            total = total + by * mid + bo * outer
            total = total + bu * sp[o, r, d, z + 2, pl.ds(PAD + start, chunk), :]
            total = total + bd * sp[o, r, d, z, pl.ds(PAD + start, chunk), :]
            pulled.append(total)
        return pulled

    def relax(c, r, z, lifting=False):
        for start in range(0, k, chunk):
            pulled = pull(c, r, z, start)
            current = [sp[c, r, d, z + 1, pl.ds(PAD + start, chunk), :] for d in range(3)]
            for d, value in enumerate(reflect(current, pulled)):
                put_spin(c, r, d, z, start, value)
                if lifting:
                    lift(c, r, d, start, value)

    def heat(c, r, z, lifting=False):
        for start in range(0, k, chunk):
            part = pl.ds(start, chunk)
            pulled = pull(c, r, z, start)
            trial = [ut[c, r, d, z, part, :] for d in range(3)]
            renewed = heat_bath(pulled, beta_ref[r], lv[c, r, z, part, :], trial)
            for d, value in enumerate(renewed):
                put_spin(c, r, d, z, start, value)
                if lifting:
                    lift(c, r, d, start, value)
            if c == 1:
                terms = dot3(renewed, pulled)
                eacc[r] = eacc[r] + sum(terms[j : j + 8] for j in range(0, chunk, 8))

    def pack_heat(r, z):
        for start in range(0, k, chunk):
            part = pl.ds(start, chunk)
            e = parity(r, z, chunk)
            even, odd = halves(level_in, (r, z), start, chunk)
            lv[0, r, z, part, :] = jnp.where(e, odd, even)
            lv[1, r, z, part, :] = jnp.where(e, even, odd)
            angles = halves(angle_in, (r, z), start, chunk)
            heights = halves(height_in, (r, z), start, chunk)
            trials = []
            for angle, height in zip(angles, heights):
                side = jnp.sqrt(jnp.maximum(1.0 - height * height, 0.0))
                cosine, sine = cos_sin(angle)
                trials.append((side * cosine, side * sine, height))
            for d in range(3):
                ut[0, r, d, z, part, :] = jnp.where(e, trials[1][d], trials[0][d])
                ut[1, r, d, z, part, :] = jnp.where(e, trials[0][d], trials[1][d])

    def take_halo(x, r, side):
        halo(x, r, 1 - side).wait_recv()
        if x >= 1:
            halo(x - 1, r, side).wait_send()

    eacc[...] = jnp.zeros_like(eacc)
    relaxing = 2 * OR_SWEEPS
    for x in range(HALVES - 1):
        c = x % 2
        work = functools.partial(relax if x < relaxing else heat, c)
        for r in range(count):
            for side, z in ((0, 0), (1, last)):
                take_halo(x, r, side)
                work(r, z, lifting=side == 1)
                halo(x + 1, r, side).start()
            inner(r, work)
            if x == 0 and r == 0:
                for load in loads[6:]:
                    load.wait()
            for z in range(planes):
                if z % relaxing == x:
                    pack_heat(r, z)

    def settle(c, z):
        for r in range(0, count, 2):
            taking = flag(bits_ref, r, k, width)
            for d in range(3):
                low = sp[c, r, d, z + 1, pl.ds(PAD, k), :]
                top = sp[c, r + 1, d, z + 1, pl.ds(PAD, k), :]
                evened[r, c, z, d] = jnp.where(taking, top, low)
                evened[r + 1, c, z, d] = jnp.where(taking, low, top)

    def ship(c, z, side):
        return pltpu.make_async_remote_copy(
            src_ref=evened.at[count - 1 if side == 0 else 0, c, z],
            dst_ref=rbuf.at[side, c, z],
            send_sem=xsend.at[c, z, side],
            recv_sem=xrecv.at[c, z, side],
            device_id={"temp": t + 1 if side == 0 else t - 1},
            device_id_type=MESH,
        )

    def send_off(c, z):
        settle(c, z)
        along(1, lambda: ship(c, z, 0).start())
        along(-1, lambda: ship(c, z, 1).start())

    x = HALVES - 1
    work = functools.partial(heat, 1)
    for z in range(planes):
        send_off(0, z)
    for r in range(count):
        inner(r, work)
    for z in range(1, last):
        send_off(1, z)
    for r in range(count):
        for side, z in ((0, 0), (1, last)):
            take_halo(x, r, side)
            work(r, z)
            if r == count - 1:
                send_off(1, z)
    for r in range(count):
        ebuf[1, g, r : r + 1] = jnp.sum(eacc[r], axis=0, keepdims=True)

    def received(c, z):
        along(1, lambda: ship(c, z, 1).wait_recv())
        along(-1, lambda: ship(c, z, 0).wait_recv())

    for z in range(planes):
        received(0, z)
    along(1, lambda: tell(1).wait_recv())
    along(-1, lambda: tell(0).wait_recv())

    def share(dt, source, there):
        return pltpu.make_async_remote_copy(
            src_ref=ebuf.at[1, source],
            dst_ref=ebuf.at[1 - dt, source],
            send_sem=esend.at[1 - dt, there],
            recv_sem=erecv.at[1 - dt, source],
            device_id=peer(dt, there),
            device_id_type=MESH,
        )

    def spread(dt, action):
        def all_of():
            for d in range(1 if dt == 0 else 0, n):
                action(lax.rem(g + d, n))

        along(dt, all_of)

    for dt in (0, 1, -1):
        spread(dt, lambda there, dt=dt: share(dt, g, there).start())
    for z in range(1, last):
        received(1, z)
    for r in range(count):
        for side in (0, 1):
            halo(x, r, side).wait_send()
    along(1, lambda: tell(0).wait_send())
    along(-1, lambda: tell(1).wait_send())
    for z in range(planes):
        for c in (0, 1):
            along(1, lambda: ship(c, z, 0).wait_send())
            along(-1, lambda: ship(c, z, 1).wait_send())
    for z in (0, last):
        received(1, z)
    for dt in (0, 1, -1):
        spread(dt, lambda there, dt=dt: share(dt, g, there).wait_send())
    for dt in (0, 1, -1):
        spread(-dt, lambda there, dt=dt: share(dt, there, there).wait_recv())


def finish_kernel(
    dims,
    evened,
    rbuf,
    trecv,
    ebuf,
    out_hbm,
    eout_ref,
    stage,
    out_sem,
):
    count, planes, rows, width, n, m = dims
    k = rows // 2
    g = lax.axis_index("gz")
    t = lax.axis_index("temp")
    below, above = (t > 0).astype(jnp.int32), (t < m - 1).astype(jnp.int32)

    def number(side, row):
        return trecv[side, row : row + 1]

    def own_order(r):
        return number(2, r)

    def own_bit(r):
        return number(2, count + r)

    def mask(value, size):
        return jnp.broadcast_to(value, (size, width)) > 0.5

    def plan(r):
        if r == 0:
            met = jnp.full((1, width), below, jnp.int32) != 0
            return rbuf.at[0], jnp.where(met, number(0, 1), 0.0), jnp.where(met, number(0, 0), 0.0)
        if r == count - 1:
            met = jnp.full((1, width), above, jnp.int32) != 0
            return rbuf.at[1], jnp.where(met, own_bit(r), 0.0), jnp.where(met, number(1, 0), 0.0)
        other = r + 1 if r % 2 else r - 1
        return evened.at[other], own_bit(min(r, other)), own_order(other)

    lane = lax.broadcasted_iota(jnp.int32, (k, width), 1)
    plans = [plan(r) for r in range(count)]
    orders = [
        jnp.where(take > 0.5, order, own_order(r)).astype(jnp.int32)
        for r, (_, take, order) in enumerate(plans)
    ]
    copies = []
    for z in range(planes):
        for r in range(count):
            other, take, _ = plans[r]
            taking = mask(take, k)
            e = ((lane + (jnp.broadcast_to(orders[r], (k, width)) + (g * planes + z))) & 1) != 0
            for d in range(3):
                first, second = [
                    jnp.where(taking, other[c, z, d], evened[r, c, z, d]) for c in (0, 1)
                ]
                stage[r, d, z, pl.ds(0, k, stride=2), :] = jnp.where(e, second, first)
                stage[r, d, z, pl.ds(1, k, stride=2), :] = jnp.where(e, first, second)
            copy = pltpu.make_async_copy(
                stage.at[r, :, z], out_hbm.at[r, :, z], out_sem.at[r, z]
            )
            copy.start()
            copies.append(copy)

    sites = float(width * rows * planes * n)

    def total(slot, r):
        summed = ebuf[slot, 0, r : r + 1]
        for j in range(1, n):
            summed = summed + ebuf[slot, j, r : r + 1]
        return jnp.broadcast_to(jnp.sum(-summed, axis=1, keepdims=True) / sites, (1, width))

    energy = []
    for r in range(0, count, 2):
        taking = own_bit(r) > 0.5
        low, top = total(1, r), total(1, r + 1)
        energy += [jnp.where(taking, top, low), jnp.where(taking, low, top)]
    for r in range(count):
        other, take, _ = plans[r]
        if r == 0:
            swapped = number(0, 2) > 0.5
            partner = jnp.where(swapped, total(0, count - 2), total(0, count - 1))
        elif r == count - 1:
            swapped = number(1, 2) > 0.5
            partner = jnp.where(swapped, total(2, 1), total(2, 0))
        else:
            partner = energy[r + 1 if r % 2 else r - 1]
        eout_ref[r] = jnp.max(jnp.where(take > 0.5, partner, energy[r]))
    for copy in copies:
        copy.wait()


def on_device(n, m, spin, coup, beta, order, level, height, angle, bits):
    count, _, planes, rows, width = spin.shape
    k = rows // 2
    f32 = jnp.float32
    hbm = pl.BlockSpec(memory_space=pltpu.HBM)
    smem = pl.BlockSpec(memory_space=pltpu.SMEM)
    vmem = pl.BlockSpec(memory_space=pltpu.VMEM)
    dma = pltpu.SemaphoreType.DMA
    bonds = pltpu.VMEM((2, count, planes, k, width), f32)
    dims = (count, planes, rows, width, n, m)
    handed = pl.pallas_call(
        functools.partial(sweep_kernel, dims),
        out_shape=(
            pltpu.VMEM((count, 2, planes, 3, k, width), f32),
            pltpu.VMEM((2, 2, planes, 3, k, width), f32),
            pltpu.VMEM((3, max(8, 2 * count), width), f32),
            pltpu.VMEM((3, n, count, width), f32),
        ),
        in_specs=[hbm, hbm, smem, smem, hbm, hbm, hbm, smem],
        out_specs=(vmem,) * 4,
        scratch_shapes=[
            pltpu.VMEM(spin.shape, f32),
            pltpu.VMEM(coup.shape, f32),
            pltpu.VMEM(level.shape, f32),
            pltpu.VMEM(level.shape, f32),
            pltpu.VMEM(level.shape, f32),
            pltpu.VMEM((2, count, 3, k, width), f32),
            pltpu.VMEM((2, count, 3, planes + 2, k + 2 * PAD, width), f32),
            bonds,
            bonds,
            pltpu.VMEM((count, planes, k, width), f32),
            bonds,
            bonds,
            bonds,
            bonds,
            pltpu.VMEM((2, count, 3, planes, k, width), f32),
            pltpu.VMEM((count, 8, width), f32),
            pltpu.VMEM((2, max(8, 2 * count), width), f32),
            dma((9,)),
            dma((HALVES, count, 2)),
            dma((HALVES, count, 2)),
            dma((3, n)),
            dma((3, n)),
            dma((2,)),
            dma((2,)),
            dma((2, planes, 2)),
            dma((2, planes, 2)),
            pltpu.SemaphoreType.REGULAR,
        ],
        compiler_params=pltpu.CompilerParams(
            collective_id=0, has_side_effects=True, vmem_limit_bytes=58 * 1024 * 1024
        ),
    )(spin, coup, beta, order, level, height, angle, bits)
    return pl.pallas_call(
        functools.partial(finish_kernel, dims),
        out_shape=(
            jax.ShapeDtypeStruct(spin.shape, f32),
            jax.ShapeDtypeStruct((count,), f32),
        ),
        in_specs=[vmem] * 4,
        out_specs=(hbm, smem),
        scratch_shapes=[pltpu.VMEM(spin.shape, f32), dma((count, planes))],
        compiler_params=pltpu.CompilerParams(vmem_limit_bytes=16 * 1024 * 1024),
    )(*handed)


def solution(mesh):
    n, m = mesh.shape["gz"], mesh.shape["temp"]
    return jax.shard_map(
        functools.partial(on_device, n, m),
        mesh=mesh,
        in_specs=(
            P(("group", "temp"), None, "gz", None, None),
            P(None, ("group", "gz"), None, None),
            P(("group", "temp")),
            P(("group", "temp")),
            P(("group", "temp"), "gz", None, None),
            P(("group", "temp"), "gz", None, None),
            P(("group", "temp"), "gz", None, None),
            P(("group", "temp")),
        ),
        out_specs=(P(("group", "temp"), None, "gz", None, None), P(("group", "temp"))),
        check_vma=False,
    )
```

```python
import functools
import math

import jax
import jax.numpy as jnp
from jax import lax
from jax.experimental import pallas as pl
from jax.experimental.pallas import tpu as pltpu
from jax.sharding import PartitionSpec as P

OR_SWEEPS = 2
HALVES = 2 * OR_SWEEPS + 2
PAD = 8
MESH = pl.DeviceIdType.MESH
SIN_TERMS = [(-1.0) ** i / math.factorial(2 * i + 1) for i in range(8)]
COS_TERMS = [(-1.0) ** i / math.factorial(2 * i) for i in range(9)]


def horner(terms, value):
    total = jnp.full_like(value, terms[-1])
    for term in terms[-2::-1]:
        total = total * value + term
    return total


def cos_sin(angle):
    half = 0.5 * angle
    square = half * half
    sine = half * horner(SIN_TERMS, square)
    cosine = horner(COS_TERMS, square)
    return 1.0 - 2.0 * sine * sine, 2.0 * sine * cosine


def dot3(a, b):
    return a[0] * b[0] + a[1] * b[1] + a[2] * b[2]


def reflect(current, pulled):
    factor = 2.0 * dot3(current, pulled) / jnp.maximum(dot3(pulled, pulled), 0.01)
    return [factor * p - s for p, s in zip(pulled, current)]


def heat_bath(pulled, beta, level, trial):
    strength = jnp.sqrt(jnp.maximum(dot3(pulled, pulled), 0.01))
    inverse = 1.0 / strength
    axis = [p * inverse for p in pulled]
    reach = beta * strength
    shrink = -jnp.tanh(reach) * (jnp.exp(-2.0 * reach) + 1.0)
    cosine = 1.0 + jnp.log1p(level * shrink) / reach
    along = dot3(trial, axis)
    tangent = [t - along * a for t, a in zip(trial, axis)]
    scale = jnp.sqrt(jnp.maximum(1.0 - cosine * cosine, 0.0)) * (
        1.0 / jnp.sqrt(jnp.maximum(dot3(tangent, tangent), 0.0001))
    )
    return [cosine * a + scale * t for a, t in zip(axis, tangent)]


def flag(bits_ref, j, size, width):
    return jnp.full((size, width), bits_ref[j], jnp.int32) != 0


def sweep_kernel(
    dims,
    spin_hbm,
    coup_hbm,
    beta_hbm,
    order_hbm,
    level_hbm,
    height_hbm,
    angle_hbm,
    bits_hbm,
    evened,
    rbuf,
    trecv,
    ebuf,
    spin_in,
    coup_in,
    level_in,
    height_in,
    angle_in,
    lifted,
    sp,
    xo,
    xr,
    yi,
    yo,
    zu,
    zd,
    lv,
    ut,
    eacc,
    tsend,
    beta_ref,
    order_ref,
    bits_ref,
    in_sem,
    hsend,
    hrecv,
    esend,
    erecv,
    tssem,
    trsem,
    xsend,
    xrecv,
    wrap_sem,
):
    count, planes, rows, width, n, m = dims
    k = rows // 2
    chunk = 32 if k % 32 == 0 else 8
    last = planes - 1
    g = lax.axis_index("gz")
    t = lax.axis_index("temp")
    up, down = lax.rem(g + 1, n), lax.rem(g + n - 1, n)
    has_below, has_above = t > 0, t < m - 1
    near = 2 < n <= 2 * HALVES - 2

    loads = [
        pltpu.make_async_copy(src, dst, in_sem.at[i])
        for i, (src, dst) in enumerate(
            (
                (spin_hbm.at[:, :, pl.ds(0, 1)], spin_in.at[:, :, pl.ds(0, 1)]),
                (spin_hbm.at[:, :, pl.ds(last, 1)], spin_in.at[:, :, pl.ds(last, 1)]),
                (coup_hbm.at[2, last], coup_in.at[2, last]),
                (coup_hbm.at[pl.ds(0, 2)], coup_in.at[pl.ds(0, 2)]),
                (coup_hbm.at[2, pl.ds(0, last)], coup_in.at[2, pl.ds(0, last)]),
                (
                    spin_hbm.at[:, :, pl.ds(1, planes - 2)],
                    spin_in.at[:, :, pl.ds(1, planes - 2)],
                ),
                (level_hbm, level_in),
                (height_hbm, height_in),
                (angle_hbm, angle_in),
                (order_hbm, order_ref),
                (bits_hbm, bits_ref),
                (beta_hbm, beta_ref),
            )
        )
    ]

    def peer(dt, there):
        return {"gz": there} if dt == 0 else {"temp": t + dt, "gz": there}

    def along(dt, action):
        if dt == 0:
            action()
        else:
            pl.when(has_below if dt < 0 else has_above)(action)

    scalars = loads[9:]
    for load in loads[:3] + scalars:
        load.start()

    barrier = pltpu.get_barrier_semaphore()

    def greet(dt, there):
        pl.semaphore_signal(barrier, inc=1, device_id=peer(dt, there), device_id_type=MESH)

    sides = has_below.astype(jnp.int32) + has_above.astype(jnp.int32)
    if near:

        @pl.when(g < n - 1)
        def _():
            greet(0, up)

        greet(0, down)
        along(-1, lambda: greet(-1, g))
        along(1, lambda: greet(1, g))
        expected = sides + jnp.where(g == 0, 1, 2)
    else:
        for dt in (-1, 0, 1):

            def greet_all(dt=dt):
                for d in range(1 if dt == 0 else 0, n):
                    greet(dt, lax.rem(g + d, n))

            along(dt, greet_all)
        expected = n - 1 + n * sides

    def parity(r, z, size):
        lane = lax.broadcasted_iota(jnp.int32, (size, width), 1)
        return ((lane + (g * planes + z + order_ref[r])) & 1) != 0

    def halves(ref, index, start, size):
        even = ref[index + (pl.ds(2 * start, size, stride=2), slice(None))]
        odd = ref[index + (pl.ds(2 * start + 1, size, stride=2), slice(None))]
        return even, odd

    def put_spin(c, r, d, z, start, value):
        size = value.shape[0]
        sp[c, r, d, z + 1, pl.ds(PAD + start, size), :] = value
        if start == 0:
            sp[c, r, d, z + 1, pl.ds(PAD + k, 1), :] = value[0:1]
        if start + size == k:
            sp[c, r, d, z + 1, pl.ds(PAD - 1, 1), :] = value[size - 1 : size]

    def pack_spin(r, z):
        e = parity(r, z, k)
        for d in range(3):
            even, odd = halves(spin_in, (r, d, z), 0, k)
            put_spin(0, r, d, z, 0, jnp.where(e, odd, even))
            put_spin(1, r, d, z, 0, jnp.where(e, even, odd))

    middle = k // chunk // 2 * chunk

    def parts(x, r):
        split = x == HALVES - 1 and r == count - 1 and middle > 0
        return [(0, middle), (middle, k)] if split else [(0, k)]

    def halo(x, r, side, part=0):
        c = 1 - x % 2
        start, stop = parts(x, r)[part]
        size = stop - start
        plain = sp.at[c, r, :, 1, pl.ds(PAD + start, size), :]
        above = planes + 1 if side == 0 else 0
        return pltpu.make_async_remote_copy(
            src_ref=plain if side == 0 else lifted.at[c, r, :, pl.ds(start, size), :],
            dst_ref=sp.at[c, r, :, above, pl.ds(PAD + start, size), :],
            send_sem=hsend.at[x + part, r, side],
            recv_sem=hrecv.at[x + part, r, side],
            device_id={"gz": down if side == 0 else up},
            device_id_type=MESH,
        )

    def lift(c, r, d, start, value):
        part = pl.ds(start, value.shape[0])
        lifted[c, r, d, part, :] = zu[c, r, last, part, :] * value

    def inner(r, action):
        if planes > 2:
            lax.fori_loop(1, last, lambda z, carry: (action(r, z), carry)[1], 0)

    def ready():
        pl.semaphore_wait(barrier, expected)

    if near:

        @pl.when(g == n - 1)
        def _():
            ready()
            pl.semaphore_signal(wrap_sem, inc=1, device_id={"gz": up}, device_id_type=MESH)

    for load in loads[:3] + scalars:
        load.wait()
    for load in loads[3:9]:
        load.start()

    def pack_edges(r):
        e = parity(r, last, k)
        even, odd = halves(coup_in, (2, last), 0, k)
        zu[0, r, last] = jnp.where(e, odd, even)
        zu[1, r, last] = jnp.where(e, even, odd)
        pack_spin(r, last)
        for d in range(3):
            lift(1, r, d, 0, sp[1, r, d, planes, pl.ds(PAD, k), :])
        pack_spin(r, 0)

    def slot_order(r):
        other = order_ref[r ^ 1]
        return jnp.where(bits_ref[r - r % 2] != 0, other, order_ref[r])

    def wide(value):
        return jnp.full((1, width), value, jnp.int32).astype(jnp.float32)

    for r in range(count):
        pack_edges(r)
        if r == 0:
            if near:
                pl.when(g < n - 1)(ready)
            else:
                ready()
        halo(0, r, 1).start()
        if r == 0 and near:

            @pl.when(g == 0)
            def _():
                pl.semaphore_wait(wrap_sem, 1)

        halo(0, r, 0).start()

    tsend[0, 0:1] = wide(slot_order(count - 1))
    tsend[0, 1:2] = wide(bits_ref[count - 1])
    tsend[0, 2:3] = wide(bits_ref[count - 2])
    tsend[1, 0:1] = wide(slot_order(0))
    tsend[1, 1:2] = wide(0)
    tsend[1, 2:3] = wide(bits_ref[0])
    for r in range(count):
        trecv[2, r : r + 1] = wide(slot_order(r))
        trecv[2, count + r : count + r + 1] = wide(bits_ref[r])

    def tell(side):
        return pltpu.make_async_remote_copy(
            src_ref=tsend.at[side],
            dst_ref=trecv.at[side],
            send_sem=tssem.at[side],
            recv_sem=trsem.at[side],
            device_id={"temp": t + 1 if side == 0 else t - 1},
            device_id_type=MESH,
        )

    along(1, lambda: tell(0).start())
    along(-1, lambda: tell(1).start())

    for load in loads[3:6]:
        load.wait()

    def pack_bonds(i, carry):
        r, z = i // planes, i % planes
        e = parity(r, z, k)
        even, odd = halves(coup_in, (0, z), 0, k)
        first, second = jnp.where(e, odd, even), jnp.where(e, even, odd)
        xo[0, r, z] = first
        xo[1, r, z] = second
        xr[0, r, z] = pltpu.roll(second, 1, 1)
        xr[1, r, z] = pltpu.roll(first, 1, 1)
        even, odd = halves(coup_in, (1, z), 0, k)
        before = pltpu.roll(odd, 1, 0)
        yi[r, z] = even
        yo[0, r, z] = jnp.where(e, odd, before)
        yo[1, r, z] = jnp.where(e, before, odd)
        return carry

    def pack_lower(i, carry):
        r, z = i // last, 1 + i % last
        e = parity(r, z, k)
        even, odd = halves(coup_in, (2, z - 1), 0, k)
        zd[0, r, z] = jnp.where(e, odd, even)
        zd[1, r, z] = jnp.where(e, even, odd)
        zu[0, r, z - 1] = jnp.where(e, even, odd)
        zu[1, r, z - 1] = jnp.where(e, odd, even)
        return carry

    for r in range(count):
        inner(r, pack_spin)
    lax.fori_loop(0, count * planes, pack_bonds, 0)
    lax.fori_loop(0, count * last, pack_lower, 0)
    for r in range(count):
        for c in (0, 1):
            zd[c, r, 0] = jnp.ones((k, width), jnp.float32)

    def pull(c, r, z, start):
        o = 1 - c
        part = pl.ds(start, chunk)
        e = parity(r, z, chunk)
        bx, br, by = xo[c, r, z, part, :], xr[c, r, z, part, :], yi[r, z, part, :]
        bo, bu, bd = yo[c, r, z, part, :], zu[c, r, z, part, :], zd[c, r, z, part, :]
        pulled = []
        for d in range(3):
            mid = sp[o, r, d, z + 1, pl.ds(PAD + start, chunk), :]
            nxt = sp[o, r, d, z + 1, pl.ds(PAD + start + 1, chunk), :]
            prv = sp[o, r, d, z + 1, pl.ds(PAD + start - 1, chunk), :]
            outer = jnp.where(e, nxt, prv) if c == 0 else jnp.where(e, prv, nxt)
            total = bx * pltpu.roll(mid, width - 1, 1) + br * pltpu.roll(mid, 1, 1)
            total = total + by * mid + bo * outer
            total = total + bu * sp[o, r, d, z + 2, pl.ds(PAD + start, chunk), :]
            total = total + bd * sp[o, r, d, z, pl.ds(PAD + start, chunk), :]
            pulled.append(total)
        return pulled

    def relax(c, r, z, lifting=False):
        for start in range(0, k, chunk):
            pulled = pull(c, r, z, start)
            current = [sp[c, r, d, z + 1, pl.ds(PAD + start, chunk), :] for d in range(3)]
            for d, value in enumerate(reflect(current, pulled)):
                put_spin(c, r, d, z, start, value)
                if lifting:
                    lift(c, r, d, start, value)

    def heat(c, r, z, lifting=False, rows_of=(0, k)):
        for start in range(*rows_of, chunk):
            part = pl.ds(start, chunk)
            pulled = pull(c, r, z, start)
            trial = [ut[c, r, d, z, part, :] for d in range(3)]
            renewed = heat_bath(pulled, beta_ref[r], lv[c, r, z, part, :], trial)
            for d, value in enumerate(renewed):
                put_spin(c, r, d, z, start, value)
                if lifting:
                    lift(c, r, d, start, value)
            if c == 1:
                terms = dot3(renewed, pulled)
                eacc[r] = eacc[r] + sum(terms[j : j + 8] for j in range(0, chunk, 8))

    def pack_heat(r, z):
        for start in range(0, k, chunk):
            part = pl.ds(start, chunk)
            e = parity(r, z, chunk)
            even, odd = halves(level_in, (r, z), start, chunk)
            lv[0, r, z, part, :] = jnp.where(e, odd, even)
            lv[1, r, z, part, :] = jnp.where(e, even, odd)
            angles = halves(angle_in, (r, z), start, chunk)
            heights = halves(height_in, (r, z), start, chunk)
            trials = []
            for angle, height in zip(angles, heights):
                side = jnp.sqrt(jnp.maximum(1.0 - height * height, 0.0))
                cosine, sine = cos_sin(angle)
                trials.append((side * cosine, side * sine, height))
            for d in range(3):
                ut[0, r, d, z, part, :] = jnp.where(e, trials[1][d], trials[0][d])
                ut[1, r, d, z, part, :] = jnp.where(e, trials[0][d], trials[1][d])

    def take_halo(x, r, side):
        halo(x, r, 1 - side).wait_recv()
        if x >= 1:
            halo(x - 1, r, side).wait_send()

    eacc[...] = jnp.zeros_like(eacc)
    relaxing = 2 * OR_SWEEPS
    for x in range(HALVES - 1):
        c = x % 2
        work = functools.partial(relax if x < relaxing else heat, c)
        for r in range(count):
            for side, z in ((0, 0), (1, last)):
                take_halo(x, r, side)
                work(r, z, lifting=side == 1)
                if len(parts(x + 1, r)) == 1:
                    halo(x + 1, r, side).start()
            if len(parts(x + 1, r)) > 1:
                for part in (0, 1):
                    for side in (0, 1):
                        halo(x + 1, r, side, part).start()
            inner(r, work)
            if x == 0 and r == 0:
                for load in loads[6:9]:
                    load.wait()
            for z in range(planes):
                if z % relaxing == x:
                    pack_heat(r, z)

    def settle(c, z, start, stop):
        size = stop - start
        part, packed = pl.ds(start, size), pl.ds(PAD + start, size)
        for r in range(0, count, 2):
            taking = flag(bits_ref, r, size, width)
            for d in range(3):
                low = sp[c, r, d, z + 1, packed, :]
                top = sp[c, r + 1, d, z + 1, packed, :]
                evened[r, c, z, d, part, :] = jnp.where(taking, top, low)
                evened[r + 1, c, z, d, part, :] = jnp.where(taking, low, top)

    final = parts(HALVES - 1, count - 1)

    def pieces(c, z):
        return final if c == 1 and z in (0, last) else [(0, k)]

    def ship(c, z, side, part):
        start, stop = pieces(c, z)[part]
        rows_of = pl.ds(start, stop - start)
        return pltpu.make_async_remote_copy(
            src_ref=evened.at[count - 1 if side == 0 else 0, c, z, :, rows_of, :],
            dst_ref=rbuf.at[side, c, z, :, rows_of, :],
            send_sem=xsend.at[c, z, side, part],
            recv_sem=xrecv.at[c, z, side, part],
            device_id={"temp": t + 1 if side == 0 else t - 1},
            device_id_type=MESH,
        )

    def send_off(c, z, part=0):
        settle(c, z, *pieces(c, z)[part])
        along(1, lambda: ship(c, z, 0, part).start())
        along(-1, lambda: ship(c, z, 1, part).start())

    x = HALVES - 1
    work = functools.partial(heat, 1)
    for z in range(planes):
        send_off(0, z)
    for r in range(count):
        inner(r, work)
    for z in range(1, last):
        send_off(1, z)
    for r in range(count):
        for part, rows_of in enumerate(parts(x, r)):
            for side, z in ((0, 0), (1, last)):
                halo(x, r, 1 - side, part).wait_recv()
                if part == 0:
                    halo(x - 1, r, side).wait_send()
                work(r, z, rows_of=rows_of)
                if r == count - 1:
                    send_off(1, z, part)
    for r in range(count):
        ebuf[1, g, r : r + 1] = jnp.sum(eacc[r], axis=0, keepdims=True)

    def received(c, z):
        for part in range(len(pieces(c, z))):
            along(1, lambda: ship(c, z, 1, part).wait_recv())
            along(-1, lambda: ship(c, z, 0, part).wait_recv())

    for z in range(planes):
        received(0, z)
    along(1, lambda: tell(1).wait_recv())
    along(-1, lambda: tell(0).wait_recv())

    def share(dt, source, there):
        return pltpu.make_async_remote_copy(
            src_ref=ebuf.at[1, source],
            dst_ref=ebuf.at[1 - dt, source],
            send_sem=esend.at[1 - dt, there],
            recv_sem=erecv.at[1 - dt, source],
            device_id=peer(dt, there),
            device_id_type=MESH,
        )

    def spread(dt, action):
        def all_of():
            for d in range(1 if dt == 0 else 0, n):
                action(lax.rem(g + d, n))

        along(dt, all_of)

    for dt in (0, 1, -1):
        spread(dt, lambda there, dt=dt: share(dt, g, there).start())
    for z in range(1, last):
        received(1, z)
    for r in range(count):
        for side in (0, 1):
            for part in range(len(parts(x, r))):
                halo(x, r, side, part).wait_send()
    along(1, lambda: tell(0).wait_send())
    along(-1, lambda: tell(1).wait_send())
    for z in range(planes):
        for c in (0, 1):
            for part in range(len(pieces(c, z))):
                along(1, lambda: ship(c, z, 0, part).wait_send())
                along(-1, lambda: ship(c, z, 1, part).wait_send())
    for z in (0, last):
        received(1, z)
    for dt in (0, 1, -1):
        spread(dt, lambda there, dt=dt: share(dt, g, there).wait_send())
    for dt in (0, 1, -1):
        spread(-dt, lambda there, dt=dt: share(dt, there, there).wait_recv())


def finish_kernel(
    dims,
    evened,
    rbuf,
    trecv,
    ebuf,
    out_hbm,
    eout_hbm,
    stage,
    eout_ref,
    out_sem,
    eout_sem,
):
    count, planes, rows, width, n, m = dims
    k = rows // 2
    g = lax.axis_index("gz")
    t = lax.axis_index("temp")
    below, above = (t > 0).astype(jnp.int32), (t < m - 1).astype(jnp.int32)

    def number(side, row):
        return trecv[side, row : row + 1]

    def own_order(r):
        return number(2, r)

    def own_bit(r):
        return number(2, count + r)

    def mask(value, size):
        return jnp.broadcast_to(value, (size, width)) > 0.5

    def plan(r):
        if r == 0:
            met = jnp.full((1, width), below, jnp.int32) != 0
            return rbuf.at[0], jnp.where(met, number(0, 1), 0.0), jnp.where(met, number(0, 0), 0.0)
        if r == count - 1:
            met = jnp.full((1, width), above, jnp.int32) != 0
            return rbuf.at[1], jnp.where(met, own_bit(r), 0.0), jnp.where(met, number(1, 0), 0.0)
        other = r + 1 if r % 2 else r - 1
        return evened.at[other], own_bit(min(r, other)), own_order(other)

    lane = lax.broadcasted_iota(jnp.int32, (k, width), 1)
    plans = [plan(r) for r in range(count)]
    orders = [
        jnp.where(take > 0.5, order, own_order(r)).astype(jnp.int32)
        for r, (_, take, order) in enumerate(plans)
    ]
    sites = float(width * rows * planes * n)

    def total(slot, r):
        summed = ebuf[slot, 0, r : r + 1]
        for j in range(1, n):
            summed = summed + ebuf[slot, j, r : r + 1]
        return jnp.broadcast_to(jnp.sum(-summed, axis=1, keepdims=True) / sites, (1, width))

    energy = []
    for r in range(0, count, 2):
        taking = own_bit(r) > 0.5
        low, top = total(1, r), total(1, r + 1)
        energy += [jnp.where(taking, top, low), jnp.where(taking, low, top)]
    for r in range(count):
        other, take, _ = plans[r]
        if r == 0:
            swapped = number(0, 2) > 0.5
            partner = jnp.where(swapped, total(0, count - 2), total(0, count - 1))
        elif r == count - 1:
            swapped = number(1, 2) > 0.5
            partner = jnp.where(swapped, total(2, 1), total(2, 0))
        else:
            partner = energy[r + 1 if r % 2 else r - 1]
        eout_ref[r] = jnp.max(jnp.where(take > 0.5, partner, energy[r]))
    told = pltpu.make_async_copy(eout_ref, eout_hbm, eout_sem)
    told.start()
    copies = []
    for z in range(planes):
        for r in range(count):
            other, take, _ = plans[r]
            taking = mask(take, k)
            e = ((lane + (jnp.broadcast_to(orders[r], (k, width)) + (g * planes + z))) & 1) != 0
            for d in range(3):
                first, second = [
                    jnp.where(taking, other[c, z, d], evened[r, c, z, d]) for c in (0, 1)
                ]
                stage[r, d, z, pl.ds(0, k, stride=2), :] = jnp.where(e, second, first)
                stage[r, d, z, pl.ds(1, k, stride=2), :] = jnp.where(e, first, second)
            copy = pltpu.make_async_copy(
                stage.at[r, :, z], out_hbm.at[r, :, z], out_sem.at[r, z]
            )
            copy.start()
            copies.append(copy)
    told.wait()
    for copy in copies:
        copy.wait()


def on_device(n, m, spin, coup, beta, order, level, height, angle, bits):
    count, _, planes, rows, width = spin.shape
    k = rows // 2
    f32 = jnp.float32
    hbm = pl.BlockSpec(memory_space=pltpu.HBM)
    vmem = pl.BlockSpec(memory_space=pltpu.VMEM)
    dma = pltpu.SemaphoreType.DMA
    bonds = pltpu.VMEM((2, count, planes, k, width), f32)
    dims = (count, planes, rows, width, n, m)
    handed = pl.pallas_call(
        functools.partial(sweep_kernel, dims),
        out_shape=(
            pltpu.VMEM((count, 2, planes, 3, k, width), f32),
            pltpu.VMEM((2, 2, planes, 3, k, width), f32),
            pltpu.VMEM((3, max(8, 2 * count), width), f32),
            pltpu.VMEM((3, n, count, width), f32),
        ),
        in_specs=[hbm] * 8,
        out_specs=(vmem,) * 4,
        scratch_shapes=[
            pltpu.VMEM(spin.shape, f32),
            pltpu.VMEM(coup.shape, f32),
            pltpu.VMEM(level.shape, f32),
            pltpu.VMEM(level.shape, f32),
            pltpu.VMEM(level.shape, f32),
            pltpu.VMEM((2, count, 3, k, width), f32),
            pltpu.VMEM((2, count, 3, planes + 2, k + 2 * PAD, width), f32),
            bonds,
            bonds,
            pltpu.VMEM((count, planes, k, width), f32),
            bonds,
            bonds,
            bonds,
            bonds,
            pltpu.VMEM((2, count, 3, planes, k, width), f32),
            pltpu.VMEM((count, 8, width), f32),
            pltpu.VMEM((2, max(8, 2 * count), width), f32),
            pltpu.SMEM((count,), f32),
            pltpu.SMEM((count,), jnp.int32),
            pltpu.SMEM((count,), jnp.int32),
            dma((12,)),
            dma((HALVES + 1, count, 2)),
            dma((HALVES + 1, count, 2)),
            dma((3, n)),
            dma((3, n)),
            dma((2,)),
            dma((2,)),
            dma((2, planes, 2, 2)),
            dma((2, planes, 2, 2)),
            pltpu.SemaphoreType.REGULAR,
        ],
        compiler_params=pltpu.CompilerParams(
            collective_id=0, has_side_effects=True, vmem_limit_bytes=58 * 1024 * 1024
        ),
    )(spin, coup, beta, order, level, height, angle, bits)
    return pl.pallas_call(
        functools.partial(finish_kernel, dims),
        out_shape=(
            jax.ShapeDtypeStruct(spin.shape, f32),
            jax.ShapeDtypeStruct((count,), f32),
        ),
        in_specs=[vmem] * 4,
        out_specs=(hbm, hbm),
        scratch_shapes=[
            pltpu.VMEM(spin.shape, f32),
            pltpu.SMEM((count,), f32),
            dma((count, planes)),
            dma(()),
        ],
        compiler_params=pltpu.CompilerParams(vmem_limit_bytes=16 * 1024 * 1024),
    )(*handed)


def solution(mesh):
    n, m = mesh.shape["gz"], mesh.shape["temp"]
    return jax.shard_map(
        functools.partial(on_device, n, m),
        mesh=mesh,
        in_specs=(
            P(("group", "temp"), None, "gz", None, None),
            P(None, ("group", "gz"), None, None),
            P(("group", "temp")),
            P(("group", "temp")),
            P(("group", "temp"), "gz", None, None),
            P(("group", "temp"), "gz", None, None),
            P(("group", "temp"), "gz", None, None),
            P(("group", "temp")),
        ),
        out_specs=(P(("group", "temp"), None, "gz", None, None), P(("group", "temp"))),
        check_vma=False,
    )
```

```python
import functools
import math

import jax
import jax.numpy as jnp
from jax import lax
from jax.experimental import pallas as pl
from jax.experimental.pallas import tpu as pltpu
from jax.sharding import PartitionSpec as P

OR_SWEEPS = 2
HALVES = 2 * OR_SWEEPS + 2
PAD = 8
MESH = pl.DeviceIdType.MESH
SIN_TERMS = [(-1.0) ** i / math.factorial(2 * i + 1) for i in range(8)]
COS_TERMS = [(-1.0) ** i / math.factorial(2 * i) for i in range(9)]


def horner(terms, value):
    total = jnp.full_like(value, terms[-1])
    for term in terms[-2::-1]:
        total = total * value + term
    return total


def cos_sin(angle):
    half = 0.5 * angle
    square = half * half
    sine = half * horner(SIN_TERMS, square)
    cosine = horner(COS_TERMS, square)
    return 1.0 - 2.0 * sine * sine, 2.0 * sine * cosine


def dot3(a, b):
    return a[0] * b[0] + a[1] * b[1] + a[2] * b[2]


def reflect(current, pulled):
    factor = 2.0 * dot3(current, pulled) / jnp.maximum(dot3(pulled, pulled), 0.01)
    return [factor * p - s for p, s in zip(pulled, current)]


def heat_bath(pulled, beta, level, trial):
    strength = jnp.sqrt(jnp.maximum(dot3(pulled, pulled), 0.01))
    inverse = 1.0 / strength
    axis = [p * inverse for p in pulled]
    reach = beta * strength
    shrink = -jnp.tanh(reach) * (jnp.exp(-2.0 * reach) + 1.0)
    cosine = 1.0 + jnp.log1p(level * shrink) / reach
    along = dot3(trial, axis)
    tangent = [t - along * a for t, a in zip(trial, axis)]
    scale = jnp.sqrt(jnp.maximum(1.0 - cosine * cosine, 0.0)) * (
        1.0 / jnp.sqrt(jnp.maximum(dot3(tangent, tangent), 0.0001))
    )
    return [cosine * a + scale * t for a, t in zip(axis, tangent)]


def flag(bits_ref, j, size, width):
    return jnp.full((size, width), bits_ref[j], jnp.int32) != 0


def sweep_kernel(
    dims,
    spin_hbm,
    coup_hbm,
    beta_hbm,
    order_hbm,
    level_hbm,
    height_hbm,
    angle_hbm,
    bits_hbm,
    evened,
    rbuf,
    trecv,
    ebuf,
    spin_in,
    coup_in,
    level_in,
    height_in,
    angle_in,
    lifted,
    sp,
    xo,
    xr,
    yi,
    yo,
    zu,
    zd,
    lv,
    ut,
    eacc,
    tsend,
    beta_ref,
    order_ref,
    bits_ref,
    in_sem,
    hsend,
    hrecv,
    esend,
    erecv,
    tssem,
    trsem,
    xsend,
    xrecv,
    wrap_sem,
):
    count, planes, rows, width, n, m = dims
    k = rows // 2
    chunk = 32 if k % 32 == 0 else 8
    last = planes - 1
    g = lax.axis_index("gz")
    t = lax.axis_index("temp")
    up, down = lax.rem(g + 1, n), lax.rem(g + n - 1, n)
    has_below, has_above = t > 0, t < m - 1
    near = 2 < n <= 2 * HALVES - 2

    loads = [
        pltpu.make_async_copy(src, dst, in_sem.at[i % 6])
        for i, (src, dst) in enumerate(
            (
                (spin_hbm.at[:, :, pl.ds(0, 1)], spin_in.at[:, :, pl.ds(0, 1)]),
                (spin_hbm.at[:, :, pl.ds(last, 1)], spin_in.at[:, :, pl.ds(last, 1)]),
                (coup_hbm.at[2, last], coup_in.at[2, last]),
                (order_hbm, order_ref),
                (bits_hbm, bits_ref),
                (beta_hbm, beta_ref),
                (coup_hbm.at[pl.ds(0, 2)], coup_in.at[pl.ds(0, 2)]),
                (coup_hbm.at[2, pl.ds(0, last)], coup_in.at[2, pl.ds(0, last)]),
                (
                    spin_hbm.at[:, :, pl.ds(1, planes - 2)],
                    spin_in.at[:, :, pl.ds(1, planes - 2)],
                ),
                (level_hbm, level_in),
                (height_hbm, height_in),
                (angle_hbm, angle_in),
            )
        )
    ]

    def peer(dt, there):
        return {"gz": there} if dt == 0 else {"temp": t + dt, "gz": there}

    def along(dt, action):
        if dt == 0:
            action()
        else:
            pl.when(has_below if dt < 0 else has_above)(action)

    for load in loads[:6]:
        load.start()

    barrier = pltpu.get_barrier_semaphore()

    def greet(dt, there):
        pl.semaphore_signal(barrier, inc=1, device_id=peer(dt, there), device_id_type=MESH)

    sides = has_below.astype(jnp.int32) + has_above.astype(jnp.int32)
    if near:

        @pl.when(g < n - 1)
        def _():
            greet(0, up)

        greet(0, down)
        along(-1, lambda: greet(-1, g))
        along(1, lambda: greet(1, g))
        expected = sides + jnp.where(g == 0, 1, 2)
    else:
        for dt in (-1, 0, 1):

            def greet_all(dt=dt):
                for d in range(1 if dt == 0 else 0, n):
                    greet(dt, lax.rem(g + d, n))

            along(dt, greet_all)
        expected = n - 1 + n * sides

    def parity(r, z, size):
        lane = lax.broadcasted_iota(jnp.int32, (size, width), 1)
        return ((lane + (g * planes + z + order_ref[r])) & 1) != 0

    def halves(ref, index, start, size):
        even = ref[index + (pl.ds(2 * start, size, stride=2), slice(None))]
        odd = ref[index + (pl.ds(2 * start + 1, size, stride=2), slice(None))]
        return even, odd

    def put_spin(c, r, d, z, start, value):
        size = value.shape[0]
        sp[c, r, d, z + 1, pl.ds(PAD + start, size), :] = value
        if start == 0:
            sp[c, r, d, z + 1, pl.ds(PAD + k, 1), :] = value[0:1]
        if start + size == k:
            sp[c, r, d, z + 1, pl.ds(PAD - 1, 1), :] = value[size - 1 : size]

    def pack_spin(r, z):
        e = parity(r, z, k)
        for d in range(3):
            even, odd = halves(spin_in, (r, d, z), 0, k)
            put_spin(0, r, d, z, 0, jnp.where(e, odd, even))
            put_spin(1, r, d, z, 0, jnp.where(e, even, odd))

    middle = k // chunk // 2 * chunk

    def parts(x, r):
        split = x == HALVES - 1 and r == count - 1 and middle > 0
        return [(0, middle), (middle, k)] if split else [(0, k)]

    def halo(x, r, side, part=0):
        c = 1 - x % 2
        start, stop = parts(x, r)[part]
        size = stop - start
        plain = sp.at[c, r, :, 1, pl.ds(PAD + start, size), :]
        above = planes + 1 if side == 0 else 0
        return pltpu.make_async_remote_copy(
            src_ref=plain if side == 0 else lifted.at[c, r, :, pl.ds(start, size), :],
            dst_ref=sp.at[c, r, :, above, pl.ds(PAD + start, size), :],
            send_sem=hsend.at[x % 2, r],
            recv_sem=hrecv.at[2 if part else x % 2, r if part == 0 else 0, side],
            device_id={"gz": down if side == 0 else up},
            device_id_type=MESH,
        )

    def sent(x, r):
        both = lifted.at[:, r]
        pltpu.make_async_copy(both, both, hsend.at[x % 2, r]).wait()

    def lift(c, r, d, start, value):
        part = pl.ds(start, value.shape[0])
        lifted[c, r, d, part, :] = zu[c, r, last, part, :] * value

    def inner(r, action):
        if planes > 2:
            lax.fori_loop(1, last, lambda z, carry: (action(r, z), carry)[1], 0)

    def ready():
        pl.semaphore_wait(barrier, expected)

    if near:

        @pl.when(g == n - 1)
        def _():
            ready()
            pl.semaphore_signal(wrap_sem, inc=1, device_id={"gz": up}, device_id_type=MESH)

    for load in loads[:6]:
        load.wait()
    for load in loads[6:]:
        load.start()

    def pack_edges(r):
        e = parity(r, last, k)
        even, odd = halves(coup_in, (2, last), 0, k)
        zu[0, r, last] = jnp.where(e, odd, even)
        zu[1, r, last] = jnp.where(e, even, odd)
        pack_spin(r, last)
        for d in range(3):
            lift(1, r, d, 0, sp[1, r, d, planes, pl.ds(PAD, k), :])
        pack_spin(r, 0)

    def slot_order(r):
        other = order_ref[r ^ 1]
        return jnp.where(bits_ref[r - r % 2] != 0, other, order_ref[r])

    def wide(value):
        return jnp.full((1, width), value, jnp.int32).astype(jnp.float32)

    for r in range(count):
        pack_edges(r)
        if r == 0:
            if near:
                pl.when(g < n - 1)(ready)
            else:
                ready()
        halo(0, r, 1).start()
        if near:
            pl.when(g > 0)(lambda: halo(0, r, 0).start())
        else:
            halo(0, r, 0).start()

    tsend[0, 0:1] = wide(slot_order(count - 1))
    tsend[0, 1:2] = wide(bits_ref[count - 1])
    tsend[0, 2:3] = wide(bits_ref[count - 2])
    tsend[1, 0:1] = wide(slot_order(0))
    tsend[1, 1:2] = wide(0)
    tsend[1, 2:3] = wide(bits_ref[0])
    for r in range(count):
        trecv[2, r : r + 1] = wide(slot_order(r))
        trecv[2, count + r : count + r + 1] = wide(bits_ref[r])

    def tell(side):
        return pltpu.make_async_remote_copy(
            src_ref=tsend.at[side],
            dst_ref=trecv.at[side],
            send_sem=tssem.at[side],
            recv_sem=trsem.at[side],
            device_id={"temp": t + 1 if side == 0 else t - 1},
            device_id_type=MESH,
        )

    along(1, lambda: tell(0).start())
    along(-1, lambda: tell(1).start())

    for load in loads[6:9]:
        load.wait()

    def pack_bonds(i, carry):
        r, z = i // planes, i % planes
        e = parity(r, z, k)
        even, odd = halves(coup_in, (0, z), 0, k)
        first, second = jnp.where(e, odd, even), jnp.where(e, even, odd)
        xo[0, r, z] = first
        xo[1, r, z] = second
        xr[0, r, z] = pltpu.roll(second, 1, 1)
        xr[1, r, z] = pltpu.roll(first, 1, 1)
        even, odd = halves(coup_in, (1, z), 0, k)
        before = pltpu.roll(odd, 1, 0)
        yi[r, z] = even
        yo[0, r, z] = jnp.where(e, odd, before)
        yo[1, r, z] = jnp.where(e, before, odd)
        return carry

    def pack_lower(i, carry):
        r, z = i // last, 1 + i % last
        e = parity(r, z, k)
        even, odd = halves(coup_in, (2, z - 1), 0, k)
        zd[0, r, z] = jnp.where(e, odd, even)
        zd[1, r, z] = jnp.where(e, even, odd)
        zu[0, r, z - 1] = jnp.where(e, even, odd)
        zu[1, r, z - 1] = jnp.where(e, odd, even)
        return carry

    for r in range(count):
        inner(r, pack_spin)
    lax.fori_loop(0, count * planes, pack_bonds, 0)
    lax.fori_loop(0, count * last, pack_lower, 0)
    for r in range(count):
        for c in (0, 1):
            zd[c, r, 0] = jnp.ones((k, width), jnp.float32)

    if near:

        @pl.when(g == 0)
        def _():
            pl.semaphore_wait(wrap_sem, 1)
            for r in range(count):
                halo(0, r, 0).start()

    def pull(c, r, z, start):
        o = 1 - c
        part = pl.ds(start, chunk)
        e = parity(r, z, chunk)
        bx, br, by = xo[c, r, z, part, :], xr[c, r, z, part, :], yi[r, z, part, :]
        bo, bu, bd = yo[c, r, z, part, :], zu[c, r, z, part, :], zd[c, r, z, part, :]
        pulled = []
        for d in range(3):
            mid = sp[o, r, d, z + 1, pl.ds(PAD + start, chunk), :]
            nxt = sp[o, r, d, z + 1, pl.ds(PAD + start + 1, chunk), :]
            prv = sp[o, r, d, z + 1, pl.ds(PAD + start - 1, chunk), :]
            outer = jnp.where(e, nxt, prv) if c == 0 else jnp.where(e, prv, nxt)
            total = bx * pltpu.roll(mid, width - 1, 1) + br * pltpu.roll(mid, 1, 1)
            total = total + by * mid + bo * outer
            total = total + bu * sp[o, r, d, z + 2, pl.ds(PAD + start, chunk), :]
            total = total + bd * sp[o, r, d, z, pl.ds(PAD + start, chunk), :]
            pulled.append(total)
        return pulled

    def relax(c, r, z, lifting=False):
        for start in range(0, k, chunk):
            pulled = pull(c, r, z, start)
            current = [sp[c, r, d, z + 1, pl.ds(PAD + start, chunk), :] for d in range(3)]
            for d, value in enumerate(reflect(current, pulled)):
                put_spin(c, r, d, z, start, value)
                if lifting:
                    lift(c, r, d, start, value)

    def heat(c, r, z, lifting=False, rows_of=(0, k)):
        for start in range(*rows_of, chunk):
            part = pl.ds(start, chunk)
            pulled = pull(c, r, z, start)
            trial = [ut[c, r, d, z, part, :] for d in range(3)]
            renewed = heat_bath(pulled, beta_ref[r], lv[c, r, z, part, :], trial)
            for d, value in enumerate(renewed):
                put_spin(c, r, d, z, start, value)
                if lifting:
                    lift(c, r, d, start, value)
            if c == 1:
                terms = dot3(renewed, pulled)
                eacc[r] = eacc[r] + sum(terms[j : j + 8] for j in range(0, chunk, 8))

    def pack_heat(r, z):
        for start in range(0, k, chunk):
            part = pl.ds(start, chunk)
            e = parity(r, z, chunk)
            even, odd = halves(level_in, (r, z), start, chunk)
            lv[0, r, z, part, :] = jnp.where(e, odd, even)
            lv[1, r, z, part, :] = jnp.where(e, even, odd)
            angles = halves(angle_in, (r, z), start, chunk)
            heights = halves(height_in, (r, z), start, chunk)
            trials = []
            for angle, height in zip(angles, heights):
                side = jnp.sqrt(jnp.maximum(1.0 - height * height, 0.0))
                cosine, sine = cos_sin(angle)
                trials.append((side * cosine, side * sine, height))
            for d in range(3):
                ut[0, r, d, z, part, :] = jnp.where(e, trials[1][d], trials[0][d])
                ut[1, r, d, z, part, :] = jnp.where(e, trials[0][d], trials[1][d])

    def take_halo(x, r, side):
        halo(x, r, 1 - side).wait_recv()
        if x >= 1 and side == 0:
            sent(x - 1, r)

    def settle(c, z, start, stop):
        size = stop - start
        part, packed = pl.ds(start, size), pl.ds(PAD + start, size)
        for r in range(0, count, 2):
            taking = flag(bits_ref, r, size, width)
            for d in range(3):
                low = sp[c, r, d, z + 1, packed, :]
                top = sp[c, r + 1, d, z + 1, packed, :]
                evened[r, c * planes + z, d, part, :] = jnp.where(taking, top, low)
                evened[r + 1, c * planes + z, d, part, :] = jnp.where(taking, low, top)

    final = parts(HALVES - 1, count - 1)

    def pieces(c, z):
        return final if c == 1 and z in (0, last) else [(0, k)]

    def ship(c, z, side, part=0, many=1):
        start, stop = pieces(c, z)[part]
        rows_of = pl.ds(start, stop - start)
        here = pl.ds(c * planes + z, many)
        early = c == 0 and 0 < z < last
        return pltpu.make_async_remote_copy(
            src_ref=evened.at[count - 1 if side == 0 else 0, here, :, rows_of, :],
            dst_ref=rbuf.at[side, here, :, rows_of, :],
            send_sem=xsend.at[side],
            recv_sem=xrecv.at[0 if early else 1, side],
            device_id={"temp": t + 1 if side == 0 else t - 1},
            device_id_type=MESH,
        )

    def both_ways(action):
        along(1, lambda: action(0))
        along(-1, lambda: action(1))

    def send_off(c, z, part=0):
        settle(c, z, *pieces(c, z)[part])
        both_ways(lambda side: ship(c, z, side, part).start())

    def send_inner(c):
        for z in range(1, last):
            settle(c, z, 0, k)
        if planes > 2:
            both_ways(lambda side: ship(c, 1, side, many=planes - 2).start())

    def whole(side, size, sem):
        ref = rbuf.at[side, pl.ds(0, size)]
        pltpu.make_async_copy(ref, ref, sem).wait()

    def arrived(early):
        size = planes - 2 if early else planes + 2
        if size:
            both_ways(lambda side: whole(1 - side, size, xrecv.at[0 if early else 1, 1 - side]))

    def work(x):
        return functools.partial(relax if x < relaxing else heat, x % 2)

    eacc[...] = jnp.zeros_like(eacc)
    relaxing = 2 * OR_SWEEPS
    for r in range(count):
        inner(r, work(0))
    for load in loads[9:]:
        load.wait()
    for x in range(HALVES - 1):
        for r in range(count):
            for side, z in ((0, 0), (1, last)):
                take_halo(x, r, side)
                work(x)(r, z, lifting=side == 1)
                if len(parts(x + 1, r)) == 1:
                    halo(x + 1, r, side).start()
            if len(parts(x + 1, r)) > 1:
                for part in (0, 1):
                    for side in (0, 1):
                        halo(x + 1, r, side, part).start()
            if r == count - 1 and x == relaxing:
                for z in (0, last):
                    send_off(0, z)
            for z in range(planes):
                if z % relaxing == x:
                    pack_heat(r, z)
            inner(r, work(x + 1))
        if x >= relaxing - 1:
            send_inner(x + 1 - relaxing)

    x = HALVES - 1
    for r in range(count):
        for part, rows_of in enumerate(parts(x, r)):
            for side, z in ((0, 0), (1, last)):
                halo(x, r, 1 - side, part).wait_recv()
                if part == 0 and side == 0:
                    sent(x - 1, r)
                work(x)(r, z, rows_of=rows_of)
                if r == count - 1:
                    send_off(1, z, part)
    for r in range(count):
        ebuf[1, g, r : r + 1] = jnp.sum(eacc[r], axis=0, keepdims=True)

    arrived(True)
    along(1, lambda: tell(1).wait_recv())
    along(-1, lambda: tell(0).wait_recv())

    def share(dt, source, there):
        return pltpu.make_async_remote_copy(
            src_ref=ebuf.at[1, source],
            dst_ref=ebuf.at[1 - dt, source],
            send_sem=esend.at[1 - dt],
            recv_sem=erecv.at[1 - dt],
            device_id=peer(dt, there),
            device_id_type=MESH,
        )

    def spread(dt):
        for d in range(1 if dt == 0 else 0, n):
            share(dt, g, lax.rem(g + d, n)).start()

    def shares(dt, sem):
        ref = ebuf.at[1, pl.ds(0, n - 1 if dt == 0 else n)]
        pltpu.make_async_copy(ref, ref, sem).wait()

    for dt in (0, 1, -1):
        along(dt, lambda dt=dt: spread(dt))
    for r in range(count):
        sent(x, r)
    along(1, lambda: tell(0).wait_send())
    along(-1, lambda: tell(1).wait_send())
    both_ways(lambda side: whole(side, 2 * planes, xsend.at[side]))
    arrived(False)
    for dt in (0, 1, -1):
        along(dt, lambda dt=dt: shares(dt, esend.at[1 - dt]))
        along(dt, lambda dt=dt: shares(dt, erecv.at[1 + dt]))


def finish_kernel(
    dims,
    evened,
    rbuf,
    trecv,
    ebuf,
    out_hbm,
    eout_hbm,
    stage,
    eout_ref,
    out_sem,
    eout_sem,
):
    count, planes, rows, width, n, m = dims
    k = rows // 2
    g = lax.axis_index("gz")
    t = lax.axis_index("temp")
    below, above = (t > 0).astype(jnp.int32), (t < m - 1).astype(jnp.int32)

    def number(side, row):
        return trecv[side, row : row + 1]

    def own_order(r):
        return number(2, r)

    def own_bit(r):
        return number(2, count + r)

    def mask(value, size):
        return jnp.broadcast_to(value, (size, width)) > 0.5

    def plan(r):
        if r == 0:
            met = jnp.full((1, width), below, jnp.int32) != 0
            return rbuf.at[0], jnp.where(met, number(0, 1), 0.0), jnp.where(met, number(0, 0), 0.0)
        if r == count - 1:
            met = jnp.full((1, width), above, jnp.int32) != 0
            return rbuf.at[1], jnp.where(met, own_bit(r), 0.0), jnp.where(met, number(1, 0), 0.0)
        other = r + 1 if r % 2 else r - 1
        return evened.at[other], own_bit(min(r, other)), own_order(other)

    lane = lax.broadcasted_iota(jnp.int32, (k, width), 1)
    plans = [plan(r) for r in range(count)]
    orders = [
        jnp.where(take > 0.5, order, own_order(r)).astype(jnp.int32)
        for r, (_, take, order) in enumerate(plans)
    ]
    sites = float(width * rows * planes * n)

    def total(slot, r):
        summed = ebuf[slot, 0, r : r + 1]
        for j in range(1, n):
            summed = summed + ebuf[slot, j, r : r + 1]
        return jnp.broadcast_to(jnp.sum(-summed, axis=1, keepdims=True) / sites, (1, width))

    energy = []
    for r in range(0, count, 2):
        taking = own_bit(r) > 0.5
        low, top = total(1, r), total(1, r + 1)
        energy += [jnp.where(taking, top, low), jnp.where(taking, low, top)]
    for r in range(count):
        other, take, _ = plans[r]
        if r == 0:
            swapped = number(0, 2) > 0.5
            partner = jnp.where(swapped, total(0, count - 2), total(0, count - 1))
        elif r == count - 1:
            swapped = number(1, 2) > 0.5
            partner = jnp.where(swapped, total(2, 1), total(2, 0))
        else:
            partner = energy[r + 1 if r % 2 else r - 1]
        eout_ref[r] = jnp.max(jnp.where(take > 0.5, partner, energy[r]))
    told = pltpu.make_async_copy(eout_ref, eout_hbm, eout_sem)
    told.start()
    for z in range(planes):
        for r in range(count):
            other, take, _ = plans[r]
            taking = mask(take, k)
            e = ((lane + (jnp.broadcast_to(orders[r], (k, width)) + (g * planes + z))) & 1) != 0
            for d in range(3):
                first, second = [
                    jnp.where(taking, other[i, d], evened[r, i, d]) for i in (z, planes + z)
                ]
                stage[r, d, z, pl.ds(0, k, stride=2), :] = jnp.where(e, second, first)
                stage[r, d, z, pl.ds(1, k, stride=2), :] = jnp.where(e, first, second)
            copy = pltpu.make_async_copy(
                stage.at[r, :, z], out_hbm.at[r, :, z], out_sem
            )
            copy.start()
    told.wait()
    pltpu.make_async_copy(stage, out_hbm, out_sem).wait()


def on_device(n, m, spin, coup, beta, order, level, height, angle, bits):
    count, _, planes, rows, width = spin.shape
    k = rows // 2
    f32 = jnp.float32
    hbm = pl.BlockSpec(memory_space=pltpu.HBM)
    vmem = pl.BlockSpec(memory_space=pltpu.VMEM)
    dma = pltpu.SemaphoreType.DMA
    bonds = pltpu.VMEM((2, count, planes, k, width), f32)
    dims = (count, planes, rows, width, n, m)
    handed = pl.pallas_call(
        functools.partial(sweep_kernel, dims),
        out_shape=(
            pltpu.VMEM((count, 2 * planes, 3, k, width), f32),
            pltpu.VMEM((2, 2 * planes, 3, k, width), f32),
            pltpu.VMEM((3, max(8, 2 * count), width), f32),
            pltpu.VMEM((3, n, count, width), f32),
        ),
        in_specs=[hbm] * 8,
        out_specs=(vmem,) * 4,
        scratch_shapes=[
            pltpu.VMEM(spin.shape, f32),
            pltpu.VMEM(coup.shape, f32),
            pltpu.VMEM(level.shape, f32),
            pltpu.VMEM(level.shape, f32),
            pltpu.VMEM(level.shape, f32),
            pltpu.VMEM((2, count, 3, k, width), f32),
            pltpu.VMEM((2, count, 3, planes + 2, k + 2 * PAD, width), f32),
            bonds,
            bonds,
            pltpu.VMEM((count, planes, k, width), f32),
            bonds,
            bonds,
            bonds,
            bonds,
            pltpu.VMEM((2, count, 3, planes, k, width), f32),
            pltpu.VMEM((count, 8, width), f32),
            pltpu.VMEM((2, max(8, 2 * count), width), f32),
            pltpu.SMEM((count,), f32),
            pltpu.SMEM((count,), jnp.int32),
            pltpu.SMEM((count,), jnp.int32),
            dma((6,)),
            dma((2, count)),
            dma((3, count, 2)),
            dma((3,)),
            dma((3,)),
            dma((2,)),
            dma((2,)),
            dma((2,)),
            dma((2, 2)),
            pltpu.SemaphoreType.REGULAR,
        ],
        compiler_params=pltpu.CompilerParams(
            collective_id=0, has_side_effects=True, vmem_limit_bytes=58 * 1024 * 1024
        ),
    )(spin, coup, beta, order, level, height, angle, bits)
    return pl.pallas_call(
        functools.partial(finish_kernel, dims),
        out_shape=(
            jax.ShapeDtypeStruct(spin.shape, f32),
            jax.ShapeDtypeStruct((count,), f32),
        ),
        in_specs=[vmem] * 4,
        out_specs=(hbm, hbm),
        scratch_shapes=[
            pltpu.VMEM(spin.shape, f32),
            pltpu.SMEM((count,), f32),
            dma(()),
            dma(()),
        ],
        compiler_params=pltpu.CompilerParams(vmem_limit_bytes=16 * 1024 * 1024),
    )(*handed)


def solution(mesh):
    n, m = mesh.shape["gz"], mesh.shape["temp"]
    return jax.shard_map(
        functools.partial(on_device, n, m),
        mesh=mesh,
        in_specs=(
            P(("group", "temp"), None, "gz", None, None),
            P(None, ("group", "gz"), None, None),
            P(("group", "temp")),
            P(("group", "temp")),
            P(("group", "temp"), "gz", None, None),
            P(("group", "temp"), "gz", None, None),
            P(("group", "temp"), "gz", None, None),
            P(("group", "temp")),
        ),
        out_specs=(P(("group", "temp"), None, "gz", None, None), P(("group", "temp"))),
        check_vma=False,
    )
```

```python
import functools
import math

import jax
import jax.numpy as jnp
from jax import lax
from jax.experimental import pallas as pl
from jax.experimental.pallas import tpu as pltpu
from jax.sharding import PartitionSpec as P

OR_SWEEPS = 2
HALVES = 2 * OR_SWEEPS + 2
PAD = 8
MESH = pl.DeviceIdType.MESH
SIN_TERMS = [(-1.0) ** i / math.factorial(2 * i + 1) for i in range(8)]
COS_TERMS = [(-1.0) ** i / math.factorial(2 * i) for i in range(9)]


def horner(terms, value):
    total = jnp.full_like(value, terms[-1])
    for term in terms[-2::-1]:
        total = total * value + term
    return total


def cos_sin(angle):
    half = 0.5 * angle
    square = half * half
    sine = half * horner(SIN_TERMS, square)
    cosine = horner(COS_TERMS, square)
    return 1.0 - 2.0 * sine * sine, 2.0 * sine * cosine


def dot3(a, b):
    return a[0] * b[0] + a[1] * b[1] + a[2] * b[2]


def reflect(current, pulled):
    factor = 2.0 * dot3(current, pulled) / jnp.maximum(dot3(pulled, pulled), 0.01)
    return [factor * p - s for p, s in zip(pulled, current)]


def heat_bath(pulled, beta, level, trial):
    strength = jnp.sqrt(jnp.maximum(dot3(pulled, pulled), 0.01))
    inverse = 1.0 / strength
    axis = [p * inverse for p in pulled]
    reach = beta * strength
    shrink = -jnp.tanh(reach) * (jnp.exp(-2.0 * reach) + 1.0)
    cosine = 1.0 + jnp.log1p(level * shrink) / reach
    along = dot3(trial, axis)
    tangent = [t - along * a for t, a in zip(trial, axis)]
    scale = jnp.sqrt(jnp.maximum(1.0 - cosine * cosine, 0.0)) * (
        1.0 / jnp.sqrt(jnp.maximum(dot3(tangent, tangent), 0.0001))
    )
    return [cosine * a + scale * t for a, t in zip(axis, tangent)]


def flag(bits_ref, j, size, width):
    return jnp.full((size, width), bits_ref[j], jnp.int32) != 0


def sweep_kernel(
    dims,
    spin_hbm,
    coup_hbm,
    beta_hbm,
    order_hbm,
    level_hbm,
    height_hbm,
    angle_hbm,
    bits_hbm,
    evened,
    rbuf,
    trecv,
    ebuf,
    spin_in,
    coup_in,
    level_in,
    height_in,
    angle_in,
    lifted,
    sp,
    xo,
    xr,
    yi,
    yo,
    zu,
    zd,
    lv,
    ut,
    eacc,
    tsend,
    beta_ref,
    order_ref,
    bits_ref,
    in_sem,
    hsend,
    hrecv,
    esend,
    erecv,
    tssem,
    trsem,
    xsend,
    xrecv,
    wrap_sem,
):
    count, planes, rows, width, n, m = dims
    k = rows // 2
    chunk = 32 if k % 32 == 0 else 8
    last = planes - 1
    g = lax.axis_index("gz")
    t = lax.axis_index("temp")
    up, down = lax.rem(g + 1, n), lax.rem(g + n - 1, n)
    has_below, has_above = t > 0, t < m - 1
    near = 2 < n <= 2 * HALVES - 2

    first = 2 * count + 4
    loads = [
        pltpu.make_async_copy(src, dst, in_sem.at[i % first])
        for i, (src, dst) in enumerate(
            (
                (order_hbm, order_ref),
                (coup_hbm.at[2, last], coup_in.at[2, last]),
                *(
                    (spin_hbm.at[r, :, z], spin_in.at[r, :, z])
                    for r in range(count)
                    for z in (last, 0)
                ),
                (bits_hbm, bits_ref),
                (beta_hbm, beta_ref),
                (coup_hbm.at[pl.ds(0, 2)], coup_in.at[pl.ds(0, 2)]),
                (coup_hbm.at[2, pl.ds(0, last)], coup_in.at[2, pl.ds(0, last)]),
                (
                    spin_hbm.at[:, :, pl.ds(1, planes - 2)],
                    spin_in.at[:, :, pl.ds(1, planes - 2)],
                ),
                (level_hbm, level_in),
                (height_hbm, height_in),
                (angle_hbm, angle_in),
            )
        )
    ]

    def peer(dt, there):
        return {"gz": there} if dt == 0 else {"temp": t + dt, "gz": there}

    def along(dt, action):
        if dt == 0:
            action()
        else:
            pl.when(has_below if dt < 0 else has_above)(action)

    for load in loads[:first]:
        load.start()

    barrier = pltpu.get_barrier_semaphore()

    def greet(dt, there):
        pl.semaphore_signal(barrier, inc=1, device_id=peer(dt, there), device_id_type=MESH)

    sides = has_below.astype(jnp.int32) + has_above.astype(jnp.int32)
    if near:

        @pl.when(g < n - 1)
        def _():
            greet(0, up)

        greet(0, down)
        along(-1, lambda: greet(-1, g))
        along(1, lambda: greet(1, g))
        expected = sides + jnp.where(g == 0, 1, 2)
    else:
        for dt in (-1, 0, 1):

            def greet_all(dt=dt):
                for d in range(1 if dt == 0 else 0, n):
                    greet(dt, lax.rem(g + d, n))

            along(dt, greet_all)
        expected = n - 1 + n * sides

    def parity(r, z, size):
        lane = lax.broadcasted_iota(jnp.int32, (size, width), 1)
        return ((lane + (g * planes + z + order_ref[r])) & 1) != 0

    def halves(ref, index, start, size):
        even = ref[index + (pl.ds(2 * start, size, stride=2), slice(None))]
        odd = ref[index + (pl.ds(2 * start + 1, size, stride=2), slice(None))]
        return even, odd

    def put_spin(c, r, d, z, start, value):
        size = value.shape[0]
        sp[c, r, d, z + 1, pl.ds(PAD + start, size), :] = value
        if start == 0:
            sp[c, r, d, z + 1, pl.ds(PAD + k, 1), :] = value[0:1]
        if start + size == k:
            sp[c, r, d, z + 1, pl.ds(PAD - 1, 1), :] = value[size - 1 : size]

    def pack_spin(r, z):
        e = parity(r, z, k)
        for d in range(3):
            even, odd = halves(spin_in, (r, d, z), 0, k)
            put_spin(0, r, d, z, 0, jnp.where(e, odd, even))
            put_spin(1, r, d, z, 0, jnp.where(e, even, odd))

    half, quarter = k // 2, k // 4

    def parts(x, r):
        if x < HALVES - 1 or r < count - 1 or quarter % 8:
            return [(0, k)]
        return [(0, half), (half, half + quarter), (half + quarter, k)]

    def halo(x, r, side, part=0):
        c = 1 - x % 2
        start, stop = parts(x, r)[part]
        size = stop - start
        plain = sp.at[c, r, :, 1, pl.ds(PAD + start, size), :]
        above = planes + 1 if side == 0 else 0
        return pltpu.make_async_remote_copy(
            src_ref=plain if side == 0 else lifted.at[c, r, :, pl.ds(start, size), :],
            dst_ref=sp.at[c, r, :, above, pl.ds(PAD + start, size), :],
            send_sem=hsend.at[x % 2, r],
            recv_sem=hrecv.at[part + 1 if part else x % 2, r if part == 0 else 0, side],
            device_id={"gz": down if side == 0 else up},
            device_id_type=MESH,
        )

    def sent(x, r):
        both = lifted.at[:, r]
        pltpu.make_async_copy(both, both, hsend.at[x % 2, r]).wait()

    def lift(c, r, d, start, value):
        part = pl.ds(start, value.shape[0])
        lifted[c, r, d, part, :] = zu[c, r, last, part, :] * value

    def inner(r, action):
        if planes > 2:
            lax.fori_loop(1, last, lambda z, carry: (action(r, z), carry)[1], 0)

    def ready():
        pl.semaphore_wait(barrier, expected)

    if near:

        @pl.when(g == n - 1)
        def _():
            ready()
            pl.semaphore_signal(wrap_sem, inc=1, device_id={"gz": up}, device_id_type=MESH)

    for load in loads[:4]:
        load.wait()
    for load in loads[first : first + 4]:
        load.start()

    def pack_edges(r):
        e = parity(r, last, k)
        even, odd = halves(coup_in, (2, last), 0, k)
        zu[0, r, last] = jnp.where(e, odd, even)
        zu[1, r, last] = jnp.where(e, even, odd)
        pack_spin(r, last)
        for d in range(3):
            lift(1, r, d, 0, sp[1, r, d, planes, pl.ds(PAD, k), :])
        pack_spin(r, 0)

    def slot_order(r):
        other = order_ref[r ^ 1]
        return jnp.where(bits_ref[r - r % 2] != 0, other, order_ref[r])

    def wide(value):
        return jnp.full((1, width), value, jnp.int32).astype(jnp.float32)

    for r in range(count):
        if r > 0:
            for load in loads[2 * r + 2 : 2 * r + 4]:
                load.wait()
        pack_edges(r)
        if r == 0:
            if near:
                pl.when(g < n - 1)(ready)
            else:
                ready()
        halo(0, r, 1).start()
        if near:
            pl.when(g > 0)(lambda: halo(0, r, 0).start())
        else:
            halo(0, r, 0).start()

    for load in loads[first - 2 : first]:
        load.wait()
    for load in loads[first + 4 :]:
        load.start()

    tsend[0, 0:1] = wide(slot_order(count - 1))
    tsend[0, 1:2] = wide(bits_ref[count - 1])
    tsend[0, 2:3] = wide(bits_ref[count - 2])
    tsend[1, 0:1] = wide(slot_order(0))
    tsend[1, 1:2] = wide(0)
    tsend[1, 2:3] = wide(bits_ref[0])
    for r in range(count):
        trecv[2, r : r + 1] = wide(slot_order(r))
        trecv[2, count + r : count + r + 1] = wide(bits_ref[r])

    def tell(side):
        return pltpu.make_async_remote_copy(
            src_ref=tsend.at[side],
            dst_ref=trecv.at[side],
            send_sem=tssem.at[side],
            recv_sem=trsem.at[side],
            device_id={"temp": t + 1 if side == 0 else t - 1},
            device_id_type=MESH,
        )

    along(1, lambda: tell(0).start())
    along(-1, lambda: tell(1).start())

    for load in loads[first : first + 3]:
        load.wait()

    def pack_bonds(i, carry):
        r, z = i // planes, i % planes
        e = parity(r, z, k)
        even, odd = halves(coup_in, (0, z), 0, k)
        first, second = jnp.where(e, odd, even), jnp.where(e, even, odd)
        xo[0, r, z] = first
        xo[1, r, z] = second
        xr[0, r, z] = pltpu.roll(second, 1, 1)
        xr[1, r, z] = pltpu.roll(first, 1, 1)
        even, odd = halves(coup_in, (1, z), 0, k)
        before = pltpu.roll(odd, 1, 0)
        yi[r, z] = even
        yo[0, r, z] = jnp.where(e, odd, before)
        yo[1, r, z] = jnp.where(e, before, odd)
        return carry

    def pack_lower(i, carry):
        r, z = i // last, 1 + i % last
        e = parity(r, z, k)
        even, odd = halves(coup_in, (2, z - 1), 0, k)
        zd[0, r, z] = jnp.where(e, odd, even)
        zd[1, r, z] = jnp.where(e, even, odd)
        zu[0, r, z - 1] = jnp.where(e, even, odd)
        zu[1, r, z - 1] = jnp.where(e, odd, even)
        return carry

    for r in range(count):
        inner(r, pack_spin)
    lax.fori_loop(0, count * planes, pack_bonds, 0)
    lax.fori_loop(0, count * last, pack_lower, 0)
    for r in range(count):
        for c in (0, 1):
            zd[c, r, 0] = jnp.ones((k, width), jnp.float32)

    if near:

        @pl.when(g == 0)
        def _():
            pl.semaphore_wait(wrap_sem, 1)
            for r in range(count):
                halo(0, r, 0).start()

    def pull(c, r, z, start, chunk=chunk):
        o = 1 - c
        part = pl.ds(start, chunk)
        e = parity(r, z, chunk)
        bx, br, by = xo[c, r, z, part, :], xr[c, r, z, part, :], yi[r, z, part, :]
        bo, bu, bd = yo[c, r, z, part, :], zu[c, r, z, part, :], zd[c, r, z, part, :]
        pulled = []
        for d in range(3):
            mid = sp[o, r, d, z + 1, pl.ds(PAD + start, chunk), :]
            nxt = sp[o, r, d, z + 1, pl.ds(PAD + start + 1, chunk), :]
            prv = sp[o, r, d, z + 1, pl.ds(PAD + start - 1, chunk), :]
            outer = jnp.where(e, nxt, prv) if c == 0 else jnp.where(e, prv, nxt)
            total = bx * pltpu.roll(mid, width - 1, 1) + br * pltpu.roll(mid, 1, 1)
            total = total + by * mid + bo * outer
            total = total + bu * sp[o, r, d, z + 2, pl.ds(PAD + start, chunk), :]
            total = total + bd * sp[o, r, d, z, pl.ds(PAD + start, chunk), :]
            pulled.append(total)
        return pulled

    def relax(c, r, z, lifting=False):
        for start in range(0, k, chunk):
            pulled = pull(c, r, z, start)
            current = [sp[c, r, d, z + 1, pl.ds(PAD + start, chunk), :] for d in range(3)]
            for d, value in enumerate(reflect(current, pulled)):
                put_spin(c, r, d, z, start, value)
                if lifting:
                    lift(c, r, d, start, value)

    def heat(c, r, z, lifting=False, rows_of=(0, k)):
        size = min(chunk, rows_of[1] - rows_of[0])
        for start in range(*rows_of, size):
            part = pl.ds(start, size)
            pulled = pull(c, r, z, start, size)
            trial = [ut[c, r, d, z, part, :] for d in range(3)]
            renewed = heat_bath(pulled, beta_ref[r], lv[c, r, z, part, :], trial)
            for d, value in enumerate(renewed):
                put_spin(c, r, d, z, start, value)
                if lifting:
                    lift(c, r, d, start, value)
            if c == 1:
                terms = dot3(renewed, pulled)
                eacc[r] = eacc[r] + sum(terms[j : j + 8] for j in range(0, size, 8))

    def pack_heat(r, z):
        for start in range(0, k, chunk):
            part = pl.ds(start, chunk)
            e = parity(r, z, chunk)
            even, odd = halves(level_in, (r, z), start, chunk)
            lv[0, r, z, part, :] = jnp.where(e, odd, even)
            lv[1, r, z, part, :] = jnp.where(e, even, odd)
            angles = halves(angle_in, (r, z), start, chunk)
            heights = halves(height_in, (r, z), start, chunk)
            trials = []
            for angle, height in zip(angles, heights):
                side = jnp.sqrt(jnp.maximum(1.0 - height * height, 0.0))
                cosine, sine = cos_sin(angle)
                trials.append((side * cosine, side * sine, height))
            for d in range(3):
                ut[0, r, d, z, part, :] = jnp.where(e, trials[1][d], trials[0][d])
                ut[1, r, d, z, part, :] = jnp.where(e, trials[0][d], trials[1][d])

    def take_halo(x, r, side):
        halo(x, r, 1 - side).wait_recv()
        if x >= 1 and side == 0:
            sent(x - 1, r)

    def settle(c, z, start, stop):
        size = stop - start
        part, packed = pl.ds(start, size), pl.ds(PAD + start, size)
        for r in range(0, count, 2):
            taking = flag(bits_ref, r, size, width)
            for d in range(3):
                low = sp[c, r, d, z + 1, packed, :]
                top = sp[c, r + 1, d, z + 1, packed, :]
                evened[r, c * planes + z, d, part, :] = jnp.where(taking, top, low)
                evened[r + 1, c * planes + z, d, part, :] = jnp.where(taking, low, top)

    final = parts(HALVES - 1, count - 1)

    def pieces(c, z):
        return final if c == 1 and z in (0, last) else [(0, k)]

    def ship(c, z, side, part=0, many=1):
        start, stop = pieces(c, z)[part]
        rows_of = pl.ds(start, stop - start)
        here = pl.ds(c * planes + z, many)
        early = c == 0 and 0 < z < last
        return pltpu.make_async_remote_copy(
            src_ref=evened.at[count - 1 if side == 0 else 0, here, :, rows_of, :],
            dst_ref=rbuf.at[side, here, :, rows_of, :],
            send_sem=xsend.at[side],
            recv_sem=xrecv.at[0 if early else 1, side],
            device_id={"temp": t + 1 if side == 0 else t - 1},
            device_id_type=MESH,
        )

    def both_ways(action):
        along(1, lambda: action(0))
        along(-1, lambda: action(1))

    def send_off(c, z, part=0):
        settle(c, z, *pieces(c, z)[part])
        both_ways(lambda side: ship(c, z, side, part).start())

    def send_inner(c):
        for z in range(1, last):
            settle(c, z, 0, k)
        if planes > 2:
            both_ways(lambda side: ship(c, 1, side, many=planes - 2).start())

    def whole(side, size, sem):
        ref = rbuf.at[side, pl.ds(0, size)]
        pltpu.make_async_copy(ref, ref, sem).wait()

    def arrived(early):
        size = planes - 2 if early else planes + 2
        if size:
            both_ways(lambda side: whole(1 - side, size, xrecv.at[0 if early else 1, 1 - side]))

    def work(x):
        return functools.partial(relax if x < relaxing else heat, x % 2)

    ahead = g < n - 1
    eacc[...] = jnp.zeros_like(eacc)
    relaxing = 2 * OR_SWEEPS
    for r in range(count):
        inner(r, work(0))
    for load in loads[first + 3 :]:
        load.wait()
    for x in range(HALVES - 1):
        for r in range(count):
            for side, z in ((0, 0), (1, last)):
                take_halo(x, r, side)
                work(x)(r, z, lifting=side == 1)
                if side == 0 and len(parts(x + 1, r)) == 1:
                    pl.when(ahead)(lambda: halo(x + 1, r, 0).start())
            for part in range(len(parts(x + 1, r))):
                if len(parts(x + 1, r)) > 1:
                    pl.when(ahead)(lambda: halo(x + 1, r, 0, part).start())
                halo(x + 1, r, 1, part).start()
                pl.when(~ahead)(lambda: halo(x + 1, r, 0, part).start())
            if r == count - 1 and x == relaxing:
                for z in (0, last):
                    send_off(0, z)
            for z in range(planes):
                if z % relaxing == x:
                    pack_heat(r, z)
            inner(r, work(x + 1))
        if x >= relaxing - 1:
            send_inner(x + 1 - relaxing)

    x = HALVES - 1
    for r in range(count):
        if r == count - 1:
            arrived(True)
            along(1, lambda: tell(1).wait_recv())
            along(-1, lambda: tell(0).wait_recv())
        for part, rows_of in enumerate(parts(x, r)):
            for side, z in ((0, 0), (1, last)):
                halo(x, r, 1 - side, part).wait_recv()
                if part == 0 and side == 0:
                    sent(x - 1, r)
                work(x)(r, z, rows_of=rows_of)
                if r == count - 1:
                    send_off(1, z, part)
    for r in range(count):
        ebuf[1, g, r : r + 1] = jnp.sum(eacc[r], axis=0, keepdims=True)

    def share(dt, source, there):
        return pltpu.make_async_remote_copy(
            src_ref=ebuf.at[1, source],
            dst_ref=ebuf.at[1 - dt, source],
            send_sem=esend.at[1 - dt],
            recv_sem=erecv.at[1 - dt],
            device_id=peer(dt, there),
            device_id_type=MESH,
        )

    def spread(dt):
        for d in range(1 if dt == 0 else 0, n):
            share(dt, g, lax.rem(g + d, n)).start()

    def shares(dt, sem):
        ref = ebuf.at[1, pl.ds(0, n - 1 if dt == 0 else n)]
        pltpu.make_async_copy(ref, ref, sem).wait()

    for dt in (0, 1, -1):
        along(dt, lambda dt=dt: spread(dt))
    for r in range(count):
        sent(x, r)
    along(1, lambda: tell(0).wait_send())
    along(-1, lambda: tell(1).wait_send())
    both_ways(lambda side: whole(side, 2 * planes, xsend.at[side]))
    arrived(False)
    for dt in (0, 1, -1):
        along(dt, lambda dt=dt: shares(dt, esend.at[1 - dt]))
        along(dt, lambda dt=dt: shares(dt, erecv.at[1 + dt]))


def finish_kernel(
    dims,
    evened,
    rbuf,
    trecv,
    ebuf,
    out_hbm,
    eout_hbm,
    stage,
    eout_ref,
    out_sem,
    eout_sem,
):
    count, planes, rows, width, n, m = dims
    k = rows // 2
    g = lax.axis_index("gz")
    t = lax.axis_index("temp")
    below, above = (t > 0).astype(jnp.int32), (t < m - 1).astype(jnp.int32)

    def number(side, row):
        return trecv[side, row : row + 1]

    def own_order(r):
        return number(2, r)

    def own_bit(r):
        return number(2, count + r)

    def mask(value, size):
        return jnp.broadcast_to(value, (size, width)) > 0.5

    def plan(r):
        if r == 0:
            met = jnp.full((1, width), below, jnp.int32) != 0
            return rbuf.at[0], jnp.where(met, number(0, 1), 0.0), jnp.where(met, number(0, 0), 0.0)
        if r == count - 1:
            met = jnp.full((1, width), above, jnp.int32) != 0
            return rbuf.at[1], jnp.where(met, own_bit(r), 0.0), jnp.where(met, number(1, 0), 0.0)
        other = r + 1 if r % 2 else r - 1
        return evened.at[other], own_bit(min(r, other)), own_order(other)

    lane = lax.broadcasted_iota(jnp.int32, (k, width), 1)
    plans = [plan(r) for r in range(count)]
    orders = [
        jnp.where(take > 0.5, order, own_order(r)).astype(jnp.int32)
        for r, (_, take, order) in enumerate(plans)
    ]
    sites = float(width * rows * planes * n)

    def total(slot, r):
        summed = ebuf[slot, 0, r : r + 1]
        for j in range(1, n):
            summed = summed + ebuf[slot, j, r : r + 1]
        return jnp.broadcast_to(jnp.sum(-summed, axis=1, keepdims=True) / sites, (1, width))

    energy = []
    for r in range(0, count, 2):
        taking = own_bit(r) > 0.5
        low, top = total(1, r), total(1, r + 1)
        energy += [jnp.where(taking, top, low), jnp.where(taking, low, top)]
    for r in range(count):
        other, take, _ = plans[r]
        if r == 0:
            swapped = number(0, 2) > 0.5
            partner = jnp.where(swapped, total(0, count - 2), total(0, count - 1))
        elif r == count - 1:
            swapped = number(1, 2) > 0.5
            partner = jnp.where(swapped, total(2, 1), total(2, 0))
        else:
            partner = energy[r + 1 if r % 2 else r - 1]
        eout_ref[r] = jnp.max(jnp.where(take > 0.5, partner, energy[r]))
    told = pltpu.make_async_copy(eout_ref, eout_hbm, eout_sem)
    told.start()
    for z in range(planes):
        for r in range(count):
            other, take, _ = plans[r]
            taking = mask(take, k)
            e = ((lane + (jnp.broadcast_to(orders[r], (k, width)) + (g * planes + z))) & 1) != 0
            for d in range(3):
                first, second = [
                    jnp.where(taking, other[i, d], evened[r, i, d]) for i in (z, planes + z)
                ]
                stage[r, d, z, pl.ds(0, k, stride=2), :] = jnp.where(e, second, first)
                stage[r, d, z, pl.ds(1, k, stride=2), :] = jnp.where(e, first, second)
            copy = pltpu.make_async_copy(
                stage.at[r, :, z], out_hbm.at[r, :, z], out_sem
            )
            copy.start()
    told.wait()
    pltpu.make_async_copy(stage, out_hbm, out_sem).wait()


def on_device(n, m, spin, coup, beta, order, level, height, angle, bits):
    count, _, planes, rows, width = spin.shape
    k = rows // 2
    f32 = jnp.float32
    hbm = pl.BlockSpec(memory_space=pltpu.HBM)
    vmem = pl.BlockSpec(memory_space=pltpu.VMEM)
    dma = pltpu.SemaphoreType.DMA
    bonds = pltpu.VMEM((2, count, planes, k, width), f32)
    dims = (count, planes, rows, width, n, m)
    handed = pl.pallas_call(
        functools.partial(sweep_kernel, dims),
        out_shape=(
            pltpu.VMEM((count, 2 * planes, 3, k, width), f32),
            pltpu.VMEM((2, 2 * planes, 3, k, width), f32),
            pltpu.VMEM((3, max(8, 2 * count), width), f32),
            pltpu.VMEM((3, n, count, width), f32),
        ),
        in_specs=[hbm] * 8,
        out_specs=(vmem,) * 4,
        scratch_shapes=[
            pltpu.VMEM(spin.shape, f32),
            pltpu.VMEM(coup.shape, f32),
            pltpu.VMEM(level.shape, f32),
            pltpu.VMEM(level.shape, f32),
            pltpu.VMEM(level.shape, f32),
            pltpu.VMEM((2, count, 3, k, width), f32),
            pltpu.VMEM((2, count, 3, planes + 2, k + 2 * PAD, width), f32),
            bonds,
            bonds,
            pltpu.VMEM((count, planes, k, width), f32),
            bonds,
            bonds,
            bonds,
            bonds,
            pltpu.VMEM((2, count, 3, planes, k, width), f32),
            pltpu.VMEM((count, 8, width), f32),
            pltpu.VMEM((2, max(8, 2 * count), width), f32),
            pltpu.SMEM((count,), f32),
            pltpu.SMEM((count,), jnp.int32),
            pltpu.SMEM((count,), jnp.int32),
            dma((2 * count + 4,)),
            dma((2, count)),
            dma((4, count, 2)),
            dma((3,)),
            dma((3,)),
            dma((2,)),
            dma((2,)),
            dma((2,)),
            dma((2, 2)),
            pltpu.SemaphoreType.REGULAR,
        ],
        compiler_params=pltpu.CompilerParams(
            collective_id=0, has_side_effects=True, vmem_limit_bytes=58 * 1024 * 1024
        ),
    )(spin, coup, beta, order, level, height, angle, bits)
    return pl.pallas_call(
        functools.partial(finish_kernel, dims),
        out_shape=(
            jax.ShapeDtypeStruct(spin.shape, f32),
            jax.ShapeDtypeStruct((count,), f32),
        ),
        in_specs=[vmem] * 4,
        out_specs=(hbm, hbm),
        scratch_shapes=[
            pltpu.VMEM(spin.shape, f32),
            pltpu.SMEM((count,), f32),
            dma(()),
            dma(()),
        ],
        compiler_params=pltpu.CompilerParams(vmem_limit_bytes=16 * 1024 * 1024),
    )(*handed)


def solution(mesh):
    n, m = mesh.shape["gz"], mesh.shape["temp"]
    return jax.shard_map(
        functools.partial(on_device, n, m),
        mesh=mesh,
        in_specs=(
            P(("group", "temp"), None, "gz", None, None),
            P(None, ("group", "gz"), None, None),
            P(("group", "temp")),
            P(("group", "temp")),
            P(("group", "temp"), "gz", None, None),
            P(("group", "temp"), "gz", None, None),
            P(("group", "temp"), "gz", None, None),
            P(("group", "temp")),
        ),
        out_specs=(P(("group", "temp"), None, "gz", None, None), P(("group", "temp"))),
        check_vma=False,
    )
```

```python
import functools
import math

import jax
import jax.numpy as jnp
from jax import lax
from jax.experimental import pallas as pl
from jax.experimental.pallas import tpu as pltpu
from jax.sharding import PartitionSpec as P

OR_SWEEPS = 2
HALVES = 2 * OR_SWEEPS + 2
PAD = 8
MESH = pl.DeviceIdType.MESH
SIN_TERMS = [(-1.0) ** i / math.factorial(2 * i + 1) for i in range(8)]
COS_TERMS = [(-1.0) ** i / math.factorial(2 * i) for i in range(9)]


def horner(terms, value):
    total = jnp.full_like(value, terms[-1])
    for term in terms[-2::-1]:
        total = total * value + term
    return total


def cos_sin(angle):
    half = 0.5 * angle
    square = half * half
    sine = half * horner(SIN_TERMS, square)
    cosine = horner(COS_TERMS, square)
    return 1.0 - 2.0 * sine * sine, 2.0 * sine * cosine


def with_sign(size, like):
    return jnp.where(like < 0.0, -size, size)


def to_square(vector):
    a, b, c = vector
    inverse = 1.0 / (jnp.abs(a) + jnp.abs(b) + jnp.abs(c))
    p, q = a * inverse, b * inverse
    low = c < 0.0
    return (
        jnp.where(low, with_sign(1.0 - jnp.abs(q), p), p),
        jnp.where(low, with_sign(1.0 - jnp.abs(p), q), q),
    )


def from_square(p, q):
    c = 1.0 - jnp.abs(p) - jnp.abs(q)
    low = c < 0.0
    a = jnp.where(low, with_sign(1.0 - jnp.abs(q), p), p)
    b = jnp.where(low, with_sign(1.0 - jnp.abs(p), q), q)
    inverse = 1.0 / jnp.sqrt(a * a + b * b + c * c)
    return a * inverse, b * inverse, c * inverse


def dot3(a, b):
    return a[0] * b[0] + a[1] * b[1] + a[2] * b[2]


def reflect(current, pulled):
    factor = 2.0 * dot3(current, pulled) / jnp.maximum(dot3(pulled, pulled), 0.01)
    return [factor * p - s for p, s in zip(pulled, current)]


def heat_bath(pulled, beta, level, trial):
    strength = jnp.sqrt(jnp.maximum(dot3(pulled, pulled), 0.01))
    inverse = 1.0 / strength
    axis = [p * inverse for p in pulled]
    reach = beta * strength
    shrink = -jnp.tanh(reach) * (jnp.exp(-2.0 * reach) + 1.0)
    cosine = 1.0 + jnp.log1p(level * shrink) / reach
    along = dot3(trial, axis)
    tangent = [t - along * a for t, a in zip(trial, axis)]
    scale = jnp.sqrt(jnp.maximum(1.0 - cosine * cosine, 0.0)) * (
        1.0 / jnp.sqrt(jnp.maximum(dot3(tangent, tangent), 0.0001))
    )
    return [cosine * a + scale * t for a, t in zip(axis, tangent)]


def flag(bits_ref, j, size, width):
    return jnp.full((size, width), bits_ref[j], jnp.int32) != 0


def sweep_kernel(
    dims,
    spin_hbm,
    coup_hbm,
    beta_hbm,
    order_hbm,
    level_hbm,
    height_hbm,
    angle_hbm,
    bits_hbm,
    evened,
    rbuf,
    trecv,
    ebuf,
    spin_in,
    coup_in,
    level_in,
    height_in,
    angle_in,
    lifted,
    osend,
    orecv,
    cbelow,
    sp,
    xo,
    xr,
    yi,
    yo,
    zu,
    zd,
    lv,
    ut,
    eacc,
    tsend,
    beta_ref,
    order_ref,
    bits_ref,
    in_sem,
    hsend,
    hrecv,
    esend,
    erecv,
    tssem,
    trsem,
    xsend,
    xrecv,
    csem,
    wrap_sem,
):
    count, planes, rows, width, n, m = dims
    k = rows // 2
    chunk = 32 if k % 32 == 0 else 8
    last = planes - 1
    g = lax.axis_index("gz")
    t = lax.axis_index("temp")
    up, down = lax.rem(g + 1, n), lax.rem(g + n - 1, n)
    has_below, has_above = t > 0, t < m - 1
    near = 2 < n <= 2 * HALVES - 2

    first = 2 * count + 4
    loads = [
        pltpu.make_async_copy(src, dst, in_sem.at[i % first])
        for i, (src, dst) in enumerate(
            (
                (order_hbm, order_ref),
                (coup_hbm.at[2, last], coup_in.at[2, last]),
                *(
                    (spin_hbm.at[r, :, z], spin_in.at[r, :, z])
                    for r in range(count)
                    for z in (last, 0)
                ),
                (bits_hbm, bits_ref),
                (beta_hbm, beta_ref),
                (coup_hbm.at[pl.ds(0, 2)], coup_in.at[pl.ds(0, 2)]),
                (coup_hbm.at[2, pl.ds(0, last)], coup_in.at[2, pl.ds(0, last)]),
                (
                    spin_hbm.at[:, :, pl.ds(1, planes - 2)],
                    spin_in.at[:, :, pl.ds(1, planes - 2)],
                ),
                (level_hbm, level_in),
                (height_hbm, height_in),
                (angle_hbm, angle_in),
            )
        )
    ]

    def peer(dt, there):
        return {"gz": there} if dt == 0 else {"temp": t + dt, "gz": there}

    def along(dt, action):
        if dt == 0:
            action()
        else:
            pl.when(has_below if dt < 0 else has_above)(action)

    for load in loads[:first]:
        load.start()

    barrier = pltpu.get_barrier_semaphore()

    def greet(temp, there):
        target = {"temp": temp, "gz": there}
        pl.semaphore_signal(barrier, inc=1, device_id=target, device_id_type=MESH)

    if near:
        pl.when(g < n - 1)(lambda: greet(t, up))
        greet(t, down)
        for d in range(1, m):
            greet(lax.rem(t + d, m), g)
        expected = m - 1 + jnp.where(g == 0, 1, 2)
    else:
        for i in range(1, n * m):
            greet(lax.rem(t + i // n, m), lax.rem(g + i % n, n))
        expected = n * m - 1

    def parity(r, z, size):
        lane = lax.broadcasted_iota(jnp.int32, (size, width), 1)
        return ((lane + (g * planes + z + order_ref[r])) & 1) != 0

    def halves(ref, index, start, size):
        even = ref[index + (pl.ds(2 * start, size, stride=2), slice(None))]
        odd = ref[index + (pl.ds(2 * start + 1, size, stride=2), slice(None))]
        return even, odd

    def put_spin(c, r, d, z, start, value):
        size = value.shape[0]
        sp[c, r, d, z + 1, pl.ds(PAD + start, size), :] = value
        if start == 0:
            sp[c, r, d, z + 1, pl.ds(PAD + k, 1), :] = value[0:1]
        if start + size == k:
            sp[c, r, d, z + 1, pl.ds(PAD - 1, 1), :] = value[size - 1 : size]

    def pack_spin(r, z):
        e = parity(r, z, k)
        for d in range(3):
            even, odd = halves(spin_in, (r, d, z), 0, k)
            put_spin(0, r, d, z, 0, jnp.where(e, odd, even))
            put_spin(1, r, d, z, 0, jnp.where(e, even, odd))

    half, quarter = k // 2, k // 4

    def parts(x, r):
        if x < HALVES - 1 or r < count - 1 or quarter % 8:
            return [(0, k)]
        return [(0, half), (half, half + quarter), (half + quarter, k)]

    def halo(x, r, side, part=0):
        c = 1 - x % 2
        start, stop = parts(x, r)[part]
        size = stop - start
        plain = sp.at[c, r, :, 1, pl.ds(PAD + start, size), :]
        above = planes + 1 if side == 0 else 0
        return pltpu.make_async_remote_copy(
            src_ref=plain if side == 0 else lifted.at[c, r, :, pl.ds(start, size), :],
            dst_ref=sp.at[c, r, :, above, pl.ds(PAD + start, size), :],
            send_sem=hsend.at[x % 2, r],
            recv_sem=hrecv.at[part + 1 if part else x % 2, r if part == 0 else 0, side],
            device_id={"gz": down if side == 0 else up},
            device_id_type=MESH,
        )

    def opening(r, side):
        return pltpu.make_async_remote_copy(
            src_ref=osend.at[r, side],
            dst_ref=orecv.at[r, side],
            send_sem=hsend.at[0, r],
            recv_sem=hrecv.at[0, r, side],
            device_id={"gz": down if side == 0 else up},
            device_id_type=MESH,
        )

    shares_of = m if rows % (8 * m) == 0 else 1
    size_of = rows // shares_of
    stretch = pl.ds(pl.multiple_of(t * size_of, 8) if shares_of > 1 else 0, size_of)

    def across():
        return pltpu.make_async_remote_copy(
            src_ref=coup_in.at[2, last, stretch],
            dst_ref=cbelow.at[stretch],
            send_sem=csem.at[0],
            recv_sem=csem.at[1],
            device_id={"gz": up},
            device_id_type=MESH,
        )

    def pass_on(d):
        return pltpu.make_async_remote_copy(
            src_ref=cbelow.at[stretch],
            dst_ref=cbelow.at[stretch],
            send_sem=csem.at[2],
            recv_sem=csem.at[3],
            device_id={"temp": lax.rem(t + d, m)},
            device_id_type=MESH,
        )

    def passed_on(i):
        if shares_of > 1:
            ref = cbelow.at[pl.ds(0, (m - 1) * size_of)]
            pltpu.make_async_copy(ref, ref, csem.at[i]).wait()

    def sent(x, r):
        both = lifted.at[:, r] if x else osend.at[r]
        pltpu.make_async_copy(both, both, hsend.at[x % 2, r]).wait()

    def lift(c, r, d, start, value):
        part = pl.ds(start, value.shape[0])
        lifted[c, r, d, part, :] = zu[c, r, last, part, :] * value

    def inner(r, action):
        if planes > 2:
            lax.fori_loop(1, last, lambda z, carry: (action(r, z), carry)[1], 0)

    def ready():
        pl.semaphore_wait(barrier, expected)

    if near:

        @pl.when(g == n - 1)
        def _():
            ready()
            pl.semaphore_signal(wrap_sem, inc=1, device_id={"gz": up}, device_id_type=MESH)

    for load in loads[:4]:
        load.wait()
    if near:
        pl.when(g == n - 1)(lambda: across().start())
    for load in loads[first : first + 4]:
        load.start()

    def pack_edges(r):
        e = parity(r, last, k)
        even, odd = halves(coup_in, (2, last), 0, k)
        zu[0, r, last] = jnp.where(e, odd, even)
        zu[1, r, last] = jnp.where(e, even, odd)
        for side, z in ((1, last), (0, 0)):
            pack_spin(r, z)
            edge = to_square([sp[1, r, d, z + 1, pl.ds(PAD, k), :] for d in range(3)])
            osend[r, side, 0], osend[r, side, 1] = edge

    def slot_order(r):
        other = order_ref[r ^ 1]
        return jnp.where(bits_ref[r - r % 2] != 0, other, order_ref[r])

    def wide(value):
        return jnp.full((1, width), value, jnp.int32).astype(jnp.float32)

    for r in range(count):
        if r > 0:
            for load in loads[2 * r + 2 : 2 * r + 4]:
                load.wait()
        pack_edges(r)
        if r == 0:
            if near:

                @pl.when(g < n - 1)
                def _():
                    ready()
                    across().start()

            else:
                ready()
                across().start()
        opening(r, 1).start()
        if near:
            pl.when(g > 0)(lambda: opening(r, 0).start())
        else:
            opening(r, 0).start()

    for load in loads[first - 2 : first]:
        load.wait()
    for load in loads[first + 4 :]:
        load.start()

    tsend[0, 0:1] = wide(slot_order(count - 1))
    tsend[0, 1:2] = wide(bits_ref[count - 1])
    tsend[0, 2:3] = wide(bits_ref[count - 2])
    tsend[1, 0:1] = wide(slot_order(0))
    tsend[1, 1:2] = wide(0)
    tsend[1, 2:3] = wide(bits_ref[0])
    for r in range(count):
        trecv[2, r : r + 1] = wide(slot_order(r))
        trecv[2, count + r : count + r + 1] = wide(bits_ref[r])

    def tell(side):
        return pltpu.make_async_remote_copy(
            src_ref=tsend.at[side],
            dst_ref=trecv.at[side],
            send_sem=tssem.at[side],
            recv_sem=trsem.at[side],
            device_id={"temp": t + 1 if side == 0 else t - 1},
            device_id_type=MESH,
        )

    along(1, lambda: tell(0).start())
    along(-1, lambda: tell(1).start())

    for load in loads[first : first + 3]:
        load.wait()

    def pack_bonds(i, carry):
        r, z = i // planes, i % planes
        e = parity(r, z, k)
        even, odd = halves(coup_in, (0, z), 0, k)
        first, second = jnp.where(e, odd, even), jnp.where(e, even, odd)
        xo[0, r, z] = first
        xo[1, r, z] = second
        xr[0, r, z] = pltpu.roll(second, 1, 1)
        xr[1, r, z] = pltpu.roll(first, 1, 1)
        even, odd = halves(coup_in, (1, z), 0, k)
        before = pltpu.roll(odd, 1, 0)
        yi[r, z] = even
        yo[0, r, z] = jnp.where(e, odd, before)
        yo[1, r, z] = jnp.where(e, before, odd)
        return carry

    def pack_lower(i, carry):
        r, z = i // last, 1 + i % last
        e = parity(r, z, k)
        even, odd = halves(coup_in, (2, z - 1), 0, k)
        zd[0, r, z] = jnp.where(e, odd, even)
        zd[1, r, z] = jnp.where(e, even, odd)
        zu[0, r, z - 1] = jnp.where(e, even, odd)
        zu[1, r, z - 1] = jnp.where(e, odd, even)
        return carry

    for r in range(count):
        inner(r, pack_spin)
    lax.fori_loop(0, count * planes, pack_bonds, 0)
    lax.fori_loop(0, count * last, pack_lower, 0)
    for r in range(count):
        for c in (0, 1):
            zd[c, r, 0] = jnp.ones((k, width), jnp.float32)

    if near:

        @pl.when(g == 0)
        def _():
            pl.semaphore_wait(wrap_sem, 1)
            for r in range(count):
                opening(r, 0).start()

    def pull(c, r, z, start, chunk=chunk):
        o = 1 - c
        part = pl.ds(start, chunk)
        e = parity(r, z, chunk)
        bx, br, by = xo[c, r, z, part, :], xr[c, r, z, part, :], yi[r, z, part, :]
        bo, bu, bd = yo[c, r, z, part, :], zu[c, r, z, part, :], zd[c, r, z, part, :]
        pulled = []
        for d in range(3):
            mid = sp[o, r, d, z + 1, pl.ds(PAD + start, chunk), :]
            nxt = sp[o, r, d, z + 1, pl.ds(PAD + start + 1, chunk), :]
            prv = sp[o, r, d, z + 1, pl.ds(PAD + start - 1, chunk), :]
            outer = jnp.where(e, nxt, prv) if c == 0 else jnp.where(e, prv, nxt)
            total = bx * pltpu.roll(mid, width - 1, 1) + br * pltpu.roll(mid, 1, 1)
            total = total + by * mid + bo * outer
            total = total + bu * sp[o, r, d, z + 2, pl.ds(PAD + start, chunk), :]
            total = total + bd * sp[o, r, d, z, pl.ds(PAD + start, chunk), :]
            pulled.append(total)
        return pulled

    def relax(c, r, z, lifting=False):
        for start in range(0, k, chunk):
            pulled = pull(c, r, z, start)
            current = [sp[c, r, d, z + 1, pl.ds(PAD + start, chunk), :] for d in range(3)]
            for d, value in enumerate(reflect(current, pulled)):
                put_spin(c, r, d, z, start, value)
                if lifting:
                    lift(c, r, d, start, value)

    def heat(c, r, z, lifting=False, rows_of=(0, k)):
        size = min(chunk, rows_of[1] - rows_of[0])
        for start in range(*rows_of, size):
            part = pl.ds(start, size)
            pulled = pull(c, r, z, start, size)
            trial = [ut[c, r, d, z, part, :] for d in range(3)]
            renewed = heat_bath(pulled, beta_ref[r], lv[c, r, z, part, :], trial)
            for d, value in enumerate(renewed):
                put_spin(c, r, d, z, start, value)
                if lifting:
                    lift(c, r, d, start, value)
            if c == 1:
                terms = dot3(renewed, pulled)
                eacc[r] = eacc[r] + sum(terms[j : j + 8] for j in range(0, size, 8))

    def pack_heat(r, z):
        for start in range(0, k, chunk):
            part = pl.ds(start, chunk)
            e = parity(r, z, chunk)
            even, odd = halves(level_in, (r, z), start, chunk)
            lv[0, r, z, part, :] = jnp.where(e, odd, even)
            lv[1, r, z, part, :] = jnp.where(e, even, odd)
            angles = halves(angle_in, (r, z), start, chunk)
            heights = halves(height_in, (r, z), start, chunk)
            trials = []
            for angle, height in zip(angles, heights):
                side = jnp.sqrt(jnp.maximum(1.0 - height * height, 0.0))
                cosine, sine = cos_sin(angle)
                trials.append((side * cosine, side * sine, height))
            for d in range(3):
                ut[0, r, d, z, part, :] = jnp.where(e, trials[1][d], trials[0][d])
                ut[1, r, d, z, part, :] = jnp.where(e, trials[0][d], trials[1][d])

    def take_halo(x, r, side):
        halo(x, r, 1 - side).wait_recv()
        if side == 0:
            sent(x - 1, r)

    def take_opening(r, side):
        opening(r, 1 - side).wait_recv()
        vector = from_square(orecv[r, 1 - side, 0], orecv[r, 1 - side, 1])
        if side == 0:
            even, odd = halves(cbelow, (), 0, k)
            bond = jnp.where(parity(r, 0, k), odd, even)
            vector = [bond * v for v in vector]
        for d in range(3):
            sp[1, r, d, planes + 1 if side else 0, pl.ds(PAD, k), :] = vector[d]

    def settle(c, z, start, stop):
        size = stop - start
        part, packed = pl.ds(start, size), pl.ds(PAD + start, size)
        for r in range(0, count, 2):
            taking = flag(bits_ref, r, size, width)
            for d in range(3):
                low = sp[c, r, d, z + 1, packed, :]
                top = sp[c, r + 1, d, z + 1, packed, :]
                evened[r, c * planes + z, d, part, :] = jnp.where(taking, top, low)
                evened[r + 1, c * planes + z, d, part, :] = jnp.where(taking, low, top)

    final = parts(HALVES - 1, count - 1)

    def pieces(c, z):
        return final if c == 1 and z in (0, last) else [(0, k)]

    def ship(c, z, side, part=0, many=1):
        start, stop = pieces(c, z)[part]
        rows_of = pl.ds(start, stop - start)
        here = pl.ds(c * planes + z, many)
        early = c == 0 and 0 < z < last
        return pltpu.make_async_remote_copy(
            src_ref=evened.at[count - 1 if side == 0 else 0, here, :, rows_of, :],
            dst_ref=rbuf.at[side, here, :, rows_of, :],
            send_sem=xsend.at[side],
            recv_sem=xrecv.at[0 if early else 1, side],
            device_id={"temp": t + 1 if side == 0 else t - 1},
            device_id_type=MESH,
        )

    def both_ways(action):
        along(1, lambda: action(0))
        along(-1, lambda: action(1))

    def send_off(c, z, part=0):
        settle(c, z, *pieces(c, z)[part])
        both_ways(lambda side: ship(c, z, side, part).start())

    def send_inner(c):
        for z in range(1, last):
            settle(c, z, 0, k)
        if planes > 2:
            both_ways(lambda side: ship(c, 1, side, many=planes - 2).start())

    def whole(side, size, sem):
        ref = rbuf.at[side, pl.ds(0, size)]
        pltpu.make_async_copy(ref, ref, sem).wait()

    def arrived(early):
        size = planes - 2 if early else planes + 2
        if size:
            both_ways(lambda side: whole(1 - side, size, xrecv.at[0 if early else 1, 1 - side]))

    def work(x):
        return functools.partial(relax if x < relaxing else heat, x % 2)

    ahead = g < n - 1
    eacc[...] = jnp.zeros_like(eacc)
    relaxing = 2 * OR_SWEEPS
    for r in range(count):
        inner(r, work(0))
    for load in loads[first + 3 :]:
        load.wait()
    across().wait_recv()
    if shares_of > 1:
        for d in range(1, m):
            pass_on(d).start()
    for x in range(HALVES - 1):
        for r in range(count):
            for side, z in ((0, 0), (1, last)) if x else ((1, last), (0, 0)):
                if x:
                    take_halo(x, r, side)
                else:
                    if r == 0 and side == 0:
                        passed_on(3)
                    take_opening(r, side)
                work(x)(r, z, lifting=side == 1)
                if x == 0:
                    halo(1, r, side).start()
                elif side == 0 and len(parts(x + 1, r)) == 1:
                    pl.when(ahead)(lambda: halo(x + 1, r, 0).start())
            for part in range(len(parts(x + 1, r)) if x else 0):
                if len(parts(x + 1, r)) > 1:
                    pl.when(ahead)(lambda: halo(x + 1, r, 0, part).start())
                halo(x + 1, r, 1, part).start()
                pl.when(~ahead)(lambda: halo(x + 1, r, 0, part).start())
            if r == count - 1 and x == relaxing:
                for z in (0, last):
                    send_off(0, z)
            for z in range(planes):
                if z % relaxing == x:
                    pack_heat(r, z)
            inner(r, work(x + 1))
        if x >= relaxing - 1:
            send_inner(x + 1 - relaxing)

    x = HALVES - 1
    for r in range(count):
        if r == count - 1:
            arrived(True)
            along(1, lambda: tell(1).wait_recv())
            along(-1, lambda: tell(0).wait_recv())
        for part, rows_of in enumerate(parts(x, r)):
            for side, z in ((0, 0), (1, last)):
                halo(x, r, 1 - side, part).wait_recv()
                if part == 0 and side == 0:
                    sent(x - 1, r)
                work(x)(r, z, rows_of=rows_of)
                if r == count - 1:
                    send_off(1, z, part)
    for r in range(count):
        ebuf[1, g, r : r + 1] = jnp.sum(eacc[r], axis=0, keepdims=True)

    def share(dt, source, there):
        return pltpu.make_async_remote_copy(
            src_ref=ebuf.at[1, source],
            dst_ref=ebuf.at[1 - dt, source],
            send_sem=esend.at[1 - dt],
            recv_sem=erecv.at[1 - dt],
            device_id=peer(dt, there),
            device_id_type=MESH,
        )

    def spread(dt):
        for d in range(1 if dt == 0 else 0, n):
            share(dt, g, lax.rem(g + d, n)).start()

    def shares(dt, sem):
        ref = ebuf.at[1, pl.ds(0, n - 1 if dt == 0 else n)]
        pltpu.make_async_copy(ref, ref, sem).wait()

    for dt in (0, 1, -1):
        along(dt, lambda dt=dt: spread(dt))
    for r in range(count):
        sent(x, r)
    across().wait_send()
    passed_on(2)
    along(1, lambda: tell(0).wait_send())
    along(-1, lambda: tell(1).wait_send())
    both_ways(lambda side: whole(side, 2 * planes, xsend.at[side]))
    arrived(False)
    for dt in (0, 1, -1):
        along(dt, lambda dt=dt: shares(dt, esend.at[1 - dt]))
        along(dt, lambda dt=dt: shares(dt, erecv.at[1 + dt]))


def finish_kernel(
    dims,
    evened,
    rbuf,
    trecv,
    ebuf,
    out_hbm,
    eout_hbm,
    stage,
    eout_ref,
    out_sem,
    eout_sem,
):
    count, planes, rows, width, n, m = dims
    k = rows // 2
    g = lax.axis_index("gz")
    t = lax.axis_index("temp")
    below, above = (t > 0).astype(jnp.int32), (t < m - 1).astype(jnp.int32)

    def number(side, row):
        return trecv[side, row : row + 1]

    def own_order(r):
        return number(2, r)

    def own_bit(r):
        return number(2, count + r)

    def mask(value, size):
        return jnp.broadcast_to(value, (size, width)) > 0.5

    def plan(r):
        if r == 0:
            met = jnp.full((1, width), below, jnp.int32) != 0
            return rbuf.at[0], jnp.where(met, number(0, 1), 0.0), jnp.where(met, number(0, 0), 0.0)
        if r == count - 1:
            met = jnp.full((1, width), above, jnp.int32) != 0
            return rbuf.at[1], jnp.where(met, own_bit(r), 0.0), jnp.where(met, number(1, 0), 0.0)
        other = r + 1 if r % 2 else r - 1
        return evened.at[other], own_bit(min(r, other)), own_order(other)

    lane = lax.broadcasted_iota(jnp.int32, (k, width), 1)
    plans = [plan(r) for r in range(count)]
    orders = [
        jnp.where(take > 0.5, order, own_order(r)).astype(jnp.int32)
        for r, (_, take, order) in enumerate(plans)
    ]
    sites = float(width * rows * planes * n)

    def total(slot, r):
        summed = ebuf[slot, 0, r : r + 1]
        for j in range(1, n):
            summed = summed + ebuf[slot, j, r : r + 1]
        return jnp.broadcast_to(jnp.sum(-summed, axis=1, keepdims=True) / sites, (1, width))

    energy = []
    for r in range(0, count, 2):
        taking = own_bit(r) > 0.5
        low, top = total(1, r), total(1, r + 1)
        energy += [jnp.where(taking, top, low), jnp.where(taking, low, top)]
    for r in range(count):
        other, take, _ = plans[r]
        if r == 0:
            swapped = number(0, 2) > 0.5
            partner = jnp.where(swapped, total(0, count - 2), total(0, count - 1))
        elif r == count - 1:
            swapped = number(1, 2) > 0.5
            partner = jnp.where(swapped, total(2, 1), total(2, 0))
        else:
            partner = energy[r + 1 if r % 2 else r - 1]
        eout_ref[r] = jnp.max(jnp.where(take > 0.5, partner, energy[r]))
    told = pltpu.make_async_copy(eout_ref, eout_hbm, eout_sem)
    told.start()
    for z in range(planes):
        for r in range(count):
            other, take, _ = plans[r]
            taking = mask(take, k)
            e = ((lane + (jnp.broadcast_to(orders[r], (k, width)) + (g * planes + z))) & 1) != 0
            for d in range(3):
                first, second = [
                    jnp.where(taking, other[i, d], evened[r, i, d]) for i in (z, planes + z)
                ]
                stage[r, d, z, pl.ds(0, k, stride=2), :] = jnp.where(e, second, first)
                stage[r, d, z, pl.ds(1, k, stride=2), :] = jnp.where(e, first, second)
            copy = pltpu.make_async_copy(
                stage.at[r, :, z], out_hbm.at[r, :, z], out_sem
            )
            copy.start()
    told.wait()
    pltpu.make_async_copy(stage, out_hbm, out_sem).wait()


def on_device(n, m, spin, coup, beta, order, level, height, angle, bits):
    count, _, planes, rows, width = spin.shape
    k = rows // 2
    f32 = jnp.float32
    hbm = pl.BlockSpec(memory_space=pltpu.HBM)
    vmem = pl.BlockSpec(memory_space=pltpu.VMEM)
    dma = pltpu.SemaphoreType.DMA
    bonds = pltpu.VMEM((2, count, planes, k, width), f32)
    dims = (count, planes, rows, width, n, m)
    handed = pl.pallas_call(
        functools.partial(sweep_kernel, dims),
        out_shape=(
            pltpu.VMEM((count, 2 * planes, 3, k, width), f32),
            pltpu.VMEM((2, 2 * planes, 3, k, width), f32),
            pltpu.VMEM((3, max(8, 2 * count), width), f32),
            pltpu.VMEM((3, n, count, width), f32),
        ),
        in_specs=[hbm] * 8,
        out_specs=(vmem,) * 4,
        scratch_shapes=[
            pltpu.VMEM(spin.shape, f32),
            pltpu.VMEM(coup.shape, f32),
            pltpu.VMEM(level.shape, f32),
            pltpu.VMEM(level.shape, f32),
            pltpu.VMEM(level.shape, f32),
            pltpu.VMEM((2, count, 3, k, width), f32),
            pltpu.VMEM((count, 2, 2, k, width), f32),
            pltpu.VMEM((count, 2, 2, k, width), f32),
            pltpu.VMEM((rows, width), f32),
            pltpu.VMEM((2, count, 3, planes + 2, k + 2 * PAD, width), f32),
            bonds,
            bonds,
            pltpu.VMEM((count, planes, k, width), f32),
            bonds,
            bonds,
            bonds,
            bonds,
            pltpu.VMEM((2, count, 3, planes, k, width), f32),
            pltpu.VMEM((count, 8, width), f32),
            pltpu.VMEM((2, max(8, 2 * count), width), f32),
            pltpu.SMEM((count,), f32),
            pltpu.SMEM((count,), jnp.int32),
            pltpu.SMEM((count,), jnp.int32),
            dma((2 * count + 4,)),
            dma((2, count)),
            dma((4, count, 2)),
            dma((3,)),
            dma((3,)),
            dma((2,)),
            dma((2,)),
            dma((2,)),
            dma((2, 2)),
            dma((4,)),
            pltpu.SemaphoreType.REGULAR,
        ],
        compiler_params=pltpu.CompilerParams(
            collective_id=0, has_side_effects=True, vmem_limit_bytes=58 * 1024 * 1024
        ),
    )(spin, coup, beta, order, level, height, angle, bits)
    return pl.pallas_call(
        functools.partial(finish_kernel, dims),
        out_shape=(
            jax.ShapeDtypeStruct(spin.shape, f32),
            jax.ShapeDtypeStruct((count,), f32),
        ),
        in_specs=[vmem] * 4,
        out_specs=(hbm, hbm),
        scratch_shapes=[
            pltpu.VMEM(spin.shape, f32),
            pltpu.SMEM((count,), f32),
            dma(()),
            dma(()),
        ],
        compiler_params=pltpu.CompilerParams(vmem_limit_bytes=16 * 1024 * 1024),
    )(*handed)


def solution(mesh):
    n, m = mesh.shape["gz"], mesh.shape["temp"]
    return jax.shard_map(
        functools.partial(on_device, n, m),
        mesh=mesh,
        in_specs=(
            P(("group", "temp"), None, "gz", None, None),
            P(None, ("group", "gz"), None, None),
            P(("group", "temp")),
            P(("group", "temp")),
            P(("group", "temp"), "gz", None, None),
            P(("group", "temp"), "gz", None, None),
            P(("group", "temp"), "gz", None, None),
            P(("group", "temp")),
        ),
        out_specs=(P(("group", "temp"), None, "gz", None, None), P(("group", "temp"))),
        check_vma=False,
    )
```

```python
import functools
import math

import jax
import jax.numpy as jnp
from jax import lax
from jax.experimental import pallas as pl
from jax.experimental.pallas import tpu as pltpu
from jax.sharding import PartitionSpec as P

OR_SWEEPS = 2
HALVES = 2 * OR_SWEEPS + 2
PAD = 8
MESH = pl.DeviceIdType.MESH
SIN_TERMS = [(-1.0) ** i / math.factorial(2 * i + 1) for i in range(8)]
COS_TERMS = [(-1.0) ** i / math.factorial(2 * i) for i in range(9)]


def horner(terms, value):
    total = jnp.full_like(value, terms[-1])
    for term in terms[-2::-1]:
        total = total * value + term
    return total


def cos_sin(angle):
    half = 0.5 * angle
    square = half * half
    sine = half * horner(SIN_TERMS, square)
    cosine = horner(COS_TERMS, square)
    return 1.0 - 2.0 * sine * sine, 2.0 * sine * cosine


def with_sign(size, like):
    return jnp.where(like < 0.0, -size, size)


def to_square(vector):
    a, b, c = vector
    inverse = 1.0 / (jnp.abs(a) + jnp.abs(b) + jnp.abs(c))
    p, q = a * inverse, b * inverse
    low = c < 0.0
    return (
        jnp.where(low, with_sign(1.0 - jnp.abs(q), p), p),
        jnp.where(low, with_sign(1.0 - jnp.abs(p), q), q),
    )


def from_square(p, q):
    c = 1.0 - jnp.abs(p) - jnp.abs(q)
    low = c < 0.0
    a = jnp.where(low, with_sign(1.0 - jnp.abs(q), p), p)
    b = jnp.where(low, with_sign(1.0 - jnp.abs(p), q), q)
    inverse = 1.0 / jnp.sqrt(a * a + b * b + c * c)
    return a * inverse, b * inverse, c * inverse


def dot3(a, b):
    return a[0] * b[0] + a[1] * b[1] + a[2] * b[2]


def reflect(current, pulled):
    factor = 2.0 * dot3(current, pulled) / jnp.maximum(dot3(pulled, pulled), 0.01)
    return [factor * p - s for p, s in zip(pulled, current)]


def heat_bath(pulled, beta, level, trial):
    strength = jnp.sqrt(jnp.maximum(dot3(pulled, pulled), 0.01))
    inverse = 1.0 / strength
    axis = [p * inverse for p in pulled]
    reach = beta * strength
    shrink = -jnp.tanh(reach) * (jnp.exp(-2.0 * reach) + 1.0)
    cosine = 1.0 + jnp.log1p(level * shrink) / reach
    along = dot3(trial, axis)
    tangent = [t - along * a for t, a in zip(trial, axis)]
    scale = jnp.sqrt(jnp.maximum(1.0 - cosine * cosine, 0.0)) * (
        1.0 / jnp.sqrt(jnp.maximum(dot3(tangent, tangent), 0.0001))
    )
    return [cosine * a + scale * t for a, t in zip(axis, tangent)]


def flag(bits_ref, j, size, width):
    return jnp.full((size, width), bits_ref[j], jnp.int32) != 0


def sweep_kernel(
    dims,
    spin_hbm,
    coup_hbm,
    beta_hbm,
    order_hbm,
    level_hbm,
    height_hbm,
    angle_hbm,
    bits_hbm,
    evened,
    rbuf,
    trecv,
    ebuf,
    spin_in,
    coup_in,
    level_in,
    height_in,
    angle_in,
    lifted,
    osend,
    orecv,
    cbelow,
    sp,
    xo,
    xr,
    yi,
    yo,
    zu,
    zd,
    lv,
    ut,
    eacc,
    tsend,
    beta_ref,
    order_ref,
    bits_ref,
    in_sem,
    hsend,
    hrecv,
    esend,
    erecv,
    tssem,
    trsem,
    xsend,
    xrecv,
    csem,
    wrap_sem,
):
    count, planes, rows, width, n, m = dims
    k = rows // 2
    chunk = 32 if k % 32 == 0 else 8
    last = planes - 1
    g = lax.axis_index("gz")
    t = lax.axis_index("temp")
    up, down = lax.rem(g + 1, n), lax.rem(g + n - 1, n)
    has_below, has_above = t > 0, t < m - 1
    near = 2 < n <= 2 * HALVES - 2

    first = 2 * count + 4
    loads = [
        pltpu.make_async_copy(src, dst, in_sem.at[i % first])
        for i, (src, dst) in enumerate(
            (
                (order_hbm, order_ref),
                (coup_hbm.at[2, last], coup_in.at[2, last]),
                *(
                    (spin_hbm.at[r, :, z], spin_in.at[r, :, z])
                    for r in range(count)
                    for z in (last, 0)
                ),
                (bits_hbm, bits_ref),
                (beta_hbm, beta_ref),
                (coup_hbm.at[pl.ds(0, 2)], coup_in.at[pl.ds(0, 2)]),
                (coup_hbm.at[2, pl.ds(0, last)], coup_in.at[2, pl.ds(0, last)]),
                (
                    spin_hbm.at[:, :, pl.ds(1, planes - 2)],
                    spin_in.at[:, :, pl.ds(1, planes - 2)],
                ),
                (level_hbm, level_in),
                (height_hbm, height_in),
                (angle_hbm, angle_in),
            )
        )
    ]

    def peer(dt, there):
        return {"gz": there} if dt == 0 else {"temp": t + dt, "gz": there}

    def along(dt, action):
        if dt == 0:
            action()
        else:
            pl.when(has_below if dt < 0 else has_above)(action)

    for load in loads[:first]:
        load.start()

    barrier = pltpu.get_barrier_semaphore()

    def greet(temp, there):
        target = {"temp": temp, "gz": there}
        pl.semaphore_signal(barrier, inc=1, device_id=target, device_id_type=MESH)

    if near:
        pl.when(g < n - 1)(lambda: greet(t, up))
        greet(t, down)
        for d in range(1, m):
            greet(lax.rem(t + d, m), g)
        expected = m - 1 + jnp.where(g == 0, 1, 2)
    else:
        for i in range(1, n * m):
            greet(lax.rem(t + i // n, m), lax.rem(g + i % n, n))
        expected = n * m - 1

    def parity(r, z, size):
        lane = lax.broadcasted_iota(jnp.int32, (size, width), 1)
        return ((lane + (g * planes + z + order_ref[r])) & 1) != 0

    def halves(ref, index, start, size):
        even = ref[index + (pl.ds(2 * start, size, stride=2), slice(None))]
        odd = ref[index + (pl.ds(2 * start + 1, size, stride=2), slice(None))]
        return even, odd

    def put_spin(c, r, d, z, start, value):
        size = value.shape[0]
        sp[c, r, d, z + 1, pl.ds(PAD + start, size), :] = value
        if start == 0:
            sp[c, r, d, z + 1, pl.ds(PAD + k, 1), :] = value[0:1]
        if start + size == k:
            sp[c, r, d, z + 1, pl.ds(PAD - 1, 1), :] = value[size - 1 : size]

    def pack_spin(r, z):
        e = parity(r, z, k)
        for d in range(3):
            even, odd = halves(spin_in, (r, d, z), 0, k)
            put_spin(0, r, d, z, 0, jnp.where(e, odd, even))
            put_spin(1, r, d, z, 0, jnp.where(e, even, odd))

    half, quarter = k // 2, k // 4

    def parts(x, r):
        if x < HALVES - 1 or quarter % 8 or r < count - 1:
            return [(0, k)]
        return [(0, half), (half, half + quarter), (half + quarter, k)]

    def halo(x, r, side, part=0):
        c = 1 - x % 2
        start, stop = parts(x, r)[part]
        size = stop - start
        plain = sp.at[c, r, :, 1, pl.ds(PAD + start, size), :]
        above = planes + 1 if side == 0 else 0
        return pltpu.make_async_remote_copy(
            src_ref=plain if side == 0 else lifted.at[c, r, :, pl.ds(start, size), :],
            dst_ref=sp.at[c, r, :, above, pl.ds(PAD + start, size), :],
            send_sem=hsend.at[x % 2, r],
            recv_sem=hrecv.at[part + 1 if part else x % 2, r if part == 0 else 0, side],
            device_id={"gz": down if side == 0 else up},
            device_id_type=MESH,
        )

    def opening(r, side):
        return pltpu.make_async_remote_copy(
            src_ref=osend.at[r, side],
            dst_ref=orecv.at[r, side],
            send_sem=hsend.at[0, r],
            recv_sem=hrecv.at[0, r, side],
            device_id={"gz": down if side == 0 else up},
            device_id_type=MESH,
        )

    shares_of = m if rows % (8 * m) == 0 else 1
    size_of = rows // shares_of
    stretch = pl.ds(pl.multiple_of(t * size_of, 8) if shares_of > 1 else 0, size_of)

    def across():
        return pltpu.make_async_remote_copy(
            src_ref=coup_in.at[2, last, stretch],
            dst_ref=cbelow.at[stretch],
            send_sem=csem.at[0],
            recv_sem=csem.at[1],
            device_id={"gz": up},
            device_id_type=MESH,
        )

    def pass_on(d):
        return pltpu.make_async_remote_copy(
            src_ref=cbelow.at[stretch],
            dst_ref=cbelow.at[stretch],
            send_sem=csem.at[2],
            recv_sem=csem.at[3],
            device_id={"temp": lax.rem(t + d, m)},
            device_id_type=MESH,
        )

    def passed_on(i):
        if shares_of > 1:
            ref = cbelow.at[pl.ds(0, (m - 1) * size_of)]
            pltpu.make_async_copy(ref, ref, csem.at[i]).wait()

    def sent(x, r):
        both = lifted.at[:, r] if x else osend.at[r]
        pltpu.make_async_copy(both, both, hsend.at[x % 2, r]).wait()

    def lift(c, r, d, start, value):
        part = pl.ds(start, value.shape[0])
        lifted[c, r, d, part, :] = zu[c, r, last, part, :] * value

    def inner(r, action):
        if planes > 2:
            lax.fori_loop(1, last, lambda z, carry: (action(r, z), carry)[1], 0)

    for load in loads[:4]:
        load.wait()
    for load in loads[first : first + 4]:
        load.start()

    def pack_edges(r):
        e = parity(r, last, k)
        even, odd = halves(coup_in, (2, last), 0, k)
        zu[0, r, last] = jnp.where(e, odd, even)
        zu[1, r, last] = jnp.where(e, even, odd)
        for side, z in ((1, last), (0, 0)):
            pack_spin(r, z)
            edge = to_square([sp[1, r, d, z + 1, pl.ds(PAD, k), :] for d in range(3)])
            osend[r, side, 0], osend[r, side, 1] = edge

    def slot_order(r):
        other = order_ref[r ^ 1]
        return jnp.where(bits_ref[r - r % 2] != 0, other, order_ref[r])

    def wide(value):
        return jnp.full((1, width), value, jnp.int32).astype(jnp.float32)

    for r in range(count):
        if r > 0:
            for load in loads[2 * r + 2 : 2 * r + 4]:
                load.wait()
        pack_edges(r)
        if r == 0:
            pl.semaphore_wait(barrier, expected)
            if near:

                @pl.when(g == n - 1)
                def _():
                    pl.semaphore_signal(wrap_sem, inc=1, device_id={"gz": up}, device_id_type=MESH)

            across().start()
        opening(r, 1).start()
        if near:
            pl.when(g > 0)(lambda: opening(r, 0).start())
        else:
            opening(r, 0).start()

    for load in loads[first - 2 : first]:
        load.wait()
    for load in loads[first + 4 :]:
        load.start()

    tsend[0, 0:1] = wide(slot_order(count - 1))
    tsend[0, 1:2] = wide(bits_ref[count - 1])
    tsend[0, 2:3] = wide(bits_ref[count - 2])
    tsend[1, 0:1] = wide(slot_order(0))
    tsend[1, 1:2] = wide(0)
    tsend[1, 2:3] = wide(bits_ref[0])
    for r in range(count):
        trecv[2, r : r + 1] = wide(slot_order(r))
        trecv[2, count + r : count + r + 1] = wide(bits_ref[r])

    def tell(side):
        return pltpu.make_async_remote_copy(
            src_ref=tsend.at[side],
            dst_ref=trecv.at[side],
            send_sem=tssem.at[side],
            recv_sem=trsem.at[side],
            device_id={"temp": t + 1 if side == 0 else t - 1},
            device_id_type=MESH,
        )

    along(1, lambda: tell(0).start())
    along(-1, lambda: tell(1).start())

    for load in loads[first : first + 3]:
        load.wait()

    def pack_bonds(i, carry):
        r, z = i // planes, i % planes
        e = parity(r, z, k)
        even, odd = halves(coup_in, (0, z), 0, k)
        first, second = jnp.where(e, odd, even), jnp.where(e, even, odd)
        xo[0, r, z] = first
        xo[1, r, z] = second
        xr[0, r, z] = pltpu.roll(second, 1, 1)
        xr[1, r, z] = pltpu.roll(first, 1, 1)
        even, odd = halves(coup_in, (1, z), 0, k)
        before = pltpu.roll(odd, 1, 0)
        yi[r, z] = even
        yo[0, r, z] = jnp.where(e, odd, before)
        yo[1, r, z] = jnp.where(e, before, odd)
        return carry

    def pack_lower(i, carry):
        r, z = i // last, 1 + i % last
        e = parity(r, z, k)
        even, odd = halves(coup_in, (2, z - 1), 0, k)
        zd[0, r, z] = jnp.where(e, odd, even)
        zd[1, r, z] = jnp.where(e, even, odd)
        zu[0, r, z - 1] = jnp.where(e, even, odd)
        zu[1, r, z - 1] = jnp.where(e, odd, even)
        return carry

    for r in range(count):
        inner(r, pack_spin)
    lax.fori_loop(0, count * planes, pack_bonds, 0)
    lax.fori_loop(0, count * last, pack_lower, 0)
    for r in range(count):
        for c in (0, 1):
            zd[c, r, 0] = jnp.ones((k, width), jnp.float32)

    if near:

        @pl.when(g == 0)
        def _():
            pl.semaphore_wait(wrap_sem, 1)
            for r in range(count):
                opening(r, 0).start()

    def pull(c, r, z, start, chunk=chunk):
        o = 1 - c
        part = pl.ds(start, chunk)
        e = parity(r, z, chunk)
        bx, br, by = xo[c, r, z, part, :], xr[c, r, z, part, :], yi[r, z, part, :]
        bo, bu, bd = yo[c, r, z, part, :], zu[c, r, z, part, :], zd[c, r, z, part, :]
        pulled = []
        for d in range(3):
            mid = sp[o, r, d, z + 1, pl.ds(PAD + start, chunk), :]
            nxt = sp[o, r, d, z + 1, pl.ds(PAD + start + 1, chunk), :]
            prv = sp[o, r, d, z + 1, pl.ds(PAD + start - 1, chunk), :]
            outer = jnp.where(e, nxt, prv) if c == 0 else jnp.where(e, prv, nxt)
            total = bx * pltpu.roll(mid, width - 1, 1) + br * pltpu.roll(mid, 1, 1)
            total = total + by * mid + bo * outer
            total = total + bu * sp[o, r, d, z + 2, pl.ds(PAD + start, chunk), :]
            total = total + bd * sp[o, r, d, z, pl.ds(PAD + start, chunk), :]
            pulled.append(total)
        return pulled

    def relax(c, r, z, lifting=False):
        for start in range(0, k, chunk):
            pulled = pull(c, r, z, start)
            current = [sp[c, r, d, z + 1, pl.ds(PAD + start, chunk), :] for d in range(3)]
            for d, value in enumerate(reflect(current, pulled)):
                put_spin(c, r, d, z, start, value)
                if lifting:
                    lift(c, r, d, start, value)

    def heat(c, r, z, lifting=False, rows_of=(0, k)):
        size = min(chunk, rows_of[1] - rows_of[0])
        for start in range(*rows_of, size):
            part = pl.ds(start, size)
            pulled = pull(c, r, z, start, size)
            trial = [ut[c, r, d, z, part, :] for d in range(3)]
            renewed = heat_bath(pulled, beta_ref[r], lv[c, r, z, part, :], trial)
            for d, value in enumerate(renewed):
                put_spin(c, r, d, z, start, value)
                if lifting:
                    lift(c, r, d, start, value)
            if c == 1:
                terms = dot3(renewed, pulled)
                eacc[r] = eacc[r] + sum(terms[j : j + 8] for j in range(0, size, 8))

    def pack_heat(r, z):
        for start in range(0, k, chunk):
            part = pl.ds(start, chunk)
            e = parity(r, z, chunk)
            even, odd = halves(level_in, (r, z), start, chunk)
            lv[0, r, z, part, :] = jnp.where(e, odd, even)
            lv[1, r, z, part, :] = jnp.where(e, even, odd)
            angles = halves(angle_in, (r, z), start, chunk)
            heights = halves(height_in, (r, z), start, chunk)
            trials = []
            for angle, height in zip(angles, heights):
                side = jnp.sqrt(jnp.maximum(1.0 - height * height, 0.0))
                cosine, sine = cos_sin(angle)
                trials.append((side * cosine, side * sine, height))
            for d in range(3):
                ut[0, r, d, z, part, :] = jnp.where(e, trials[1][d], trials[0][d])
                ut[1, r, d, z, part, :] = jnp.where(e, trials[0][d], trials[1][d])

    def take_halo(x, r, side):
        halo(x, r, 1 - side).wait_recv()
        if side == 0:
            sent(x - 1, r)

    def take_opening(r, side):
        opening(r, 1 - side).wait_recv()
        vector = from_square(orecv[r, 1 - side, 0], orecv[r, 1 - side, 1])
        if side == 0:
            even, odd = halves(cbelow, (), 0, k)
            bond = jnp.where(parity(r, 0, k), odd, even)
            vector = [bond * v for v in vector]
        for d in range(3):
            sp[1, r, d, planes + 1 if side else 0, pl.ds(PAD, k), :] = vector[d]

    def settle(c, z, start, stop):
        size = stop - start
        part, packed = pl.ds(start, size), pl.ds(PAD + start, size)
        for r in range(0, count, 2):
            taking = flag(bits_ref, r, size, width)
            for d in range(3):
                low = sp[c, r, d, z + 1, packed, :]
                top = sp[c, r + 1, d, z + 1, packed, :]
                evened[r, c * planes + z, d, part, :] = jnp.where(taking, top, low)
                evened[r + 1, c * planes + z, d, part, :] = jnp.where(taking, low, top)

    final = parts(HALVES - 1, count - 1)

    def pieces(c, z):
        return final if c == 1 and z in (0, last) else [(0, k)]

    def ship(c, z, side, part=0, many=1):
        start, stop = pieces(c, z)[part]
        rows_of = pl.ds(start, stop - start)
        here = pl.ds(c * planes + z, many)
        early = c == 0 and 0 < z < last
        return pltpu.make_async_remote_copy(
            src_ref=evened.at[count - 1 if side == 0 else 0, here, :, rows_of, :],
            dst_ref=rbuf.at[side, here, :, rows_of, :],
            send_sem=xsend.at[side],
            recv_sem=xrecv.at[0 if early else 1, side],
            device_id={"temp": t + 1 if side == 0 else t - 1},
            device_id_type=MESH,
        )

    def both_ways(action):
        along(1, lambda: action(0))
        along(-1, lambda: action(1))

    def send_off(c, z, part=0):
        settle(c, z, *pieces(c, z)[part])
        both_ways(lambda side: ship(c, z, side, part).start())

    def send_inner(c):
        for z in range(1, last):
            settle(c, z, 0, k)
        if planes > 2:
            both_ways(lambda side: ship(c, 1, side, many=planes - 2).start())

    def whole(side, size, sem):
        ref = rbuf.at[side, pl.ds(0, size)]
        pltpu.make_async_copy(ref, ref, sem).wait()

    def arrived(early):
        size = planes - 2 if early else planes + 2
        if size:
            both_ways(lambda side: whole(1 - side, size, xrecv.at[0 if early else 1, 1 - side]))

    def work(x):
        return functools.partial(relax if x < relaxing else heat, x % 2)

    ahead = g < n - 1
    eacc[...] = jnp.zeros_like(eacc)
    relaxing = 2 * OR_SWEEPS
    for r in range(count):
        inner(r, work(0))
    for load in loads[first + 3 :]:
        load.wait()
    across().wait_recv()
    if shares_of > 1:
        for d in range(1, m):
            pass_on(d).start()

    ends = (g == 0) | (g == n - 1)
    outer = jnp.where(g == n - 1, 0, 1)
    bonds_at = jnp.where(g == 0, count, jnp.where(g == n - 1, 0, 1))

    def first_step(i, carry):
        r = jnp.where(ends, lax.rem(i, count), i // 2)
        side = jnp.where(ends, jnp.where(i < count, outer, 1 - outer), 1 - lax.rem(i, 2))
        pl.when(i == bonds_at)(lambda: passed_on(3))

        @pl.when(side == 1)
        def _():
            take_opening(r, 1)
            work(0)(r, last, lifting=True)
            halo(1, r, 1).start()

        @pl.when(side == 0)
        def _():
            take_opening(r, 0)
            work(0)(r, 0)
            halo(1, r, 0).start()

        return carry

    lax.fori_loop(0, 2 * count, first_step, 0)
    for x in range(HALVES - 1):
        for r in range(count):
            for side, z in ((0, 0), (1, last)) if x else ():
                take_halo(x, r, side)
                work(x)(r, z, lifting=side == 1)
                if side == 0 and len(parts(x + 1, r)) == 1:
                    pl.when(ahead)(lambda: halo(x + 1, r, 0).start())
            for part in range(len(parts(x + 1, r)) if x else 0):
                if len(parts(x + 1, r)) > 1:
                    pl.when(ahead)(lambda: halo(x + 1, r, 0, part).start())
                halo(x + 1, r, 1, part).start()
                pl.when(~ahead)(lambda: halo(x + 1, r, 0, part).start())
            if r == count - 1 and x == relaxing:
                for z in (0, last):
                    send_off(0, z)
            for z in range(planes):
                if z % relaxing == x:
                    pack_heat(r, z)
            inner(r, work(x + 1))
        if x >= relaxing - 1:
            send_inner(x + 1 - relaxing)

    x = HALVES - 1
    for r in range(count):
        if r == count - 1:
            arrived(True)
            along(1, lambda: tell(1).wait_recv())
            along(-1, lambda: tell(0).wait_recv())
        for part, rows_of in enumerate(parts(x, r)):
            for side, z in ((0, 0), (1, last)):
                halo(x, r, 1 - side, part).wait_recv()
                if part == 0 and side == 0:
                    sent(x - 1, r)
                work(x)(r, z, rows_of=rows_of)
                if r == count - 1:
                    send_off(1, z, part)
    for r in range(count):
        ebuf[1, g, r : r + 1] = jnp.sum(eacc[r], axis=0, keepdims=True)

    def share(dt, source, there):
        return pltpu.make_async_remote_copy(
            src_ref=ebuf.at[1, source],
            dst_ref=ebuf.at[1 - dt, source],
            send_sem=esend.at[1 - dt],
            recv_sem=erecv.at[1 - dt],
            device_id=peer(dt, there),
            device_id_type=MESH,
        )

    def spread(dt):
        for d in range(1 if dt == 0 else 0, n):
            share(dt, g, lax.rem(g + d, n)).start()

    def shares(dt, sem):
        ref = ebuf.at[1, pl.ds(0, n - 1 if dt == 0 else n)]
        pltpu.make_async_copy(ref, ref, sem).wait()

    for dt in (0, 1, -1):
        along(dt, lambda dt=dt: spread(dt))
    for r in range(count):
        sent(x, r)
    across().wait_send()
    passed_on(2)
    along(1, lambda: tell(0).wait_send())
    along(-1, lambda: tell(1).wait_send())
    both_ways(lambda side: whole(side, 2 * planes, xsend.at[side]))
    arrived(False)
    for dt in (0, 1, -1):
        along(dt, lambda dt=dt: shares(dt, esend.at[1 - dt]))
        along(dt, lambda dt=dt: shares(dt, erecv.at[1 + dt]))


def finish_kernel(
    dims,
    evened,
    rbuf,
    trecv,
    ebuf,
    out_hbm,
    eout_hbm,
    stage,
    eout_ref,
    out_sem,
    eout_sem,
):
    count, planes, rows, width, n, m = dims
    k = rows // 2
    g = lax.axis_index("gz")
    t = lax.axis_index("temp")
    below, above = (t > 0).astype(jnp.int32), (t < m - 1).astype(jnp.int32)

    def number(side, row):
        return trecv[side, row : row + 1]

    def own_order(r):
        return number(2, r)

    def own_bit(r):
        return number(2, count + r)

    def mask(value, size):
        return jnp.broadcast_to(value, (size, width)) > 0.5

    def plan(r):
        if r == 0:
            met = jnp.full((1, width), below, jnp.int32) != 0
            return rbuf.at[0], jnp.where(met, number(0, 1), 0.0), jnp.where(met, number(0, 0), 0.0)
        if r == count - 1:
            met = jnp.full((1, width), above, jnp.int32) != 0
            return rbuf.at[1], jnp.where(met, own_bit(r), 0.0), jnp.where(met, number(1, 0), 0.0)
        other = r + 1 if r % 2 else r - 1
        return evened.at[other], own_bit(min(r, other)), own_order(other)

    lane = lax.broadcasted_iota(jnp.int32, (k, width), 1)
    plans = [plan(r) for r in range(count)]
    orders = [
        jnp.where(take > 0.5, order, own_order(r)).astype(jnp.int32)
        for r, (_, take, order) in enumerate(plans)
    ]
    sites = float(width * rows * planes * n)

    def total(slot, r):
        summed = ebuf[slot, 0, r : r + 1]
        for j in range(1, n):
            summed = summed + ebuf[slot, j, r : r + 1]
        return jnp.broadcast_to(jnp.sum(-summed, axis=1, keepdims=True) / sites, (1, width))

    energy = []
    for r in range(0, count, 2):
        taking = own_bit(r) > 0.5
        low, top = total(1, r), total(1, r + 1)
        energy += [jnp.where(taking, top, low), jnp.where(taking, low, top)]
    for r in range(count):
        other, take, _ = plans[r]
        if r == 0:
            swapped = number(0, 2) > 0.5
            partner = jnp.where(swapped, total(0, count - 2), total(0, count - 1))
        elif r == count - 1:
            swapped = number(1, 2) > 0.5
            partner = jnp.where(swapped, total(2, 1), total(2, 0))
        else:
            partner = energy[r + 1 if r % 2 else r - 1]
        eout_ref[r] = jnp.max(jnp.where(take > 0.5, partner, energy[r]))
    told = pltpu.make_async_copy(eout_ref, eout_hbm, eout_sem)
    told.start()
    for z in range(planes):
        for r in range(count):
            other, take, _ = plans[r]
            taking = mask(take, k)
            e = ((lane + (jnp.broadcast_to(orders[r], (k, width)) + (g * planes + z))) & 1) != 0
            for d in range(3):
                first, second = [
                    jnp.where(taking, other[i, d], evened[r, i, d]) for i in (z, planes + z)
                ]
                stage[r, d, z, pl.ds(0, k, stride=2), :] = jnp.where(e, second, first)
                stage[r, d, z, pl.ds(1, k, stride=2), :] = jnp.where(e, first, second)
            copy = pltpu.make_async_copy(
                stage.at[r, :, z], out_hbm.at[r, :, z], out_sem
            )
            copy.start()
    told.wait()
    pltpu.make_async_copy(stage, out_hbm, out_sem).wait()


def on_device(n, m, spin, coup, beta, order, level, height, angle, bits):
    count, _, planes, rows, width = spin.shape
    k = rows // 2
    f32 = jnp.float32
    hbm = pl.BlockSpec(memory_space=pltpu.HBM)
    vmem = pl.BlockSpec(memory_space=pltpu.VMEM)
    dma = pltpu.SemaphoreType.DMA
    bonds = pltpu.VMEM((2, count, planes, k, width), f32)
    dims = (count, planes, rows, width, n, m)
    handed = pl.pallas_call(
        functools.partial(sweep_kernel, dims),
        out_shape=(
            pltpu.VMEM((count, 2 * planes, 3, k, width), f32),
            pltpu.VMEM((2, 2 * planes, 3, k, width), f32),
            pltpu.VMEM((3, max(8, 2 * count), width), f32),
            pltpu.VMEM((3, n, count, width), f32),
        ),
        in_specs=[hbm] * 8,
        out_specs=(vmem,) * 4,
        scratch_shapes=[
            pltpu.VMEM(spin.shape, f32),
            pltpu.VMEM(coup.shape, f32),
            pltpu.VMEM(level.shape, f32),
            pltpu.VMEM(level.shape, f32),
            pltpu.VMEM(level.shape, f32),
            pltpu.VMEM((2, count, 3, k, width), f32),
            pltpu.VMEM((count, 2, 2, k, width), f32),
            pltpu.VMEM((count, 2, 2, k, width), f32),
            pltpu.VMEM((rows, width), f32),
            pltpu.VMEM((2, count, 3, planes + 2, k + 2 * PAD, width), f32),
            bonds,
            bonds,
            pltpu.VMEM((count, planes, k, width), f32),
            bonds,
            bonds,
            bonds,
            bonds,
            pltpu.VMEM((2, count, 3, planes, k, width), f32),
            pltpu.VMEM((count, 8, width), f32),
            pltpu.VMEM((2, max(8, 2 * count), width), f32),
            pltpu.SMEM((count,), f32),
            pltpu.SMEM((count,), jnp.int32),
            pltpu.SMEM((count,), jnp.int32),
            dma((2 * count + 4,)),
            dma((2, count)),
            dma((4, count, 2)),
            dma((3,)),
            dma((3,)),
            dma((2,)),
            dma((2,)),
            dma((2,)),
            dma((2, 2)),
            dma((4,)),
            pltpu.SemaphoreType.REGULAR,
        ],
        compiler_params=pltpu.CompilerParams(
            collective_id=0, has_side_effects=True, vmem_limit_bytes=58 * 1024 * 1024
        ),
    )(spin, coup, beta, order, level, height, angle, bits)
    return pl.pallas_call(
        functools.partial(finish_kernel, dims),
        out_shape=(
            jax.ShapeDtypeStruct(spin.shape, f32),
            jax.ShapeDtypeStruct((count,), f32),
        ),
        in_specs=[vmem] * 4,
        out_specs=(hbm, hbm),
        scratch_shapes=[
            pltpu.VMEM(spin.shape, f32),
            pltpu.SMEM((count,), f32),
            dma(()),
            dma(()),
        ],
        compiler_params=pltpu.CompilerParams(vmem_limit_bytes=16 * 1024 * 1024),
    )(*handed)


def solution(mesh):
    n, m = mesh.shape["gz"], mesh.shape["temp"]
    return jax.shard_map(
        functools.partial(on_device, n, m),
        mesh=mesh,
        in_specs=(
            P(("group", "temp"), None, "gz", None, None),
            P(None, ("group", "gz"), None, None),
            P(("group", "temp")),
            P(("group", "temp")),
            P(("group", "temp"), "gz", None, None),
            P(("group", "temp"), "gz", None, None),
            P(("group", "temp"), "gz", None, None),
            P(("group", "temp")),
        ),
        out_specs=(P(("group", "temp"), None, "gz", None, None), P(("group", "temp"))),
        check_vma=False,
    )
```

```python
import functools
import math

import jax
import jax.numpy as jnp
from jax import lax
from jax.experimental import pallas as pl
from jax.experimental.pallas import tpu as pltpu
from jax.sharding import PartitionSpec as P

OR_SWEEPS = 2
HALVES = 2 * OR_SWEEPS + 2
PAD = 8
MESH = pl.DeviceIdType.MESH
SIN_TERMS = [(-1.0) ** i / math.factorial(2 * i + 1) for i in range(8)]
COS_TERMS = [(-1.0) ** i / math.factorial(2 * i) for i in range(9)]


def horner(terms, value):
    total = jnp.full_like(value, terms[-1])
    for term in terms[-2::-1]:
        total = total * value + term
    return total


def cos_sin(angle):
    half = 0.5 * angle
    square = half * half
    sine = half * horner(SIN_TERMS, square)
    cosine = horner(COS_TERMS, square)
    return 1.0 - 2.0 * sine * sine, 2.0 * sine * cosine


def with_sign(size, like):
    return jnp.where(like < 0.0, -size, size)


def to_square(vector):
    a, b, c = vector
    inverse = 1.0 / (jnp.abs(a) + jnp.abs(b) + jnp.abs(c))
    p, q = a * inverse, b * inverse
    low = c < 0.0
    return (
        jnp.where(low, with_sign(1.0 - jnp.abs(q), p), p),
        jnp.where(low, with_sign(1.0 - jnp.abs(p), q), q),
    )


def from_square(p, q):
    c = 1.0 - jnp.abs(p) - jnp.abs(q)
    low = c < 0.0
    a = jnp.where(low, with_sign(1.0 - jnp.abs(q), p), p)
    b = jnp.where(low, with_sign(1.0 - jnp.abs(p), q), q)
    inverse = 1.0 / jnp.sqrt(a * a + b * b + c * c)
    return a * inverse, b * inverse, c * inverse


def dot3(a, b):
    return a[0] * b[0] + a[1] * b[1] + a[2] * b[2]


def reflect(current, pulled):
    factor = 2.0 * dot3(current, pulled) / jnp.maximum(dot3(pulled, pulled), 0.01)
    return [factor * p - s for p, s in zip(pulled, current)]


def heat_bath(pulled, beta, level, trial):
    strength = jnp.sqrt(jnp.maximum(dot3(pulled, pulled), 0.01))
    inverse = 1.0 / strength
    axis = [p * inverse for p in pulled]
    reach = beta * strength
    shrink = -jnp.tanh(reach) * (jnp.exp(-2.0 * reach) + 1.0)
    cosine = 1.0 + jnp.log1p(level * shrink) / reach
    along = dot3(trial, axis)
    tangent = [t - along * a for t, a in zip(trial, axis)]
    scale = jnp.sqrt(jnp.maximum(1.0 - cosine * cosine, 0.0)) * (
        1.0 / jnp.sqrt(jnp.maximum(dot3(tangent, tangent), 0.0001))
    )
    return [cosine * a + scale * t for a, t in zip(axis, tangent)]


def flag(bits_ref, j, size, width):
    return jnp.full((size, width), bits_ref[j], jnp.int32) != 0


def sweep_kernel(
    dims,
    spin_hbm,
    coup_hbm,
    beta_hbm,
    order_hbm,
    level_hbm,
    height_hbm,
    angle_hbm,
    bits_hbm,
    evened,
    rbuf,
    trecv,
    ebuf,
    spin_in,
    coup_in,
    level_in,
    height_in,
    angle_in,
    lifted,
    osend,
    orecv,
    cbelow,
    sp,
    xo,
    xr,
    yi,
    yo,
    zu,
    zd,
    lv,
    ut,
    eacc,
    tsend,
    beta_ref,
    order_ref,
    bits_ref,
    in_sem,
    hsend,
    hrecv,
    esend,
    erecv,
    tssem,
    trsem,
    xsend,
    xrecv,
    csem,
    wrap_sem,
    temp_sem,
):
    count, planes, rows, width, n, m = dims
    k = rows // 2
    chunk = 32 if k % 32 == 0 else 8
    last = planes - 1
    g = lax.axis_index("gz")
    t = lax.axis_index("temp")
    up, down = lax.rem(g + 1, n), lax.rem(g + n - 1, n)
    has_below, has_above = t > 0, t < m - 1
    near = 2 < n <= 2 * HALVES - 2

    first = 2 * count + 4
    loads = [
        pltpu.make_async_copy(src, dst, in_sem.at[i % first])
        for i, (src, dst) in enumerate(
            (
                (order_hbm, order_ref),
                (coup_hbm.at[2, last], coup_in.at[2, last]),
                *(
                    (spin_hbm.at[r, :, z], spin_in.at[r, :, z])
                    for r in range(count)
                    for z in (last, 0)
                ),
                (bits_hbm, bits_ref),
                (beta_hbm, beta_ref),
                (coup_hbm.at[pl.ds(0, 2)], coup_in.at[pl.ds(0, 2)]),
                (coup_hbm.at[2, pl.ds(0, last)], coup_in.at[2, pl.ds(0, last)]),
                (
                    spin_hbm.at[:, :, pl.ds(1, planes - 2)],
                    spin_in.at[:, :, pl.ds(1, planes - 2)],
                ),
                (level_hbm, level_in),
                (height_hbm, height_in),
                (angle_hbm, angle_in),
            )
        )
    ]

    def peer(dt, there):
        return {"gz": there} if dt == 0 else {"temp": t + dt, "gz": there}

    def along(dt, action):
        if dt == 0:
            action()
        else:
            pl.when(has_below if dt < 0 else has_above)(action)

    for load in loads[:first]:
        load.start()

    barrier = pltpu.get_barrier_semaphore()

    def greet(temp, there):
        target = {"temp": temp, "gz": there}
        pl.semaphore_signal(barrier, inc=1, device_id=target, device_id_type=MESH)

    if near:
        pl.when(g < n - 1)(lambda: greet(t, up))
        greet(t, down)
        for d in range(1, m):
            pl.when(t + d < m)(lambda: greet(t + d, g))
        expected = t + jnp.where(g == 0, 1, 2)
    else:
        for i in range(1, n * m):
            greet(lax.rem(t + i // n, m), lax.rem(g + i % n, n))
        expected = n * m - 1

    def parity(r, z, size):
        lane = lax.broadcasted_iota(jnp.int32, (size, width), 1)
        return ((lane + (g * planes + z + order_ref[r])) & 1) != 0

    def halves(ref, index, start, size):
        even = ref[index + (pl.ds(2 * start, size, stride=2), slice(None))]
        odd = ref[index + (pl.ds(2 * start + 1, size, stride=2), slice(None))]
        return even, odd

    def put_spin(c, r, d, z, start, value):
        size = value.shape[0]
        sp[c, r, d, z + 1, pl.ds(PAD + start, size), :] = value
        if start == 0:
            sp[c, r, d, z + 1, pl.ds(PAD + k, 1), :] = value[0:1]
        if start + size == k:
            sp[c, r, d, z + 1, pl.ds(PAD - 1, 1), :] = value[size - 1 : size]

    def pack_spin(r, z):
        e = parity(r, z, k)
        for d in range(3):
            even, odd = halves(spin_in, (r, d, z), 0, k)
            put_spin(0, r, d, z, 0, jnp.where(e, odd, even))
            put_spin(1, r, d, z, 0, jnp.where(e, even, odd))

    half, quarter = k // 2, k // 4

    def parts(x, r):
        if x < HALVES - 1 or r < count - 1 or quarter % 8:
            return [(0, k)]
        return [(0, half), (half, half + quarter), (half + quarter, k)]

    def halo(x, r, side, part=0):
        c = 1 - x % 2
        start, stop = parts(x, r)[part]
        size = stop - start
        plain = sp.at[c, r, :, 1, pl.ds(PAD + start, size), :]
        above = planes + 1 if side == 0 else 0
        return pltpu.make_async_remote_copy(
            src_ref=plain if side == 0 else lifted.at[c, r, :, pl.ds(start, size), :],
            dst_ref=sp.at[c, r, :, above, pl.ds(PAD + start, size), :],
            send_sem=hsend.at[x % 2, r],
            recv_sem=hrecv.at[part + 1 if part else x % 2, r if part == 0 else 0, side],
            device_id={"gz": down if side == 0 else up},
            device_id_type=MESH,
        )

    def opening(r, side):
        return pltpu.make_async_remote_copy(
            src_ref=osend.at[r, side],
            dst_ref=orecv.at[r, side],
            send_sem=hsend.at[0, r],
            recv_sem=hrecv.at[0, r, side],
            device_id={"gz": down if side == 0 else up},
            device_id_type=MESH,
        )

    shares_of = m if rows % (8 * m) == 0 else 1
    size_of = rows // shares_of
    stretch = pl.ds(pl.multiple_of(t * size_of, 8) if shares_of > 1 else 0, size_of)

    def across():
        return pltpu.make_async_remote_copy(
            src_ref=coup_in.at[2, last, stretch],
            dst_ref=cbelow.at[stretch],
            send_sem=csem.at[0],
            recv_sem=csem.at[1],
            device_id={"gz": up},
            device_id_type=MESH,
        )

    def pass_on(d):
        return pltpu.make_async_remote_copy(
            src_ref=cbelow.at[stretch],
            dst_ref=cbelow.at[stretch],
            send_sem=csem.at[2],
            recv_sem=csem.at[3],
            device_id={"temp": lax.rem(t + d, m)},
            device_id_type=MESH,
        )

    def passed_on(i):
        if shares_of > 1:
            ref = cbelow.at[pl.ds(0, (m - 1) * size_of)]
            pltpu.make_async_copy(ref, ref, csem.at[i]).wait()

    def sent(x, r):
        both = lifted.at[:, r] if x else osend.at[r]
        pltpu.make_async_copy(both, both, hsend.at[x % 2, r]).wait()

    def lift(c, r, d, start, value):
        part = pl.ds(start, value.shape[0])
        lifted[c, r, d, part, :] = zu[c, r, last, part, :] * value

    def inner(r, action):
        if planes > 2:
            lax.fori_loop(1, last, lambda z, carry: (action(r, z), carry)[1], 0)

    def ready():
        pl.semaphore_wait(barrier, expected)

    if near:

        @pl.when(g == n - 1)
        def _():
            ready()
            pl.semaphore_signal(wrap_sem, inc=1, device_id={"gz": up}, device_id_type=MESH)

    for load in loads[:4]:
        load.wait()
    if near:
        pl.when(g == n - 1)(lambda: across().start())
    for load in loads[first : first + 4]:
        load.start()

    def pack_edges(r):
        e = parity(r, last, k)
        even, odd = halves(coup_in, (2, last), 0, k)
        zu[0, r, last] = jnp.where(e, odd, even)
        zu[1, r, last] = jnp.where(e, even, odd)
        for side, z in ((1, last), (0, 0)):
            pack_spin(r, z)
            edge = to_square([sp[1, r, d, z + 1, pl.ds(PAD, k), :] for d in range(3)])
            osend[r, side, 0], osend[r, side, 1] = edge

    def slot_order(r):
        other = order_ref[r ^ 1]
        return jnp.where(bits_ref[r - r % 2] != 0, other, order_ref[r])

    def wide(value):
        return jnp.full((1, width), value, jnp.int32).astype(jnp.float32)

    for r in range(count):
        if r > 0:
            for load in loads[2 * r + 2 : 2 * r + 4]:
                load.wait()
        pack_edges(r)
        if r == 0:
            if near:

                @pl.when(g < n - 1)
                def _():
                    ready()
                    across().start()

            else:
                ready()
                across().start()
        opening(r, 1).start()
        if near:
            pl.when(g > 0)(lambda: opening(r, 0).start())
        else:
            opening(r, 0).start()

    for load in loads[first - 2 : first]:
        load.wait()
    for load in loads[first + 4 :]:
        load.start()

    tsend[0, 0:1] = wide(slot_order(count - 1))
    tsend[0, 1:2] = wide(bits_ref[count - 1])
    tsend[0, 2:3] = wide(bits_ref[count - 2])
    tsend[1, 0:1] = wide(slot_order(0))
    tsend[1, 1:2] = wide(0)
    tsend[1, 2:3] = wide(bits_ref[0])
    for r in range(count):
        trecv[2, r : r + 1] = wide(slot_order(r))
        trecv[2, count + r : count + r + 1] = wide(bits_ref[r])

    def tell(side):
        return pltpu.make_async_remote_copy(
            src_ref=tsend.at[side],
            dst_ref=trecv.at[side],
            send_sem=tssem.at[side],
            recv_sem=trsem.at[side],
            device_id={"temp": t + 1 if side == 0 else t - 1},
            device_id_type=MESH,
        )

    if near:
        for d in range(1, m):

            @pl.when(t >= d)
            def _():
                target = {"temp": t - d, "gz": g}
                pl.semaphore_signal(temp_sem, inc=1, device_id=target, device_id_type=MESH)


    for load in loads[first : first + 3]:
        load.wait()

    def pack_bonds(i, carry):
        r, z = i // planes, i % planes
        e = parity(r, z, k)
        even, odd = halves(coup_in, (0, z), 0, k)
        first, second = jnp.where(e, odd, even), jnp.where(e, even, odd)
        xo[0, r, z] = first
        xo[1, r, z] = second
        xr[0, r, z] = pltpu.roll(second, 1, 1)
        xr[1, r, z] = pltpu.roll(first, 1, 1)
        even, odd = halves(coup_in, (1, z), 0, k)
        before = pltpu.roll(odd, 1, 0)
        yi[r, z] = even
        yo[0, r, z] = jnp.where(e, odd, before)
        yo[1, r, z] = jnp.where(e, before, odd)
        return carry

    def pack_lower(i, carry):
        r, z = i // last, 1 + i % last
        e = parity(r, z, k)
        even, odd = halves(coup_in, (2, z - 1), 0, k)
        zd[0, r, z] = jnp.where(e, odd, even)
        zd[1, r, z] = jnp.where(e, even, odd)
        zu[0, r, z - 1] = jnp.where(e, even, odd)
        zu[1, r, z - 1] = jnp.where(e, odd, even)
        return carry

    for r in range(count):
        inner(r, pack_spin)
    lax.fori_loop(0, count * planes, pack_bonds, 0)
    lax.fori_loop(0, count * last, pack_lower, 0)
    for r in range(count):
        for c in (0, 1):
            zd[c, r, 0] = jnp.ones((k, width), jnp.float32)

    if near:

        @pl.when(g == 0)
        def _():
            pl.semaphore_wait(wrap_sem, 1)
            for r in range(count):
                opening(r, 0).start()

    def pull(c, r, z, start, chunk=chunk):
        o = 1 - c
        part = pl.ds(start, chunk)
        e = parity(r, z, chunk)
        bx, br, by = xo[c, r, z, part, :], xr[c, r, z, part, :], yi[r, z, part, :]
        bo, bu, bd = yo[c, r, z, part, :], zu[c, r, z, part, :], zd[c, r, z, part, :]
        pulled = []
        for d in range(3):
            mid = sp[o, r, d, z + 1, pl.ds(PAD + start, chunk), :]
            nxt = sp[o, r, d, z + 1, pl.ds(PAD + start + 1, chunk), :]
            prv = sp[o, r, d, z + 1, pl.ds(PAD + start - 1, chunk), :]
            outer = jnp.where(e, nxt, prv) if c == 0 else jnp.where(e, prv, nxt)
            total = bx * pltpu.roll(mid, width - 1, 1) + br * pltpu.roll(mid, 1, 1)
            total = total + by * mid + bo * outer
            total = total + bu * sp[o, r, d, z + 2, pl.ds(PAD + start, chunk), :]
            total = total + bd * sp[o, r, d, z, pl.ds(PAD + start, chunk), :]
            pulled.append(total)
        return pulled

    def relax(c, r, z, lifting=False):
        for start in range(0, k, chunk):
            pulled = pull(c, r, z, start)
            current = [sp[c, r, d, z + 1, pl.ds(PAD + start, chunk), :] for d in range(3)]
            for d, value in enumerate(reflect(current, pulled)):
                put_spin(c, r, d, z, start, value)
                if lifting:
                    lift(c, r, d, start, value)

    def heat(c, r, z, lifting=False, rows_of=(0, k)):
        size = min(chunk, rows_of[1] - rows_of[0])
        for start in range(*rows_of, size):
            part = pl.ds(start, size)
            pulled = pull(c, r, z, start, size)
            trial = [ut[c, r, d, z, part, :] for d in range(3)]
            renewed = heat_bath(pulled, beta_ref[r], lv[c, r, z, part, :], trial)
            for d, value in enumerate(renewed):
                put_spin(c, r, d, z, start, value)
                if lifting:
                    lift(c, r, d, start, value)
            if c == 1:
                terms = dot3(renewed, pulled)
                eacc[r] = eacc[r] + sum(terms[j : j + 8] for j in range(0, size, 8))

    def pack_heat(r, z):
        for start in range(0, k, chunk):
            part = pl.ds(start, chunk)
            e = parity(r, z, chunk)
            even, odd = halves(level_in, (r, z), start, chunk)
            lv[0, r, z, part, :] = jnp.where(e, odd, even)
            lv[1, r, z, part, :] = jnp.where(e, even, odd)
            angles = halves(angle_in, (r, z), start, chunk)
            heights = halves(height_in, (r, z), start, chunk)
            trials = []
            for angle, height in zip(angles, heights):
                side = jnp.sqrt(jnp.maximum(1.0 - height * height, 0.0))
                cosine, sine = cos_sin(angle)
                trials.append((side * cosine, side * sine, height))
            for d in range(3):
                ut[0, r, d, z, part, :] = jnp.where(e, trials[1][d], trials[0][d])
                ut[1, r, d, z, part, :] = jnp.where(e, trials[0][d], trials[1][d])

    def take_halo(x, r, side):
        halo(x, r, 1 - side).wait_recv()
        if side == 0:
            sent(x - 1, r)

    def take_opening(r, side):
        opening(r, 1 - side).wait_recv()
        vector = from_square(orecv[r, 1 - side, 0], orecv[r, 1 - side, 1])
        if side == 0:
            even, odd = halves(cbelow, (), 0, k)
            bond = jnp.where(parity(r, 0, k), odd, even)
            vector = [bond * v for v in vector]
        for d in range(3):
            sp[1, r, d, planes + 1 if side else 0, pl.ds(PAD, k), :] = vector[d]

    def settle(c, z, start, stop):
        size = stop - start
        part, packed = pl.ds(start, size), pl.ds(PAD + start, size)
        for r in range(0, count, 2):
            taking = flag(bits_ref, r, size, width)
            for d in range(3):
                low = sp[c, r, d, z + 1, packed, :]
                top = sp[c, r + 1, d, z + 1, packed, :]
                evened[r, c * planes + z, d, part, :] = jnp.where(taking, top, low)
                evened[r + 1, c * planes + z, d, part, :] = jnp.where(taking, low, top)

    final = parts(HALVES - 1, count - 1)

    def pieces(c, z):
        return final if c == 1 and z in (0, last) else [(0, k)]

    def ship(c, z, side, part=0, many=1):
        start, stop = pieces(c, z)[part]
        rows_of = pl.ds(start, stop - start)
        here = pl.ds(c * planes + z, many)
        early = c == 0 and 0 < z < last
        return pltpu.make_async_remote_copy(
            src_ref=evened.at[count - 1 if side == 0 else 0, here, :, rows_of, :],
            dst_ref=rbuf.at[side, here, :, rows_of, :],
            send_sem=xsend.at[side],
            recv_sem=xrecv.at[0 if early else 1, side],
            device_id={"temp": t + 1 if side == 0 else t - 1},
            device_id_type=MESH,
        )

    def both_ways(action):
        along(1, lambda: action(0))
        along(-1, lambda: action(1))

    def send_off(c, z, part=0):
        settle(c, z, *pieces(c, z)[part])
        both_ways(lambda side: ship(c, z, side, part).start())

    def send_inner(c):
        for z in range(1, last):
            settle(c, z, 0, k)
        if planes > 2:
            both_ways(lambda side: ship(c, 1, side, many=planes - 2).start())

    def whole(side, size, sem):
        ref = rbuf.at[side, pl.ds(0, size)]
        pltpu.make_async_copy(ref, ref, sem).wait()

    def arrived(early):
        size = planes - 2 if early else planes + 2
        if size:
            both_ways(lambda side: whole(1 - side, size, xrecv.at[0 if early else 1, 1 - side]))

    def work(x):
        return functools.partial(relax if x < relaxing else heat, x % 2)

    ahead = g < n - 1
    eacc[...] = jnp.zeros_like(eacc)
    relaxing = 2 * OR_SWEEPS
    for r in range(count):
        inner(r, work(0))
    for load in loads[first + 3 :]:
        load.wait()
    if near:
        along(1, lambda: pl.semaphore_wait(temp_sem, m - 1 - t))
    along(1, lambda: tell(0).start())
    along(-1, lambda: tell(1).start())
    across().wait_recv()
    if shares_of > 1:
        for d in range(1, m):
            pass_on(d).start()
    for x in range(HALVES - 1):
        for r in range(count):
            for side, z in ((0, 0), (1, last)) if x else ((1, last), (0, 0)):
                if x:
                    take_halo(x, r, side)
                else:
                    if r == 0 and side == 0:
                        passed_on(3)
                    take_opening(r, side)
                work(x)(r, z, lifting=side == 1)
                if x == 0:
                    halo(1, r, side).start()
                elif side == 0 and len(parts(x + 1, r)) == 1:
                    pl.when(ahead)(lambda: halo(x + 1, r, 0).start())
            for part in range(len(parts(x + 1, r)) if x else 0):
                if len(parts(x + 1, r)) > 1:
                    pl.when(ahead)(lambda: halo(x + 1, r, 0, part).start())
                halo(x + 1, r, 1, part).start()
                pl.when(~ahead)(lambda: halo(x + 1, r, 0, part).start())
            if r == count - 1 and x == relaxing:
                for z in (0, last):
                    send_off(0, z)
            for z in range(planes):
                if z % relaxing == x:
                    pack_heat(r, z)
            inner(r, work(x + 1))
        if x >= relaxing - 1:
            send_inner(x + 1 - relaxing)

    x = HALVES - 1
    for r in range(count):
        if r == count - 1:
            arrived(True)
            along(1, lambda: tell(1).wait_recv())
            along(-1, lambda: tell(0).wait_recv())
        for part, rows_of in enumerate(parts(x, r)):
            for side, z in ((0, 0), (1, last)):
                halo(x, r, 1 - side, part).wait_recv()
                if part == 0 and side == 0:
                    sent(x - 1, r)
                work(x)(r, z, rows_of=rows_of)
                if r == count - 1:
                    send_off(1, z, part)
    for r in range(count):
        ebuf[1, g, r : r + 1] = jnp.sum(eacc[r], axis=0, keepdims=True)

    def share(dt, source, there):
        return pltpu.make_async_remote_copy(
            src_ref=ebuf.at[1, source],
            dst_ref=ebuf.at[1 - dt, source],
            send_sem=esend.at[1 - dt],
            recv_sem=erecv.at[1 - dt],
            device_id=peer(dt, there),
            device_id_type=MESH,
        )

    def spread(dt):
        for d in range(1 if dt == 0 else 0, n):
            share(dt, g, lax.rem(g + d, n)).start()

    def shares(dt, sem):
        ref = ebuf.at[1, pl.ds(0, n - 1 if dt == 0 else n)]
        pltpu.make_async_copy(ref, ref, sem).wait()

    for dt in (0, 1, -1):
        along(dt, lambda dt=dt: spread(dt))
    for r in range(count):
        sent(x, r)
    across().wait_send()
    passed_on(2)
    along(1, lambda: tell(0).wait_send())
    along(-1, lambda: tell(1).wait_send())
    both_ways(lambda side: whole(side, 2 * planes, xsend.at[side]))
    arrived(False)
    for dt in (0, 1, -1):
        along(dt, lambda dt=dt: shares(dt, esend.at[1 - dt]))
        along(dt, lambda dt=dt: shares(dt, erecv.at[1 + dt]))


def finish_kernel(
    dims,
    evened,
    rbuf,
    trecv,
    ebuf,
    out_hbm,
    eout_hbm,
    stage,
    eout_ref,
    out_sem,
    eout_sem,
):
    count, planes, rows, width, n, m = dims
    k = rows // 2
    g = lax.axis_index("gz")
    t = lax.axis_index("temp")
    below, above = (t > 0).astype(jnp.int32), (t < m - 1).astype(jnp.int32)

    def number(side, row):
        return trecv[side, row : row + 1]

    def own_order(r):
        return number(2, r)

    def own_bit(r):
        return number(2, count + r)

    def mask(value, size):
        return jnp.broadcast_to(value, (size, width)) > 0.5

    def plan(r):
        if r == 0:
            met = jnp.full((1, width), below, jnp.int32) != 0
            return rbuf.at[0], jnp.where(met, number(0, 1), 0.0), jnp.where(met, number(0, 0), 0.0)
        if r == count - 1:
            met = jnp.full((1, width), above, jnp.int32) != 0
            return rbuf.at[1], jnp.where(met, own_bit(r), 0.0), jnp.where(met, number(1, 0), 0.0)
        other = r + 1 if r % 2 else r - 1
        return evened.at[other], own_bit(min(r, other)), own_order(other)

    lane = lax.broadcasted_iota(jnp.int32, (k, width), 1)
    plans = [plan(r) for r in range(count)]
    orders = [
        jnp.where(take > 0.5, order, own_order(r)).astype(jnp.int32)
        for r, (_, take, order) in enumerate(plans)
    ]
    sites = float(width * rows * planes * n)

    def total(slot, r):
        summed = ebuf[slot, 0, r : r + 1]
        for j in range(1, n):
            summed = summed + ebuf[slot, j, r : r + 1]
        return jnp.broadcast_to(jnp.sum(-summed, axis=1, keepdims=True) / sites, (1, width))

    energy = []
    for r in range(0, count, 2):
        taking = own_bit(r) > 0.5
        low, top = total(1, r), total(1, r + 1)
        energy += [jnp.where(taking, top, low), jnp.where(taking, low, top)]
    for r in range(count):
        other, take, _ = plans[r]
        if r == 0:
            swapped = number(0, 2) > 0.5
            partner = jnp.where(swapped, total(0, count - 2), total(0, count - 1))
        elif r == count - 1:
            swapped = number(1, 2) > 0.5
            partner = jnp.where(swapped, total(2, 1), total(2, 0))
        else:
            partner = energy[r + 1 if r % 2 else r - 1]
        eout_ref[r] = jnp.max(jnp.where(take > 0.5, partner, energy[r]))
    told = pltpu.make_async_copy(eout_ref, eout_hbm, eout_sem)
    told.start()
    for z in range(planes):
        for r in range(count):
            other, take, _ = plans[r]
            taking = mask(take, k)
            e = ((lane + (jnp.broadcast_to(orders[r], (k, width)) + (g * planes + z))) & 1) != 0
            for d in range(3):
                first, second = [
                    jnp.where(taking, other[i, d], evened[r, i, d]) for i in (z, planes + z)
                ]
                stage[r, d, z, pl.ds(0, k, stride=2), :] = jnp.where(e, second, first)
                stage[r, d, z, pl.ds(1, k, stride=2), :] = jnp.where(e, first, second)
            copy = pltpu.make_async_copy(
                stage.at[r, :, z], out_hbm.at[r, :, z], out_sem
            )
            copy.start()
    told.wait()
    pltpu.make_async_copy(stage, out_hbm, out_sem).wait()


def on_device(n, m, spin, coup, beta, order, level, height, angle, bits):
    count, _, planes, rows, width = spin.shape
    k = rows // 2
    f32 = jnp.float32
    hbm = pl.BlockSpec(memory_space=pltpu.HBM)
    vmem = pl.BlockSpec(memory_space=pltpu.VMEM)
    dma = pltpu.SemaphoreType.DMA
    bonds = pltpu.VMEM((2, count, planes, k, width), f32)
    dims = (count, planes, rows, width, n, m)
    handed = pl.pallas_call(
        functools.partial(sweep_kernel, dims),
        out_shape=(
            pltpu.VMEM((count, 2 * planes, 3, k, width), f32),
            pltpu.VMEM((2, 2 * planes, 3, k, width), f32),
            pltpu.VMEM((3, max(8, 2 * count), width), f32),
            pltpu.VMEM((3, n, count, width), f32),
        ),
        in_specs=[hbm] * 8,
        out_specs=(vmem,) * 4,
        scratch_shapes=[
            pltpu.VMEM(spin.shape, f32),
            pltpu.VMEM(coup.shape, f32),
            pltpu.VMEM(level.shape, f32),
            pltpu.VMEM(level.shape, f32),
            pltpu.VMEM(level.shape, f32),
            pltpu.VMEM((2, count, 3, k, width), f32),
            pltpu.VMEM((count, 2, 2, k, width), f32),
            pltpu.VMEM((count, 2, 2, k, width), f32),
            pltpu.VMEM((rows, width), f32),
            pltpu.VMEM((2, count, 3, planes + 2, k + 2 * PAD, width), f32),
            bonds,
            bonds,
            pltpu.VMEM((count, planes, k, width), f32),
            bonds,
            bonds,
            bonds,
            bonds,
            pltpu.VMEM((2, count, 3, planes, k, width), f32),
            pltpu.VMEM((count, 8, width), f32),
            pltpu.VMEM((2, max(8, 2 * count), width), f32),
            pltpu.SMEM((count,), f32),
            pltpu.SMEM((count,), jnp.int32),
            pltpu.SMEM((count,), jnp.int32),
            dma((2 * count + 4,)),
            dma((2, count)),
            dma((4, count, 2)),
            dma((3,)),
            dma((3,)),
            dma((2,)),
            dma((2,)),
            dma((2,)),
            dma((2, 2)),
            dma((4,)),
            pltpu.SemaphoreType.REGULAR,
            pltpu.SemaphoreType.REGULAR,
        ],
        compiler_params=pltpu.CompilerParams(
            collective_id=0, has_side_effects=True, vmem_limit_bytes=58 * 1024 * 1024
        ),
    )(spin, coup, beta, order, level, height, angle, bits)
    return pl.pallas_call(
        functools.partial(finish_kernel, dims),
        out_shape=(
            jax.ShapeDtypeStruct(spin.shape, f32),
            jax.ShapeDtypeStruct((count,), f32),
        ),
        in_specs=[vmem] * 4,
        out_specs=(hbm, hbm),
        scratch_shapes=[
            pltpu.VMEM(spin.shape, f32),
            pltpu.SMEM((count,), f32),
            dma(()),
            dma(()),
        ],
        compiler_params=pltpu.CompilerParams(vmem_limit_bytes=16 * 1024 * 1024),
    )(*handed)


def solution(mesh):
    n, m = mesh.shape["gz"], mesh.shape["temp"]
    return jax.shard_map(
        functools.partial(on_device, n, m),
        mesh=mesh,
        in_specs=(
            P(("group", "temp"), None, "gz", None, None),
            P(None, ("group", "gz"), None, None),
            P(("group", "temp")),
            P(("group", "temp")),
            P(("group", "temp"), "gz", None, None),
            P(("group", "temp"), "gz", None, None),
            P(("group", "temp"), "gz", None, None),
            P(("group", "temp")),
        ),
        out_specs=(P(("group", "temp"), None, "gz", None, None), P(("group", "temp"))),
        check_vma=False,
    )
```

```python
import functools
import math

import jax
import jax.numpy as jnp
from jax import lax
from jax.experimental import pallas as pl
from jax.experimental.pallas import tpu as pltpu
from jax.sharding import PartitionSpec as P

OR_SWEEPS = 2
HALVES = 2 * OR_SWEEPS + 2
PAD = 8
MESH = pl.DeviceIdType.MESH
SIN_TERMS = [(-1.0) ** i / math.factorial(2 * i + 1) for i in range(8)]
COS_TERMS = [(-1.0) ** i / math.factorial(2 * i) for i in range(9)]


def horner(terms, value):
    total = jnp.full_like(value, terms[-1])
    for term in terms[-2::-1]:
        total = total * value + term
    return total


def cos_sin(angle):
    half = 0.5 * angle
    square = half * half
    sine = half * horner(SIN_TERMS, square)
    cosine = horner(COS_TERMS, square)
    return 1.0 - 2.0 * sine * sine, 2.0 * sine * cosine


def with_sign(size, like):
    return jnp.where(like < 0.0, -size, size)


def to_square(vector):
    a, b, c = vector
    inverse = 1.0 / (jnp.abs(a) + jnp.abs(b) + jnp.abs(c))
    p, q = a * inverse, b * inverse
    low = c < 0.0
    return (
        jnp.where(low, with_sign(1.0 - jnp.abs(q), p), p),
        jnp.where(low, with_sign(1.0 - jnp.abs(p), q), q),
    )


def from_square(p, q):
    c = 1.0 - jnp.abs(p) - jnp.abs(q)
    low = c < 0.0
    a = jnp.where(low, with_sign(1.0 - jnp.abs(q), p), p)
    b = jnp.where(low, with_sign(1.0 - jnp.abs(p), q), q)
    inverse = 1.0 / jnp.sqrt(a * a + b * b + c * c)
    return a * inverse, b * inverse, c * inverse


def dot3(a, b):
    return a[0] * b[0] + a[1] * b[1] + a[2] * b[2]


def reflect(current, pulled):
    factor = 2.0 * dot3(current, pulled) / jnp.maximum(dot3(pulled, pulled), 0.01)
    return [factor * p - s for p, s in zip(pulled, current)]


def heat_bath(pulled, beta, level, trial):
    strength = jnp.sqrt(jnp.maximum(dot3(pulled, pulled), 0.01))
    inverse = 1.0 / strength
    axis = [p * inverse for p in pulled]
    reach = beta * strength
    shrink = -jnp.tanh(reach) * (jnp.exp(-2.0 * reach) + 1.0)
    cosine = 1.0 + jnp.log1p(level * shrink) / reach
    along = dot3(trial, axis)
    tangent = [t - along * a for t, a in zip(trial, axis)]
    scale = jnp.sqrt(jnp.maximum(1.0 - cosine * cosine, 0.0)) * (
        1.0 / jnp.sqrt(jnp.maximum(dot3(tangent, tangent), 0.0001))
    )
    return [cosine * a + scale * t for a, t in zip(axis, tangent)]


def flag(bits_ref, j, size, width):
    return jnp.full((size, width), bits_ref[j], jnp.int32) != 0


def sweep_kernel(
    dims,
    spin_hbm,
    coup_hbm,
    beta_hbm,
    order_hbm,
    level_hbm,
    height_hbm,
    angle_hbm,
    bits_hbm,
    evened,
    rbuf,
    trecv,
    ebuf,
    spin_in,
    coup_in,
    level_in,
    height_in,
    angle_in,
    lifted,
    osend,
    orecv,
    cbelow,
    sp,
    xo,
    xr,
    yi,
    yo,
    zu,
    zd,
    lv,
    ut,
    eacc,
    tsend,
    beta_ref,
    order_ref,
    bits_ref,
    in_sem,
    hsend,
    hrecv,
    esend,
    erecv,
    tssem,
    trsem,
    xsend,
    xrecv,
    csem,
    wrap_sem,
    temp_sem,
):
    count, planes, rows, width, n, m = dims
    k = rows // 2
    chunk = 32 if k % 32 == 0 else 8
    last = planes - 1
    g = lax.axis_index("gz")
    t = lax.axis_index("temp")
    up, down = lax.rem(g + 1, n), lax.rem(g + n - 1, n)
    has_below, has_above = t > 0, t < m - 1
    near = 2 < n <= 2 * HALVES - 2

    first = 2 * count + 4
    loads = [
        pltpu.make_async_copy(src, dst, in_sem.at[i % first])
        for i, (src, dst) in enumerate(
            (
                (order_hbm, order_ref),
                (coup_hbm.at[2, last], coup_in.at[2, last]),
                *(
                    (spin_hbm.at[r, :, z], spin_in.at[r, :, z])
                    for r in range(count)
                    for z in (last, 0)
                ),
                (bits_hbm, bits_ref),
                (beta_hbm, beta_ref),
                (coup_hbm.at[pl.ds(0, 2)], coup_in.at[pl.ds(0, 2)]),
                (coup_hbm.at[2, pl.ds(0, last)], coup_in.at[2, pl.ds(0, last)]),
                (
                    spin_hbm.at[:, :, pl.ds(1, planes - 2)],
                    spin_in.at[:, :, pl.ds(1, planes - 2)],
                ),
                (level_hbm, level_in),
                (height_hbm, height_in),
                (angle_hbm, angle_in),
            )
        )
    ]

    def peer(dt, there):
        return {"gz": there} if dt == 0 else {"temp": t + dt, "gz": there}

    def along(dt, action):
        if dt == 0:
            action()
        else:
            pl.when(has_below if dt < 0 else has_above)(action)

    for load in loads[:first]:
        load.start()

    barrier = pltpu.get_barrier_semaphore()

    def greet(temp, there):
        target = {"temp": temp, "gz": there}
        pl.semaphore_signal(barrier, inc=1, device_id=target, device_id_type=MESH)

    if near:
        pl.when(g < n - 1)(lambda: greet(t, up))
        greet(t, down)
        for d in range(1, m):
            pl.when(t + d < m)(lambda: greet(t + d, g))
        expected = t + jnp.where(g == 0, 1, 2)
    else:
        for i in range(1, n * m):
            greet(lax.rem(t + i // n, m), lax.rem(g + i % n, n))
        expected = n * m - 1

    def parity(r, z, size):
        lane = lax.broadcasted_iota(jnp.int32, (size, width), 1)
        return ((lane + (g * planes + z + order_ref[r])) & 1) != 0

    def halves(ref, index, start, size):
        even = ref[index + (pl.ds(2 * start, size, stride=2), slice(None))]
        odd = ref[index + (pl.ds(2 * start + 1, size, stride=2), slice(None))]
        return even, odd

    def put_spin(c, r, d, z, start, value):
        size = value.shape[0]
        sp[c, r, d, z + 1, pl.ds(PAD + start, size), :] = value
        if start == 0:
            sp[c, r, d, z + 1, pl.ds(PAD + k, 1), :] = value[0:1]
        if start + size == k:
            sp[c, r, d, z + 1, pl.ds(PAD - 1, 1), :] = value[size - 1 : size]

    def pack_spin(r, z):
        e = parity(r, z, k)
        for d in range(3):
            even, odd = halves(spin_in, (r, d, z), 0, k)
            put_spin(0, r, d, z, 0, jnp.where(e, odd, even))
            put_spin(1, r, d, z, 0, jnp.where(e, even, odd))

    half, quarter = k // 2, k // 4

    def parts(x, r):
        if x < HALVES - 1 or quarter % 8 or r < count - 1:
            return [(0, k)]
        return [(0, half), (half, half + quarter), (half + quarter, k)]

    def halo(x, r, side, part=0):
        c = 1 - x % 2
        start, stop = parts(x, r)[part]
        size = stop - start
        plain = sp.at[c, r, :, 1, pl.ds(PAD + start, size), :]
        above = planes + 1 if side == 0 else 0
        return pltpu.make_async_remote_copy(
            src_ref=plain if side == 0 else lifted.at[c, r, :, pl.ds(start, size), :],
            dst_ref=sp.at[c, r, :, above, pl.ds(PAD + start, size), :],
            send_sem=hsend.at[x % 2, r],
            recv_sem=hrecv.at[part + 1 if part else x % 2, r if part == 0 else 0, side],
            device_id={"gz": down if side == 0 else up},
            device_id_type=MESH,
        )

    def opening(r, side):
        return pltpu.make_async_remote_copy(
            src_ref=osend.at[r, side],
            dst_ref=orecv.at[r, side],
            send_sem=hsend.at[0, r],
            recv_sem=hrecv.at[0, r, side],
            device_id={"gz": down if side == 0 else up},
            device_id_type=MESH,
        )

    shares_of = m if rows % (8 * m) == 0 else 1
    size_of = rows // shares_of
    stretch = pl.ds(pl.multiple_of(t * size_of, 8) if shares_of > 1 else 0, size_of)

    def across():
        return pltpu.make_async_remote_copy(
            src_ref=coup_in.at[2, last, stretch],
            dst_ref=cbelow.at[stretch],
            send_sem=csem.at[0],
            recv_sem=csem.at[1],
            device_id={"gz": up},
            device_id_type=MESH,
        )

    def pass_on(d):
        return pltpu.make_async_remote_copy(
            src_ref=cbelow.at[stretch],
            dst_ref=cbelow.at[stretch],
            send_sem=csem.at[2],
            recv_sem=csem.at[3],
            device_id={"temp": lax.rem(t + d, m)},
            device_id_type=MESH,
        )

    def passed_on(i):
        if shares_of > 1:
            ref = cbelow.at[pl.ds(0, (m - 1) * size_of)]
            pltpu.make_async_copy(ref, ref, csem.at[i]).wait()

    def sent(x, r):
        both = lifted.at[:, r] if x else osend.at[r]
        pltpu.make_async_copy(both, both, hsend.at[x % 2, r]).wait()

    def lift(c, r, d, start, value):
        part = pl.ds(start, value.shape[0])
        lifted[c, r, d, part, :] = zu[c, r, last, part, :] * value

    def inner(r, action):
        if planes > 2:
            lax.fori_loop(1, last, lambda z, carry: (action(r, z), carry)[1], 0)

    def ready():
        pl.semaphore_wait(barrier, expected)

    if near:

        @pl.when(g == n - 1)
        def _():
            ready()
            pl.semaphore_signal(wrap_sem, inc=1, device_id={"gz": up}, device_id_type=MESH)

    for load in loads[:4]:
        load.wait()
    if near:
        pl.when(g == n - 1)(lambda: across().start())
    for load in loads[first : first + 4]:
        load.start()

    def pack_edges(r):
        e = parity(r, last, k)
        even, odd = halves(coup_in, (2, last), 0, k)
        zu[0, r, last] = jnp.where(e, odd, even)
        zu[1, r, last] = jnp.where(e, even, odd)
        for side, z in ((1, last), (0, 0)):
            pack_spin(r, z)
            edge = to_square([sp[1, r, d, z + 1, pl.ds(PAD, k), :] for d in range(3)])
            osend[r, side, 0], osend[r, side, 1] = edge

    def slot_order(r):
        other = order_ref[r ^ 1]
        return jnp.where(bits_ref[r - r % 2] != 0, other, order_ref[r])

    def wide(value):
        return jnp.full((1, width), value, jnp.int32).astype(jnp.float32)

    for r in range(count):
        if r > 0:
            for load in loads[2 * r + 2 : 2 * r + 4]:
                load.wait()
        pack_edges(r)
        if r == 0:
            if near:

                @pl.when(g < n - 1)
                def _():
                    ready()
                    across().start()

            else:
                ready()
                across().start()
        opening(r, 1).start()
        if near:
            pl.when(g > 0)(lambda: opening(r, 0).start())
        else:
            opening(r, 0).start()

    for load in loads[first - 2 : first]:
        load.wait()
    for load in loads[first + 4 :]:
        load.start()

    tsend[0, 0:1] = wide(slot_order(count - 1))
    tsend[0, 1:2] = wide(bits_ref[count - 1])
    tsend[0, 2:3] = wide(bits_ref[count - 2])
    tsend[1, 0:1] = wide(slot_order(0))
    tsend[1, 1:2] = wide(0)
    tsend[1, 2:3] = wide(bits_ref[0])
    for r in range(count):
        trecv[2, r : r + 1] = wide(slot_order(r))
        trecv[2, count + r : count + r + 1] = wide(bits_ref[r])

    def tell(side):
        return pltpu.make_async_remote_copy(
            src_ref=tsend.at[side],
            dst_ref=trecv.at[side],
            send_sem=tssem.at[side],
            recv_sem=trsem.at[side],
            device_id={"temp": t + 1 if side == 0 else t - 1},
            device_id_type=MESH,
        )

    if near:
        for d in range(1, m):

            @pl.when(t >= d)
            def _():
                target = {"temp": t - d, "gz": g}
                pl.semaphore_signal(temp_sem, inc=1, device_id=target, device_id_type=MESH)


    for load in loads[first : first + 3]:
        load.wait()

    def pack_bonds(i, carry):
        r, z = i // planes, i % planes
        e = parity(r, z, k)
        even, odd = halves(coup_in, (0, z), 0, k)
        first, second = jnp.where(e, odd, even), jnp.where(e, even, odd)
        xo[0, r, z] = first
        xo[1, r, z] = second
        xr[0, r, z] = pltpu.roll(second, 1, 1)
        xr[1, r, z] = pltpu.roll(first, 1, 1)
        even, odd = halves(coup_in, (1, z), 0, k)
        before = pltpu.roll(odd, 1, 0)
        yi[r, z] = even
        yo[0, r, z] = jnp.where(e, odd, before)
        yo[1, r, z] = jnp.where(e, before, odd)
        return carry

    def pack_lower(i, carry):
        r, z = i // last, 1 + i % last
        e = parity(r, z, k)
        even, odd = halves(coup_in, (2, z - 1), 0, k)
        zd[0, r, z] = jnp.where(e, odd, even)
        zd[1, r, z] = jnp.where(e, even, odd)
        zu[0, r, z - 1] = jnp.where(e, even, odd)
        zu[1, r, z - 1] = jnp.where(e, odd, even)
        return carry

    for r in range(count):
        inner(r, pack_spin)
    lax.fori_loop(0, count * planes, pack_bonds, 0)
    lax.fori_loop(0, count * last, pack_lower, 0)
    for r in range(count):
        for c in (0, 1):
            zd[c, r, 0] = jnp.ones((k, width), jnp.float32)

    if near:

        @pl.when(g == 0)
        def _():
            pl.semaphore_wait(wrap_sem, 1)
            for r in range(count):
                opening(r, 0).start()

    def pull(c, r, z, start, chunk=chunk):
        o = 1 - c
        part = pl.ds(start, chunk)
        e = parity(r, z, chunk)
        bx, br, by = xo[c, r, z, part, :], xr[c, r, z, part, :], yi[r, z, part, :]
        bo, bu, bd = yo[c, r, z, part, :], zu[c, r, z, part, :], zd[c, r, z, part, :]
        pulled = []
        for d in range(3):
            mid = sp[o, r, d, z + 1, pl.ds(PAD + start, chunk), :]
            nxt = sp[o, r, d, z + 1, pl.ds(PAD + start + 1, chunk), :]
            prv = sp[o, r, d, z + 1, pl.ds(PAD + start - 1, chunk), :]
            outer = jnp.where(e, nxt, prv) if c == 0 else jnp.where(e, prv, nxt)
            total = bx * pltpu.roll(mid, width - 1, 1) + br * pltpu.roll(mid, 1, 1)
            total = total + by * mid + bo * outer
            total = total + bu * sp[o, r, d, z + 2, pl.ds(PAD + start, chunk), :]
            total = total + bd * sp[o, r, d, z, pl.ds(PAD + start, chunk), :]
            pulled.append(total)
        return pulled

    def relax(c, r, z, lifting=False):
        for start in range(0, k, chunk):
            pulled = pull(c, r, z, start)
            current = [sp[c, r, d, z + 1, pl.ds(PAD + start, chunk), :] for d in range(3)]
            for d, value in enumerate(reflect(current, pulled)):
                put_spin(c, r, d, z, start, value)
                if lifting:
                    lift(c, r, d, start, value)

    def heat(c, r, z, lifting=False, rows_of=(0, k)):
        size = min(chunk, rows_of[1] - rows_of[0])
        for start in range(*rows_of, size):
            part = pl.ds(start, size)
            pulled = pull(c, r, z, start, size)
            trial = [ut[c, r, d, z, part, :] for d in range(3)]
            renewed = heat_bath(pulled, beta_ref[r], lv[c, r, z, part, :], trial)
            for d, value in enumerate(renewed):
                put_spin(c, r, d, z, start, value)
                if lifting:
                    lift(c, r, d, start, value)
            if c == 1:
                terms = dot3(renewed, pulled)
                eacc[r] = eacc[r] + sum(terms[j : j + 8] for j in range(0, size, 8))

    def pack_heat(r, z):
        for start in range(0, k, chunk):
            part = pl.ds(start, chunk)
            e = parity(r, z, chunk)
            even, odd = halves(level_in, (r, z), start, chunk)
            lv[0, r, z, part, :] = jnp.where(e, odd, even)
            lv[1, r, z, part, :] = jnp.where(e, even, odd)
            angles = halves(angle_in, (r, z), start, chunk)
            heights = halves(height_in, (r, z), start, chunk)
            trials = []
            for angle, height in zip(angles, heights):
                side = jnp.sqrt(jnp.maximum(1.0 - height * height, 0.0))
                cosine, sine = cos_sin(angle)
                trials.append((side * cosine, side * sine, height))
            for d in range(3):
                ut[0, r, d, z, part, :] = jnp.where(e, trials[1][d], trials[0][d])
                ut[1, r, d, z, part, :] = jnp.where(e, trials[0][d], trials[1][d])

    def take_halo(x, r, side):
        halo(x, r, 1 - side).wait_recv()
        if side == 0:
            sent(x - 1, r)

    def take_opening(r, side):
        opening(r, 1 - side).wait_recv()
        vector = from_square(orecv[r, 1 - side, 0], orecv[r, 1 - side, 1])
        if side == 0:
            even, odd = halves(cbelow, (), 0, k)
            bond = jnp.where(parity(r, 0, k), odd, even)
            vector = [bond * v for v in vector]
        for d in range(3):
            sp[1, r, d, planes + 1 if side else 0, pl.ds(PAD, k), :] = vector[d]

    def settle(c, z, start, stop):
        size = stop - start
        part, packed = pl.ds(start, size), pl.ds(PAD + start, size)
        for r in range(0, count, 2):
            taking = flag(bits_ref, r, size, width)
            for d in range(3):
                low = sp[c, r, d, z + 1, packed, :]
                top = sp[c, r + 1, d, z + 1, packed, :]
                evened[r, c * planes + z, d, part, :] = jnp.where(taking, top, low)
                evened[r + 1, c * planes + z, d, part, :] = jnp.where(taking, low, top)

    final = parts(HALVES - 1, count - 1)

    def pieces(c, z):
        return final if c == 1 and z in (0, last) else [(0, k)]

    def ship(c, z, side, part=0, many=1):
        start, stop = pieces(c, z)[part]
        rows_of = pl.ds(start, stop - start)
        here = pl.ds(c * planes + z, many)
        early = c == 0 and 0 < z < last
        return pltpu.make_async_remote_copy(
            src_ref=evened.at[count - 1 if side == 0 else 0, here, :, rows_of, :],
            dst_ref=rbuf.at[side, here, :, rows_of, :],
            send_sem=xsend.at[side],
            recv_sem=xrecv.at[0 if early else 1, side],
            device_id={"temp": t + 1 if side == 0 else t - 1},
            device_id_type=MESH,
        )

    def both_ways(action):
        along(1, lambda: action(0))
        along(-1, lambda: action(1))

    def send_off(c, z, part=0):
        settle(c, z, *pieces(c, z)[part])
        both_ways(lambda side: ship(c, z, side, part).start())

    def send_inner(c):
        for z in range(1, last):
            settle(c, z, 0, k)
        if planes > 2:
            both_ways(lambda side: ship(c, 1, side, many=planes - 2).start())

    def whole(side, size, sem):
        ref = rbuf.at[side, pl.ds(0, size)]
        pltpu.make_async_copy(ref, ref, sem).wait()

    def arrived(early):
        size = planes - 2 if early else planes + 2
        if size:
            both_ways(lambda side: whole(1 - side, size, xrecv.at[0 if early else 1, 1 - side]))

    def work(x):
        return functools.partial(relax if x < relaxing else heat, x % 2)

    ahead = g < n - 1
    eacc[...] = jnp.zeros_like(eacc)
    relaxing = 2 * OR_SWEEPS
    for r in range(count):
        inner(r, work(0))
    for load in loads[first + 3 :]:
        load.wait()
    if near:
        along(1, lambda: pl.semaphore_wait(temp_sem, m - 1 - t))
    along(1, lambda: tell(0).start())
    along(-1, lambda: tell(1).start())
    across().wait_recv()
    if shares_of > 1:
        for d in range(1, m):
            pass_on(d).start()

    def first_step(i, carry):
        r = jnp.where(g == 0, lax.rem(i, count), i // 2)
        side = jnp.where(g == 0, jnp.where(i < count, 1, 0), 1 - lax.rem(i, 2))
        pl.when(i == jnp.where(g == 0, count, 1))(lambda: passed_on(3))

        @pl.when(side == 1)
        def _():
            take_opening(r, 1)
            work(0)(r, last, lifting=True)
            halo(1, r, 1).start()

        @pl.when(side == 0)
        def _():
            take_opening(r, 0)
            work(0)(r, 0)
            halo(1, r, 0).start()

        return carry

    lax.fori_loop(0, 2 * count, first_step, 0)
    for x in range(HALVES - 1):
        for r in range(count):
            for side, z in ((0, 0), (1, last)) if x else ():
                take_halo(x, r, side)
                work(x)(r, z, lifting=side == 1)
                if side == 0 and len(parts(x + 1, r)) == 1:
                    pl.when(ahead)(lambda: halo(x + 1, r, 0).start())
            for part in range(len(parts(x + 1, r)) if x else 0):
                if len(parts(x + 1, r)) > 1:
                    pl.when(ahead)(lambda: halo(x + 1, r, 0, part).start())
                halo(x + 1, r, 1, part).start()
                pl.when(~ahead)(lambda: halo(x + 1, r, 0, part).start())
            if r == count - 1 and x == relaxing:
                for z in (0, last):
                    send_off(0, z)
            for z in range(planes):
                if z % relaxing == x:
                    pack_heat(r, z)
            inner(r, work(x + 1))
        if x >= relaxing - 1:
            send_inner(x + 1 - relaxing)

    x = HALVES - 1
    for r in range(count):
        if r == count - 1:
            arrived(True)
            along(1, lambda: tell(1).wait_recv())
            along(-1, lambda: tell(0).wait_recv())
        for part, rows_of in enumerate(parts(x, r)):
            for side, z in ((0, 0), (1, last)):
                halo(x, r, 1 - side, part).wait_recv()
                if part == 0 and side == 0:
                    sent(x - 1, r)
                work(x)(r, z, rows_of=rows_of)
                if r == count - 1:
                    send_off(1, z, part)
    for r in range(count):
        ebuf[1, g, r : r + 1] = jnp.sum(eacc[r], axis=0, keepdims=True)

    def share(dt, source, there):
        return pltpu.make_async_remote_copy(
            src_ref=ebuf.at[1, source],
            dst_ref=ebuf.at[1 - dt, source],
            send_sem=esend.at[1 - dt],
            recv_sem=erecv.at[1 - dt],
            device_id=peer(dt, there),
            device_id_type=MESH,
        )

    def spread(dt):
        for d in range(1 if dt == 0 else 0, n):
            share(dt, g, lax.rem(g + d, n)).start()

    def shares(dt, sem):
        ref = ebuf.at[1, pl.ds(0, n - 1 if dt == 0 else n)]
        pltpu.make_async_copy(ref, ref, sem).wait()

    for dt in (0, 1, -1):
        along(dt, lambda dt=dt: spread(dt))
    for r in range(count):
        sent(x, r)
    across().wait_send()
    passed_on(2)
    along(1, lambda: tell(0).wait_send())
    along(-1, lambda: tell(1).wait_send())
    both_ways(lambda side: whole(side, 2 * planes, xsend.at[side]))
    arrived(False)
    for dt in (0, 1, -1):
        along(dt, lambda dt=dt: shares(dt, esend.at[1 - dt]))
        along(dt, lambda dt=dt: shares(dt, erecv.at[1 + dt]))


def finish_kernel(
    dims,
    evened,
    rbuf,
    trecv,
    ebuf,
    out_hbm,
    eout_hbm,
    stage,
    eout_ref,
    out_sem,
    eout_sem,
):
    count, planes, rows, width, n, m = dims
    k = rows // 2
    g = lax.axis_index("gz")
    t = lax.axis_index("temp")
    below, above = (t > 0).astype(jnp.int32), (t < m - 1).astype(jnp.int32)

    def number(side, row):
        return trecv[side, row : row + 1]

    def own_order(r):
        return number(2, r)

    def own_bit(r):
        return number(2, count + r)

    def mask(value, size):
        return jnp.broadcast_to(value, (size, width)) > 0.5

    def plan(r):
        if r == 0:
            met = jnp.full((1, width), below, jnp.int32) != 0
            return rbuf.at[0], jnp.where(met, number(0, 1), 0.0), jnp.where(met, number(0, 0), 0.0)
        if r == count - 1:
            met = jnp.full((1, width), above, jnp.int32) != 0
            return rbuf.at[1], jnp.where(met, own_bit(r), 0.0), jnp.where(met, number(1, 0), 0.0)
        other = r + 1 if r % 2 else r - 1
        return evened.at[other], own_bit(min(r, other)), own_order(other)

    lane = lax.broadcasted_iota(jnp.int32, (k, width), 1)
    plans = [plan(r) for r in range(count)]
    orders = [
        jnp.where(take > 0.5, order, own_order(r)).astype(jnp.int32)
        for r, (_, take, order) in enumerate(plans)
    ]
    def unpack(z):
        for r in range(count):
            other, take, _ = plans[r]
            taking = mask(take, k)
            e = ((lane + (jnp.broadcast_to(orders[r], (k, width)) + (g * planes + z))) & 1) != 0
            for d in range(3):
                first, second = [
                    jnp.where(taking, other[i, d], evened[r, i, d]) for i in (z, planes + z)
                ]
                stage[r, d, z, pl.ds(0, k, stride=2), :] = jnp.where(e, second, first)
                stage[r, d, z, pl.ds(1, k, stride=2), :] = jnp.where(e, first, second)
            copy = pltpu.make_async_copy(
                stage.at[r, :, z], out_hbm.at[r, :, z], out_sem
            )
            copy.start()

    for z in range(planes // 2):
        unpack(z)
    sites = float(width * rows * planes * n)

    def total(slot, r):
        summed = ebuf[slot, 0, r : r + 1]
        for j in range(1, n):
            summed = summed + ebuf[slot, j, r : r + 1]
        return jnp.broadcast_to(jnp.sum(-summed, axis=1, keepdims=True) / sites, (1, width))

    energy = []
    for r in range(0, count, 2):
        taking = own_bit(r) > 0.5
        low, top = total(1, r), total(1, r + 1)
        energy += [jnp.where(taking, top, low), jnp.where(taking, low, top)]
    for r in range(count):
        other, take, _ = plans[r]
        if r == 0:
            swapped = number(0, 2) > 0.5
            partner = jnp.where(swapped, total(0, count - 2), total(0, count - 1))
        elif r == count - 1:
            swapped = number(1, 2) > 0.5
            partner = jnp.where(swapped, total(2, 1), total(2, 0))
        else:
            partner = energy[r + 1 if r % 2 else r - 1]
        eout_ref[r] = jnp.max(jnp.where(take > 0.5, partner, energy[r]))
    told = pltpu.make_async_copy(eout_ref, eout_hbm, eout_sem)
    told.start()
    for z in range(planes // 2, planes):
        unpack(z)
    told.wait()
    pltpu.make_async_copy(stage, out_hbm, out_sem).wait()


def on_device(n, m, spin, coup, beta, order, level, height, angle, bits):
    count, _, planes, rows, width = spin.shape
    k = rows // 2
    f32 = jnp.float32
    hbm = pl.BlockSpec(memory_space=pltpu.HBM)
    vmem = pl.BlockSpec(memory_space=pltpu.VMEM)
    dma = pltpu.SemaphoreType.DMA
    bonds = pltpu.VMEM((2, count, planes, k, width), f32)
    dims = (count, planes, rows, width, n, m)
    handed = pl.pallas_call(
        functools.partial(sweep_kernel, dims),
        out_shape=(
            pltpu.VMEM((count, 2 * planes, 3, k, width), f32),
            pltpu.VMEM((2, 2 * planes, 3, k, width), f32),
            pltpu.VMEM((3, max(8, 2 * count), width), f32),
            pltpu.VMEM((3, n, count, width), f32),
        ),
        in_specs=[hbm] * 8,
        out_specs=(vmem,) * 4,
        scratch_shapes=[
            pltpu.VMEM(spin.shape, f32),
            pltpu.VMEM(coup.shape, f32),
            pltpu.VMEM(level.shape, f32),
            pltpu.VMEM(level.shape, f32),
            pltpu.VMEM(level.shape, f32),
            pltpu.VMEM((2, count, 3, k, width), f32),
            pltpu.VMEM((count, 2, 2, k, width), f32),
            pltpu.VMEM((count, 2, 2, k, width), f32),
            pltpu.VMEM((rows, width), f32),
            pltpu.VMEM((2, count, 3, planes + 2, k + 2 * PAD, width), f32),
            bonds,
            bonds,
            pltpu.VMEM((count, planes, k, width), f32),
            bonds,
            bonds,
            bonds,
            bonds,
            pltpu.VMEM((2, count, 3, planes, k, width), f32),
            pltpu.VMEM((count, 8, width), f32),
            pltpu.VMEM((2, max(8, 2 * count), width), f32),
            pltpu.SMEM((count,), f32),
            pltpu.SMEM((count,), jnp.int32),
            pltpu.SMEM((count,), jnp.int32),
            dma((2 * count + 4,)),
            dma((2, count)),
            dma((4, count, 2)),
            dma((3,)),
            dma((3,)),
            dma((2,)),
            dma((2,)),
            dma((2,)),
            dma((2, 2)),
            dma((4,)),
            pltpu.SemaphoreType.REGULAR,
            pltpu.SemaphoreType.REGULAR,
        ],
        compiler_params=pltpu.CompilerParams(
            collective_id=0, has_side_effects=True, vmem_limit_bytes=58 * 1024 * 1024
        ),
    )(spin, coup, beta, order, level, height, angle, bits)
    return pl.pallas_call(
        functools.partial(finish_kernel, dims),
        out_shape=(
            jax.ShapeDtypeStruct(spin.shape, f32),
            jax.ShapeDtypeStruct((count,), f32),
        ),
        in_specs=[vmem] * 4,
        out_specs=(hbm, hbm),
        scratch_shapes=[
            pltpu.VMEM(spin.shape, f32),
            pltpu.SMEM((count,), f32),
            dma(()),
            dma(()),
        ],
        compiler_params=pltpu.CompilerParams(vmem_limit_bytes=16 * 1024 * 1024),
    )(*handed)


def solution(mesh):
    n, m = mesh.shape["gz"], mesh.shape["temp"]
    return jax.shard_map(
        functools.partial(on_device, n, m),
        mesh=mesh,
        in_specs=(
            P(("group", "temp"), None, "gz", None, None),
            P(None, ("group", "gz"), None, None),
            P(("group", "temp")),
            P(("group", "temp")),
            P(("group", "temp"), "gz", None, None),
            P(("group", "temp"), "gz", None, None),
            P(("group", "temp"), "gz", None, None),
            P(("group", "temp")),
        ),
        out_specs=(P(("group", "temp"), None, "gz", None, None), P(("group", "temp"))),
        check_vma=False,
    )
```

```python
import functools
import math

import jax
import jax.numpy as jnp
from jax import lax
from jax.experimental import pallas as pl
from jax.experimental.pallas import tpu as pltpu
from jax.sharding import PartitionSpec as P

OR_SWEEPS = 2
HALVES = 2 * OR_SWEEPS + 2
PAD = 8
MESH = pl.DeviceIdType.MESH
SIN_TERMS = [(-1.0) ** i / math.factorial(2 * i + 1) for i in range(8)]
COS_TERMS = [(-1.0) ** i / math.factorial(2 * i) for i in range(9)]


def horner(terms, value):
    total = jnp.full_like(value, terms[-1])
    for term in terms[-2::-1]:
        total = total * value + term
    return total


def cos_sin(angle):
    half = 0.5 * angle
    square = half * half
    sine = half * horner(SIN_TERMS, square)
    cosine = horner(COS_TERMS, square)
    return 1.0 - 2.0 * sine * sine, 2.0 * sine * cosine


def with_sign(size, like):
    return jnp.where(like < 0.0, -size, size)


def to_square(vector):
    a, b, c = vector
    inverse = 1.0 / (jnp.abs(a) + jnp.abs(b) + jnp.abs(c))
    p, q = a * inverse, b * inverse
    low = c < 0.0
    return (
        jnp.where(low, with_sign(1.0 - jnp.abs(q), p), p),
        jnp.where(low, with_sign(1.0 - jnp.abs(p), q), q),
    )


def from_square(p, q):
    c = 1.0 - jnp.abs(p) - jnp.abs(q)
    low = c < 0.0
    a = jnp.where(low, with_sign(1.0 - jnp.abs(q), p), p)
    b = jnp.where(low, with_sign(1.0 - jnp.abs(p), q), q)
    inverse = 1.0 / jnp.sqrt(a * a + b * b + c * c)
    return a * inverse, b * inverse, c * inverse


def dot3(a, b):
    return a[0] * b[0] + a[1] * b[1] + a[2] * b[2]


def reflect(current, pulled):
    factor = 2.0 * dot3(current, pulled) / jnp.maximum(dot3(pulled, pulled), 0.01)
    return [factor * p - s for p, s in zip(pulled, current)]


def heat_bath(pulled, beta, level, trial):
    strength = jnp.sqrt(jnp.maximum(dot3(pulled, pulled), 0.01))
    inverse = 1.0 / strength
    axis = [p * inverse for p in pulled]
    reach = beta * strength
    shrink = -jnp.tanh(reach) * (jnp.exp(-2.0 * reach) + 1.0)
    cosine = 1.0 + jnp.log1p(level * shrink) / reach
    along = dot3(trial, axis)
    tangent = [t - along * a for t, a in zip(trial, axis)]
    scale = jnp.sqrt(jnp.maximum(1.0 - cosine * cosine, 0.0)) * (
        1.0 / jnp.sqrt(jnp.maximum(dot3(tangent, tangent), 0.0001))
    )
    return [cosine * a + scale * t for a, t in zip(axis, tangent)]


def flag(bits_ref, j, size, width):
    return jnp.full((size, width), bits_ref[j], jnp.int32) != 0


def sweep_kernel(
    dims,
    spin_hbm,
    coup_hbm,
    beta_hbm,
    order_hbm,
    level_hbm,
    height_hbm,
    angle_hbm,
    bits_hbm,
    evened,
    rbuf,
    trecv,
    ebuf,
    spin_in,
    coup_in,
    level_in,
    height_in,
    angle_in,
    lifted,
    osend,
    orecv,
    cbelow,
    sp,
    xo,
    xr,
    yi,
    yo,
    zu,
    zd,
    lv,
    ut,
    eacc,
    tsend,
    beta_ref,
    order_ref,
    bits_ref,
    in_sem,
    hsend,
    hrecv,
    esend,
    erecv,
    tssem,
    trsem,
    xsend,
    xrecv,
    csem,
    wrap_sem,
    temp_sem,
):
    count, planes, rows, width, n, m = dims
    k = rows // 2
    chunk = 32 if k % 32 == 0 else 8
    last = planes - 1
    g = lax.axis_index("gz")
    t = lax.axis_index("temp")
    up, down = lax.rem(g + 1, n), lax.rem(g + n - 1, n)
    has_below, has_above = t > 0, t < m - 1
    near = 2 < n <= 2 * HALVES - 2

    first = 2 * count + 4
    loads = [
        pltpu.make_async_copy(src, dst, in_sem.at[i % first])
        for i, (src, dst) in enumerate(
            (
                (order_hbm, order_ref),
                (coup_hbm.at[2, last], coup_in.at[2, last]),
                *(
                    (spin_hbm.at[r, :, z], spin_in.at[r, :, z])
                    for r in range(count)
                    for z in (last, 0)
                ),
                (bits_hbm, bits_ref),
                (beta_hbm, beta_ref),
                (coup_hbm.at[pl.ds(0, 2)], coup_in.at[pl.ds(0, 2)]),
                (coup_hbm.at[2, pl.ds(0, last)], coup_in.at[2, pl.ds(0, last)]),
                (
                    spin_hbm.at[:, :, pl.ds(1, planes - 2)],
                    spin_in.at[:, :, pl.ds(1, planes - 2)],
                ),
                (level_hbm, level_in),
                (height_hbm, height_in),
                (angle_hbm, angle_in),
            )
        )
    ]

    def peer(dt, there):
        return {"gz": there} if dt == 0 else {"temp": t + dt, "gz": there}

    def along(dt, action):
        if dt == 0:
            action()
        else:
            pl.when(has_below if dt < 0 else has_above)(action)

    for load in loads[:4]:
        load.start()

    barrier = pltpu.get_barrier_semaphore()

    def greet(temp, there):
        target = {"temp": temp, "gz": there}
        pl.semaphore_signal(barrier, inc=1, device_id=target, device_id_type=MESH)

    if near:
        pl.when(g < n - 1)(lambda: greet(t, up))
        greet(t, down)
        for d in range(1, m):
            pl.when(t + d < m)(lambda: greet(t + d, g))
        expected = t + jnp.where(g == 0, 1, 2)
    else:
        for i in range(1, n * m):
            greet(lax.rem(t + i // n, m), lax.rem(g + i % n, n))
        expected = n * m - 1

    def parity(r, z, size):
        lane = lax.broadcasted_iota(jnp.int32, (size, width), 1)
        return ((lane + (g * planes + z + order_ref[r])) & 1) != 0

    def halves(ref, index, start, size):
        even = ref[index + (pl.ds(2 * start, size, stride=2), slice(None))]
        odd = ref[index + (pl.ds(2 * start + 1, size, stride=2), slice(None))]
        return even, odd

    def put_spin(c, r, d, z, start, value):
        size = value.shape[0]
        sp[c, r, d, z + 1, pl.ds(PAD + start, size), :] = value
        if start == 0:
            sp[c, r, d, z + 1, pl.ds(PAD + k, 1), :] = value[0:1]
        if start + size == k:
            sp[c, r, d, z + 1, pl.ds(PAD - 1, 1), :] = value[size - 1 : size]

    def pack_spin(r, z):
        e = parity(r, z, k)
        for d in range(3):
            even, odd = halves(spin_in, (r, d, z), 0, k)
            put_spin(0, r, d, z, 0, jnp.where(e, odd, even))
            put_spin(1, r, d, z, 0, jnp.where(e, even, odd))

    half = k // 2

    def parts(x, r):
        if x < HALVES - 1 or k % 32 or r < count - 1:
            return [(0, k)]
        return [(0, half), (half, k - 8), (k - 8, k)]

    def halo(x, r, side, part=0):
        c = 1 - x % 2
        start, stop = parts(x, r)[part]
        size = stop - start
        plain = sp.at[c, r, :, 1, pl.ds(PAD + start, size), :]
        above = planes + 1 if side == 0 else 0
        return pltpu.make_async_remote_copy(
            src_ref=plain if side == 0 else lifted.at[c, r, :, pl.ds(start, size), :],
            dst_ref=sp.at[c, r, :, above, pl.ds(PAD + start, size), :],
            send_sem=hsend.at[x % 2, r],
            recv_sem=hrecv.at[
                4 * count + 2 * part - 2 + side if part else 2 * (x % 2 * count + r) + side
            ],
            device_id={"gz": down if side == 0 else up},
            device_id_type=MESH,
        )

    def opening(r, side):
        return pltpu.make_async_remote_copy(
            src_ref=osend.at[r, side],
            dst_ref=orecv.at[r, side],
            send_sem=hsend.at[0, r],
            recv_sem=hrecv.at[2 * r + side],
            device_id={"gz": down if side == 0 else up},
            device_id_type=MESH,
        )

    shares_of = m if rows % (8 * m) == 0 else 1
    size_of = rows // shares_of
    stretch = pl.ds(pl.multiple_of(t * size_of, 8) if shares_of > 1 else 0, size_of)

    def across():
        return pltpu.make_async_remote_copy(
            src_ref=coup_in.at[2, last, stretch],
            dst_ref=cbelow.at[stretch],
            send_sem=csem.at[0],
            recv_sem=csem.at[1],
            device_id={"gz": up},
            device_id_type=MESH,
        )

    def pass_on(d):
        return pltpu.make_async_remote_copy(
            src_ref=cbelow.at[stretch],
            dst_ref=cbelow.at[stretch],
            send_sem=csem.at[2],
            recv_sem=csem.at[3],
            device_id={"temp": lax.rem(t + d, m)},
            device_id_type=MESH,
        )

    def passed_on(i):
        if shares_of > 1:
            ref = cbelow.at[pl.ds(0, (m - 1) * size_of)]
            pltpu.make_async_copy(ref, ref, csem.at[i]).wait()

    def sent(x, r):
        both = lifted.at[:, r] if x else osend.at[r]
        pltpu.make_async_copy(both, both, hsend.at[x % 2, r]).wait()

    def lift(c, r, d, start, value):
        part = pl.ds(start, value.shape[0])
        lifted[c, r, d, part, :] = zu[c, r, last, part, :] * value

    def inner(r, action):
        if planes > 2:
            lax.fori_loop(1, last, lambda z, carry: (action(r, z), carry)[1], 0)

    def ready():
        pl.semaphore_wait(barrier, expected)

    if near:

        @pl.when(g == n - 1)
        def _():
            ready()
            pl.semaphore_signal(wrap_sem, inc=1, device_id={"gz": up}, device_id_type=MESH)

    for load in loads[:4]:
        load.wait()
    if near:
        pl.when(g == n - 1)(lambda: across().start())
    for load in loads[4 : first + 4]:
        load.start()

    def pack_edges(r):
        e = parity(r, last, k)
        even, odd = halves(coup_in, (2, last), 0, k)
        zu[0, r, last] = jnp.where(e, odd, even)
        zu[1, r, last] = jnp.where(e, even, odd)
        for side, z in ((1, last), (0, 0)):
            pack_spin(r, z)
            edge = to_square([sp[1, r, d, z + 1, pl.ds(PAD, k), :] for d in range(3)])
            osend[r, side, 0], osend[r, side, 1] = edge

    def slot_order(r):
        other = order_ref[r ^ 1]
        return jnp.where(bits_ref[r - r % 2] != 0, other, order_ref[r])

    def wide(value):
        return jnp.full((1, width), value, jnp.int32).astype(jnp.float32)

    for r in range(count):
        if r > 0:
            for load in loads[2 * r + 2 : 2 * r + 4]:
                load.wait()
        pack_edges(r)
        if r == 0:
            if near:

                @pl.when(g < n - 1)
                def _():
                    ready()
                    across().start()

            else:
                ready()
                across().start()
        opening(r, 1).start()
        if near:
            pl.when(g > 0)(lambda: opening(r, 0).start())
        else:
            opening(r, 0).start()

    for load in loads[first - 2 : first]:
        load.wait()
    for load in loads[first + 4 :]:
        load.start()

    tsend[0, 0:1] = wide(slot_order(count - 1))
    tsend[0, 1:2] = wide(bits_ref[count - 1])
    tsend[0, 2:3] = wide(bits_ref[count - 2])
    tsend[1, 0:1] = wide(slot_order(0))
    tsend[1, 1:2] = wide(0)
    tsend[1, 2:3] = wide(bits_ref[0])
    for r in range(count):
        trecv[2, r : r + 1] = wide(slot_order(r))
        trecv[2, count + r : count + r + 1] = wide(bits_ref[r])

    def tell(side):
        return pltpu.make_async_remote_copy(
            src_ref=tsend.at[side],
            dst_ref=trecv.at[side],
            send_sem=tssem.at[side],
            recv_sem=trsem.at[side],
            device_id={"temp": t + 1 if side == 0 else t - 1},
            device_id_type=MESH,
        )

    if near:
        for d in range(1, m):

            @pl.when(t >= d)
            def _():
                target = {"temp": t - d, "gz": g}
                pl.semaphore_signal(temp_sem, inc=1, device_id=target, device_id_type=MESH)


    for load in loads[first : first + 3]:
        load.wait()

    def pack_bonds(i, carry):
        r, z = i // planes, i % planes
        e = parity(r, z, k)
        even, odd = halves(coup_in, (0, z), 0, k)
        first, second = jnp.where(e, odd, even), jnp.where(e, even, odd)
        xo[0, r, z] = first
        xo[1, r, z] = second
        xr[0, r, z] = pltpu.roll(second, 1, 1)
        xr[1, r, z] = pltpu.roll(first, 1, 1)
        even, odd = halves(coup_in, (1, z), 0, k)
        before = pltpu.roll(odd, 1, 0)
        yi[r, z] = even
        yo[0, r, z] = jnp.where(e, odd, before)
        yo[1, r, z] = jnp.where(e, before, odd)
        return carry

    def pack_lower(i, carry):
        r, z = i // last, 1 + i % last
        e = parity(r, z, k)
        even, odd = halves(coup_in, (2, z - 1), 0, k)
        zd[0, r, z] = jnp.where(e, odd, even)
        zd[1, r, z] = jnp.where(e, even, odd)
        zu[0, r, z - 1] = jnp.where(e, even, odd)
        zu[1, r, z - 1] = jnp.where(e, odd, even)
        return carry

    for r in range(count):
        inner(r, pack_spin)
    lax.fori_loop(0, count * planes, pack_bonds, 0)
    lax.fori_loop(0, count * last, pack_lower, 0)
    for r in range(count):
        for c in (0, 1):
            zd[c, r, 0] = jnp.ones((k, width), jnp.float32)

    if near:

        @pl.when(g == 0)
        def _():
            pl.semaphore_wait(wrap_sem, 1)
            for r in range(count):
                opening(r, 0).start()

    def pull(c, r, z, start, chunk=chunk):
        o = 1 - c
        part = pl.ds(start, chunk)
        e = parity(r, z, chunk)
        bx, br, by = xo[c, r, z, part, :], xr[c, r, z, part, :], yi[r, z, part, :]
        bo, bu, bd = yo[c, r, z, part, :], zu[c, r, z, part, :], zd[c, r, z, part, :]
        pulled = []
        for d in range(3):
            mid = sp[o, r, d, z + 1, pl.ds(PAD + start, chunk), :]
            nxt = sp[o, r, d, z + 1, pl.ds(PAD + start + 1, chunk), :]
            prv = sp[o, r, d, z + 1, pl.ds(PAD + start - 1, chunk), :]
            outer = jnp.where(e, nxt, prv) if c == 0 else jnp.where(e, prv, nxt)
            total = bx * pltpu.roll(mid, width - 1, 1) + br * pltpu.roll(mid, 1, 1)
            total = total + by * mid + bo * outer
            total = total + bu * sp[o, r, d, z + 2, pl.ds(PAD + start, chunk), :]
            total = total + bd * sp[o, r, d, z, pl.ds(PAD + start, chunk), :]
            pulled.append(total)
        return pulled

    def relax(c, r, z, lifting=False):
        for start in range(0, k, chunk):
            pulled = pull(c, r, z, start)
            current = [sp[c, r, d, z + 1, pl.ds(PAD + start, chunk), :] for d in range(3)]
            for d, value in enumerate(reflect(current, pulled)):
                put_spin(c, r, d, z, start, value)
                if lifting:
                    lift(c, r, d, start, value)

    def heat(c, r, z, lifting=False, rows_of=(0, k)):
        size = min(chunk, rows_of[1] - rows_of[0])
        for start in range(*rows_of, size):
            part = pl.ds(start, size)
            pulled = pull(c, r, z, start, size)
            trial = [ut[c, r, d, z, part, :] for d in range(3)]
            renewed = heat_bath(pulled, beta_ref[r], lv[c, r, z, part, :], trial)
            for d, value in enumerate(renewed):
                put_spin(c, r, d, z, start, value)
                if lifting:
                    lift(c, r, d, start, value)
            if c == 1:
                terms = dot3(renewed, pulled)
                eacc[r] = eacc[r] + sum(terms[j : j + 8] for j in range(0, size, 8))

    def pack_heat(r, z):
        for start in range(0, k, chunk):
            part = pl.ds(start, chunk)
            e = parity(r, z, chunk)
            even, odd = halves(level_in, (r, z), start, chunk)
            lv[0, r, z, part, :] = jnp.where(e, odd, even)
            lv[1, r, z, part, :] = jnp.where(e, even, odd)
            angles = halves(angle_in, (r, z), start, chunk)
            heights = halves(height_in, (r, z), start, chunk)
            trials = []
            for angle, height in zip(angles, heights):
                side = jnp.sqrt(jnp.maximum(1.0 - height * height, 0.0))
                cosine, sine = cos_sin(angle)
                trials.append((side * cosine, side * sine, height))
            for d in range(3):
                ut[0, r, d, z, part, :] = jnp.where(e, trials[1][d], trials[0][d])
                ut[1, r, d, z, part, :] = jnp.where(e, trials[0][d], trials[1][d])

    def take_halo(x, r, side):
        halo(x, r, 1 - side).wait_recv()
        if side == 0:
            sent(x - 1, r)

    def take_opening(r, side):
        opening(r, 1 - side).wait_recv()
        vector = from_square(orecv[r, 1 - side, 0], orecv[r, 1 - side, 1])
        if side == 0:
            even, odd = halves(cbelow, (), 0, k)
            bond = jnp.where(parity(r, 0, k), odd, even)
            vector = [bond * v for v in vector]
        for d in range(3):
            sp[1, r, d, planes + 1 if side else 0, pl.ds(PAD, k), :] = vector[d]

    def settle(c, z, start, stop):
        size = stop - start
        part, packed = pl.ds(start, size), pl.ds(PAD + start, size)
        for r in range(0, count, 2):
            taking = flag(bits_ref, r, size, width)
            for d in range(3):
                low = sp[c, r, d, z + 1, packed, :]
                top = sp[c, r + 1, d, z + 1, packed, :]
                evened[r, c * planes + z, d, part, :] = jnp.where(taking, top, low)
                evened[r + 1, c * planes + z, d, part, :] = jnp.where(taking, low, top)

    final = parts(HALVES - 1, count - 1)

    def pieces(c, z):
        return final if c == 1 and z in (0, last) else [(0, k)]

    def ship(c, z, side, part=0, many=1):
        start, stop = pieces(c, z)[part]
        rows_of = pl.ds(start, stop - start)
        here = pl.ds(c * planes + z, many)
        early = c == 0 and 0 < z < last
        return pltpu.make_async_remote_copy(
            src_ref=evened.at[count - 1 if side == 0 else 0, here, :, rows_of, :],
            dst_ref=rbuf.at[side, here, :, rows_of, :],
            send_sem=xsend.at[side],
            recv_sem=xrecv.at[0 if early else 1, side],
            device_id={"temp": t + 1 if side == 0 else t - 1},
            device_id_type=MESH,
        )

    def both_ways(action):
        along(1, lambda: action(0))
        along(-1, lambda: action(1))

    def send_off(c, z, part=0):
        settle(c, z, *pieces(c, z)[part])
        both_ways(lambda side: ship(c, z, side, part).start())

    def send_inner(c):
        for z in range(1, last):
            settle(c, z, 0, k)
        if planes > 2:
            both_ways(lambda side: ship(c, 1, side, many=planes - 2).start())

    def whole(side, size, sem):
        ref = rbuf.at[side, pl.ds(0, size)]
        pltpu.make_async_copy(ref, ref, sem).wait()

    def arrived(early):
        size = planes - 2 if early else planes + 2
        if size:
            both_ways(lambda side: whole(1 - side, size, xrecv.at[0 if early else 1, 1 - side]))

    def work(x):
        return functools.partial(relax if x < relaxing else heat, x % 2)

    ahead = g < n - 1
    eacc[...] = jnp.zeros_like(eacc)
    relaxing = 2 * OR_SWEEPS
    for r in range(count):
        inner(r, work(0))
    for load in loads[first + 3 :]:
        load.wait()
    if near:
        along(1, lambda: pl.semaphore_wait(temp_sem, m - 1 - t))
    along(1, lambda: tell(0).start())
    along(-1, lambda: tell(1).start())
    across().wait_recv()
    if shares_of > 1:
        for d in range(1, m):
            pass_on(d).start()

    def first_step(i, carry):
        r = jnp.where(g == 0, lax.rem(i, count), i // 2)
        side = jnp.where(g == 0, jnp.where(i < count, 1, 0), 1 - lax.rem(i, 2))
        pl.when(i == jnp.where(g == 0, count, 1))(lambda: passed_on(3))

        @pl.when(side == 1)
        def _():
            take_opening(r, 1)
            work(0)(r, last, lifting=True)
            halo(1, r, 1).start()

        @pl.when(side == 0)
        def _():
            take_opening(r, 0)
            work(0)(r, 0)
            halo(1, r, 0).start()

        return carry

    lax.fori_loop(0, 2 * count, first_step, 0)
    for x in range(HALVES - 1):
        for r in range(count):
            for side, z in ((0, 0), (1, last)) if x else ():
                take_halo(x, r, side)
                work(x)(r, z, lifting=side == 1)
                if side == 0 and len(parts(x + 1, r)) == 1:
                    pl.when(ahead)(lambda: halo(x + 1, r, 0).start())
            for part in range(len(parts(x + 1, r)) if x else 0):
                if len(parts(x + 1, r)) > 1:
                    pl.when(ahead)(lambda: halo(x + 1, r, 0, part).start())
                halo(x + 1, r, 1, part).start()
                pl.when(~ahead)(lambda: halo(x + 1, r, 0, part).start())
            if r == count - 1 and x == relaxing:
                for z in (0, last):
                    send_off(0, z)
            for z in range(planes):
                if z % relaxing == x:
                    pack_heat(r, z)
            inner(r, work(x + 1))
        if x >= relaxing - 1:
            send_inner(x + 1 - relaxing)

    x = HALVES - 1
    for r in range(count):
        if r == count - 1:
            arrived(True)
            along(1, lambda: tell(1).wait_recv())
            along(-1, lambda: tell(0).wait_recv())
        for part, rows_of in enumerate(parts(x, r)):
            for side, z in ((1, last), (0, 0)):
                halo(x, r, 1 - side, part).wait_recv()
                if part == 0 and side == 1:
                    sent(x - 1, r)
                work(x)(r, z, rows_of=rows_of)
                if r == count - 1:
                    send_off(1, z, part)
    for r in range(count):
        ebuf[1, g, r : r + 1] = jnp.sum(eacc[r], axis=0, keepdims=True)

    def share(dt, source, there):
        return pltpu.make_async_remote_copy(
            src_ref=ebuf.at[1, source],
            dst_ref=ebuf.at[1 - dt, source],
            send_sem=esend.at[1 - dt],
            recv_sem=erecv.at[1 - dt],
            device_id=peer(dt, there),
            device_id_type=MESH,
        )

    def spread(dt):
        for d in range(1 if dt == 0 else 0, n):
            share(dt, g, lax.rem(g + d, n)).start()

    def shares(dt, sem):
        ref = ebuf.at[1, pl.ds(0, n - 1 if dt == 0 else n)]
        pltpu.make_async_copy(ref, ref, sem).wait()

    for dt in (0, 1, -1):
        along(dt, lambda dt=dt: spread(dt))
    for r in range(count):
        sent(x, r)
    across().wait_send()
    passed_on(2)
    along(1, lambda: tell(0).wait_send())
    along(-1, lambda: tell(1).wait_send())
    both_ways(lambda side: whole(side, 2 * planes, xsend.at[side]))
    arrived(False)
    for dt in (0, 1, -1):
        along(dt, lambda dt=dt: shares(dt, esend.at[1 - dt]))
        along(dt, lambda dt=dt: shares(dt, erecv.at[1 + dt]))


def finish_kernel(
    dims,
    evened,
    rbuf,
    trecv,
    ebuf,
    out_hbm,
    eout_hbm,
    stage,
    eout_ref,
    out_sem,
    eout_sem,
):
    count, planes, rows, width, n, m = dims
    k = rows // 2
    g = lax.axis_index("gz")
    t = lax.axis_index("temp")
    below, above = (t > 0).astype(jnp.int32), (t < m - 1).astype(jnp.int32)

    def number(side, row):
        return trecv[side, row : row + 1]

    def own_order(r):
        return number(2, r)

    def own_bit(r):
        return number(2, count + r)

    def mask(value, size):
        return jnp.broadcast_to(value, (size, width)) > 0.5

    def plan(r):
        if r == 0:
            met = jnp.full((1, width), below, jnp.int32) != 0
            return rbuf.at[0], jnp.where(met, number(0, 1), 0.0), jnp.where(met, number(0, 0), 0.0)
        if r == count - 1:
            met = jnp.full((1, width), above, jnp.int32) != 0
            return rbuf.at[1], jnp.where(met, own_bit(r), 0.0), jnp.where(met, number(1, 0), 0.0)
        other = r + 1 if r % 2 else r - 1
        return evened.at[other], own_bit(min(r, other)), own_order(other)

    lane = lax.broadcasted_iota(jnp.int32, (k, width), 1)
    plans = [plan(r) for r in range(count)]
    orders = [
        jnp.where(take > 0.5, order, own_order(r)).astype(jnp.int32)
        for r, (_, take, order) in enumerate(plans)
    ]
    def unpack(z):
        for r in range(count):
            other, take, _ = plans[r]
            taking = mask(take, k)
            e = ((lane + (jnp.broadcast_to(orders[r], (k, width)) + (g * planes + z))) & 1) != 0
            for d in range(3):
                first, second = [
                    jnp.where(taking, other[i, d], evened[r, i, d]) for i in (z, planes + z)
                ]
                stage[r, d, z, pl.ds(0, k, stride=2), :] = jnp.where(e, second, first)
                stage[r, d, z, pl.ds(1, k, stride=2), :] = jnp.where(e, first, second)
            copy = pltpu.make_async_copy(
                stage.at[r, :, z], out_hbm.at[r, :, z], out_sem
            )
            copy.start()

    for z in range(planes // 2):
        unpack(z)
    sites = float(width * rows * planes * n)

    def total(slot, r):
        summed = ebuf[slot, 0, r : r + 1]
        for j in range(1, n):
            summed = summed + ebuf[slot, j, r : r + 1]
        return jnp.broadcast_to(jnp.sum(-summed, axis=1, keepdims=True) / sites, (1, width))

    energy = []
    for r in range(0, count, 2):
        taking = own_bit(r) > 0.5
        low, top = total(1, r), total(1, r + 1)
        energy += [jnp.where(taking, top, low), jnp.where(taking, low, top)]
    for r in range(count):
        other, take, _ = plans[r]
        if r == 0:
            swapped = number(0, 2) > 0.5
            partner = jnp.where(swapped, total(0, count - 2), total(0, count - 1))
        elif r == count - 1:
            swapped = number(1, 2) > 0.5
            partner = jnp.where(swapped, total(2, 1), total(2, 0))
        else:
            partner = energy[r + 1 if r % 2 else r - 1]
        eout_ref[r] = jnp.max(jnp.where(take > 0.5, partner, energy[r]))
    told = pltpu.make_async_copy(eout_ref, eout_hbm, eout_sem)
    told.start()
    for z in range(planes // 2, planes):
        unpack(z)
    told.wait()
    pltpu.make_async_copy(stage, out_hbm, out_sem).wait()


def on_device(n, m, spin, coup, beta, order, level, height, angle, bits):
    count, _, planes, rows, width = spin.shape
    k = rows // 2
    f32 = jnp.float32
    hbm = pl.BlockSpec(memory_space=pltpu.HBM)
    vmem = pl.BlockSpec(memory_space=pltpu.VMEM)
    dma = pltpu.SemaphoreType.DMA
    bonds = pltpu.VMEM((2, count, planes, k, width), f32)
    dims = (count, planes, rows, width, n, m)
    handed = pl.pallas_call(
        functools.partial(sweep_kernel, dims),
        out_shape=(
            pltpu.VMEM((count, 2 * planes, 3, k, width), f32),
            pltpu.VMEM((2, 2 * planes, 3, k, width), f32),
            pltpu.VMEM((3, max(8, 2 * count), width), f32),
            pltpu.VMEM((3, n, count, width), f32),
        ),
        in_specs=[hbm] * 8,
        out_specs=(vmem,) * 4,
        scratch_shapes=[
            pltpu.VMEM(spin.shape, f32),
            pltpu.VMEM(coup.shape, f32),
            pltpu.VMEM(level.shape, f32),
            pltpu.VMEM(level.shape, f32),
            pltpu.VMEM(level.shape, f32),
            pltpu.VMEM((2, count, 3, k, width), f32),
            pltpu.VMEM((count, 2, 2, k, width), f32),
            pltpu.VMEM((count, 2, 2, k, width), f32),
            pltpu.VMEM((rows, width), f32),
            pltpu.VMEM((2, count, 3, planes + 2, k + 2 * PAD, width), f32),
            bonds,
            bonds,
            pltpu.VMEM((count, planes, k, width), f32),
            bonds,
            bonds,
            bonds,
            bonds,
            pltpu.VMEM((2, count, 3, planes, k, width), f32),
            pltpu.VMEM((count, 8, width), f32),
            pltpu.VMEM((2, max(8, 2 * count), width), f32),
            pltpu.SMEM((count,), f32),
            pltpu.SMEM((count,), jnp.int32),
            pltpu.SMEM((count,), jnp.int32),
            dma((2 * count + 4,)),
            dma((2, count)),
            dma((4 * count + 4,)),
            dma((3,)),
            dma((3,)),
            dma((2,)),
            dma((2,)),
            dma((2,)),
            dma((2, 2)),
            dma((4,)),
            pltpu.SemaphoreType.REGULAR,
            pltpu.SemaphoreType.REGULAR,
        ],
        compiler_params=pltpu.CompilerParams(
            collective_id=0, has_side_effects=True, vmem_limit_bytes=58 * 1024 * 1024
        ),
    )(spin, coup, beta, order, level, height, angle, bits)
    return pl.pallas_call(
        functools.partial(finish_kernel, dims),
        out_shape=(
            jax.ShapeDtypeStruct(spin.shape, f32),
            jax.ShapeDtypeStruct((count,), f32),
        ),
        in_specs=[vmem] * 4,
        out_specs=(hbm, hbm),
        scratch_shapes=[
            pltpu.VMEM(spin.shape, f32),
            pltpu.SMEM((count,), f32),
            dma(()),
            dma(()),
        ],
        compiler_params=pltpu.CompilerParams(vmem_limit_bytes=16 * 1024 * 1024),
    )(*handed)


def solution(mesh):
    n, m = mesh.shape["gz"], mesh.shape["temp"]
    return jax.shard_map(
        functools.partial(on_device, n, m),
        mesh=mesh,
        in_specs=(
            P(("group", "temp"), None, "gz", None, None),
            P(None, ("group", "gz"), None, None),
            P(("group", "temp")),
            P(("group", "temp")),
            P(("group", "temp"), "gz", None, None),
            P(("group", "temp"), "gz", None, None),
            P(("group", "temp"), "gz", None, None),
            P(("group", "temp")),
        ),
        out_specs=(P(("group", "temp"), None, "gz", None, None), P(("group", "temp"))),
        check_vma=False,
    )
```

```python
import functools
import math

import jax
import jax.numpy as jnp
from jax import lax
from jax.experimental import pallas as pl
from jax.experimental.pallas import tpu as pltpu
from jax.sharding import PartitionSpec as P

OR_SWEEPS = 2
HALVES = 2 * OR_SWEEPS + 2
PAD = 8
MESH = pl.DeviceIdType.MESH
SIN_TERMS = [(-1.0) ** i / math.factorial(2 * i + 1) for i in range(8)]
COS_TERMS = [(-1.0) ** i / math.factorial(2 * i) for i in range(9)]


def horner(terms, value):
    total = jnp.full_like(value, terms[-1])
    for term in terms[-2::-1]:
        total = total * value + term
    return total


def cos_sin(angle):
    half = 0.5 * angle
    square = half * half
    sine = half * horner(SIN_TERMS, square)
    cosine = horner(COS_TERMS, square)
    return 1.0 - 2.0 * sine * sine, 2.0 * sine * cosine


def with_sign(size, like):
    return jnp.where(like < 0.0, -size, size)


def to_square(vector):
    a, b, c = vector
    inverse = 1.0 / (jnp.abs(a) + jnp.abs(b) + jnp.abs(c))
    p, q = a * inverse, b * inverse
    low = c < 0.0
    return (
        jnp.where(low, with_sign(1.0 - jnp.abs(q), p), p),
        jnp.where(low, with_sign(1.0 - jnp.abs(p), q), q),
    )


def from_square(p, q):
    c = 1.0 - jnp.abs(p) - jnp.abs(q)
    low = c < 0.0
    a = jnp.where(low, with_sign(1.0 - jnp.abs(q), p), p)
    b = jnp.where(low, with_sign(1.0 - jnp.abs(p), q), q)
    inverse = 1.0 / jnp.sqrt(a * a + b * b + c * c)
    return a * inverse, b * inverse, c * inverse


def dot3(a, b):
    return a[0] * b[0] + a[1] * b[1] + a[2] * b[2]


def reflect(current, pulled):
    factor = 2.0 * dot3(current, pulled) / jnp.maximum(dot3(pulled, pulled), 0.01)
    return [factor * p - s for p, s in zip(pulled, current)]


def heat_bath(pulled, beta, level, trial):
    strength = jnp.sqrt(jnp.maximum(dot3(pulled, pulled), 0.01))
    inverse = 1.0 / strength
    axis = [p * inverse for p in pulled]
    reach = beta * strength
    shrink = -jnp.tanh(reach) * (jnp.exp(-2.0 * reach) + 1.0)
    cosine = 1.0 + jnp.log1p(level * shrink) / reach
    along = dot3(trial, axis)
    tangent = [t - along * a for t, a in zip(trial, axis)]
    scale = jnp.sqrt(jnp.maximum(1.0 - cosine * cosine, 0.0)) * (
        1.0 / jnp.sqrt(jnp.maximum(dot3(tangent, tangent), 0.0001))
    )
    return [cosine * a + scale * t for a, t in zip(axis, tangent)]


def flag(bits_ref, j, size, width):
    return jnp.full((size, width), bits_ref[j], jnp.int32) != 0


def sweep_kernel(
    dims,
    spin_hbm,
    coup_hbm,
    beta_hbm,
    order_hbm,
    level_hbm,
    height_hbm,
    angle_hbm,
    bits_hbm,
    evened,
    rbuf,
    trecv,
    ebuf,
    spin_in,
    coup_in,
    level_in,
    height_in,
    angle_in,
    lifted,
    osend,
    orecv,
    cbelow,
    sp,
    xo,
    xr,
    yi,
    yo,
    zu,
    zd,
    lv,
    ut,
    eacc,
    tsend,
    beta_ref,
    order_ref,
    bits_ref,
    in_sem,
    hsend,
    hrecv,
    esend,
    erecv,
    tssem,
    trsem,
    xsend,
    xrecv,
    csem,
    wrap_sem,
    temp_sem,
):
    count, planes, rows, width, n, m = dims
    k = rows // 2
    chunk = 32 if k % 32 == 0 else 8
    last = planes - 1
    g = lax.axis_index("gz")
    t = lax.axis_index("temp")
    up, down = lax.rem(g + 1, n), lax.rem(g + n - 1, n)
    has_below, has_above = t > 0, t < m - 1
    near = 2 < n <= 2 * HALVES - 2

    first = 2 * count + 4
    loads = [
        pltpu.make_async_copy(src, dst, in_sem.at[i % first])
        for i, (src, dst) in enumerate(
            (
                (order_hbm, order_ref),
                (coup_hbm.at[2, last], coup_in.at[2, last]),
                *(
                    (spin_hbm.at[r, :, z], spin_in.at[r, :, z])
                    for r in range(count)
                    for z in (last, 0)
                ),
                (bits_hbm, bits_ref),
                (beta_hbm, beta_ref),
                (coup_hbm.at[pl.ds(0, 2)], coup_in.at[pl.ds(0, 2)]),
                (coup_hbm.at[2, pl.ds(0, last)], coup_in.at[2, pl.ds(0, last)]),
                (
                    spin_hbm.at[:, :, pl.ds(1, planes - 2)],
                    spin_in.at[:, :, pl.ds(1, planes - 2)],
                ),
                (level_hbm, level_in),
                (height_hbm, height_in),
                (angle_hbm, angle_in),
            )
        )
    ]

    def peer(dt, there):
        return {"gz": there} if dt == 0 else {"temp": t + dt, "gz": there}

    def along(dt, action):
        if dt == 0:
            action()
        else:
            pl.when(has_below if dt < 0 else has_above)(action)

    for load in loads[:4]:
        load.start()

    barrier = pltpu.get_barrier_semaphore()

    def greet(temp, there):
        target = {"temp": temp, "gz": there}
        pl.semaphore_signal(barrier, inc=1, device_id=target, device_id_type=MESH)

    if near:
        pl.when(g < n - 1)(lambda: greet(t, up))
        greet(t, down)
        for d in range(1, m):
            pl.when(t + d < m)(lambda: greet(t + d, g))
        expected = t + jnp.where(g == 0, 1, 2)
    else:
        for i in range(1, n * m):
            greet(lax.rem(t + i // n, m), lax.rem(g + i % n, n))
        expected = n * m - 1

    def parity(r, z, size):
        lane = lax.broadcasted_iota(jnp.int32, (size, width), 1)
        return ((lane + (g * planes + z + order_ref[r])) & 1) != 0

    def halves(ref, index, start, size):
        even = ref[index + (pl.ds(2 * start, size, stride=2), slice(None))]
        odd = ref[index + (pl.ds(2 * start + 1, size, stride=2), slice(None))]
        return even, odd

    def put_spin(c, r, d, z, start, value):
        size = value.shape[0]
        sp[c, r, d, z + 1, pl.ds(PAD + start, size), :] = value
        if start == 0:
            sp[c, r, d, z + 1, pl.ds(PAD + k, 1), :] = value[0:1]
        if start + size == k:
            sp[c, r, d, z + 1, pl.ds(PAD - 1, 1), :] = value[size - 1 : size]

    def pack_spin(r, z):
        e = parity(r, z, k)
        for d in range(3):
            even, odd = halves(spin_in, (r, d, z), 0, k)
            put_spin(0, r, d, z, 0, jnp.where(e, odd, even))
            put_spin(1, r, d, z, 0, jnp.where(e, even, odd))

    half = k // 2

    def parts(x, r):
        if x < HALVES - 1 or k % 32 or r < count - 1:
            return [(0, k)]
        return [(0, half), (half, k - 8), (k - 8, k)]

    def halo(x, r, side, part=0):
        c = 1 - x % 2
        start, stop = parts(x, r)[part]
        size = stop - start
        plain = sp.at[c, r, :, 1, pl.ds(PAD + start, size), :]
        above = planes + 1 if side == 0 else 0
        return pltpu.make_async_remote_copy(
            src_ref=plain if side == 0 else lifted.at[c, r, :, pl.ds(start, size), :],
            dst_ref=sp.at[c, r, :, above, pl.ds(PAD + start, size), :],
            send_sem=hsend.at[x % 2, r],
            recv_sem=hrecv.at[
                4 * count + 2 * part - 2 + side if part else 2 * (x % 2 * count + r) + side
            ],
            device_id={"gz": down if side == 0 else up},
            device_id_type=MESH,
        )

    def opening(r, side):
        return pltpu.make_async_remote_copy(
            src_ref=osend.at[r, side],
            dst_ref=orecv.at[r, side],
            send_sem=hsend.at[0, r],
            recv_sem=hrecv.at[2 * r + side],
            device_id={"gz": down if side == 0 else up},
            device_id_type=MESH,
        )

    shares_of = m if rows % (8 * m) == 0 else 1
    size_of = rows // shares_of
    stretch = pl.ds(pl.multiple_of(t * size_of, 8) if shares_of > 1 else 0, size_of)

    def across():
        return pltpu.make_async_remote_copy(
            src_ref=coup_in.at[2, last, stretch],
            dst_ref=cbelow.at[stretch],
            send_sem=csem.at[0],
            recv_sem=csem.at[1],
            device_id={"gz": up},
            device_id_type=MESH,
        )

    def pass_on(d):
        return pltpu.make_async_remote_copy(
            src_ref=cbelow.at[stretch],
            dst_ref=cbelow.at[stretch],
            send_sem=csem.at[2],
            recv_sem=csem.at[3],
            device_id={"temp": lax.rem(t + d, m)},
            device_id_type=MESH,
        )

    def passed_on(i):
        if shares_of > 1:
            ref = cbelow.at[pl.ds(0, (m - 1) * size_of)]
            pltpu.make_async_copy(ref, ref, csem.at[i]).wait()

    def sent(x, r):
        both = lifted.at[:, r] if x else osend.at[r]
        pltpu.make_async_copy(both, both, hsend.at[x % 2, r]).wait()

    def lift(c, r, d, start, value):
        part = pl.ds(start, value.shape[0])
        lifted[c, r, d, part, :] = zu[c, r, last, part, :] * value

    def inner(r, action):
        if planes > 2:
            lax.fori_loop(1, last, lambda z, carry: (action(r, z), carry)[1], 0)

    def ready():
        pl.semaphore_wait(barrier, expected)

    if near:

        @pl.when(g == n - 1)
        def _():
            ready()
            pl.semaphore_signal(wrap_sem, inc=1, device_id={"gz": up}, device_id_type=MESH)

    for load in loads[:4]:
        load.wait()
    if near:
        pl.when(g == n - 1)(lambda: across().start())
    for load in loads[4 : first + 4]:
        load.start()

    def pack_edges(r):
        e = parity(r, last, k)
        even, odd = halves(coup_in, (2, last), 0, k)
        zu[0, r, last] = jnp.where(e, odd, even)
        zu[1, r, last] = jnp.where(e, even, odd)
        for side, z in ((1, last), (0, 0)):
            pack_spin(r, z)
            edge = to_square([sp[1, r, d, z + 1, pl.ds(PAD, k), :] for d in range(3)])
            osend[r, side, 0], osend[r, side, 1] = edge

    def slot_order(r):
        other = order_ref[r ^ 1]
        return jnp.where(bits_ref[r - r % 2] != 0, other, order_ref[r])

    def wide(value):
        return jnp.full((1, width), value, jnp.int32).astype(jnp.float32)

    for r in range(count):
        if r > 0:
            for load in loads[2 * r + 2 : 2 * r + 4]:
                load.wait()
        pack_edges(r)
        if r == 0:
            if near:

                @pl.when(g < n - 1)
                def _():
                    ready()
                    across().start()

            else:
                ready()
                across().start()
        opening(r, 1).start()
        if near:
            pl.when(g > 0)(lambda: opening(r, 0).start())
        else:
            opening(r, 0).start()

    for load in loads[first - 2 : first]:
        load.wait()
    for load in loads[first + 4 :]:
        load.start()

    tsend[0, 0:1] = wide(slot_order(count - 1))
    tsend[0, 1:2] = wide(bits_ref[count - 1])
    tsend[0, 2:3] = wide(bits_ref[count - 2])
    tsend[1, 0:1] = wide(slot_order(0))
    tsend[1, 1:2] = wide(0)
    tsend[1, 2:3] = wide(bits_ref[0])
    for r in range(count):
        trecv[2, r : r + 1] = wide(slot_order(r))
        trecv[2, count + r : count + r + 1] = wide(bits_ref[r])

    def tell(side):
        return pltpu.make_async_remote_copy(
            src_ref=tsend.at[side],
            dst_ref=trecv.at[side],
            send_sem=tssem.at[side],
            recv_sem=trsem.at[side],
            device_id={"temp": t + 1 if side == 0 else t - 1},
            device_id_type=MESH,
        )

    if near:
        for d in range(1, m):

            @pl.when(t >= d)
            def _():
                target = {"temp": t - d, "gz": g}
                pl.semaphore_signal(temp_sem, inc=1, device_id=target, device_id_type=MESH)


    for load in loads[first : first + 3]:
        load.wait()

    def pack_bonds(i, carry):
        r, z = i // planes, i % planes
        e = parity(r, z, k)
        even, odd = halves(coup_in, (0, z), 0, k)
        first, second = jnp.where(e, odd, even), jnp.where(e, even, odd)
        xo[0, r, z] = first
        xo[1, r, z] = second
        xr[0, r, z] = pltpu.roll(second, 1, 1)
        xr[1, r, z] = pltpu.roll(first, 1, 1)
        even, odd = halves(coup_in, (1, z), 0, k)
        before = pltpu.roll(odd, 1, 0)
        yi[r, z] = even
        yo[0, r, z] = jnp.where(e, odd, before)
        yo[1, r, z] = jnp.where(e, before, odd)
        return carry

    def pack_lower(i, carry):
        r, z = i // last, 1 + i % last
        e = parity(r, z, k)
        even, odd = halves(coup_in, (2, z - 1), 0, k)
        zd[0, r, z] = jnp.where(e, odd, even)
        zd[1, r, z] = jnp.where(e, even, odd)
        zu[0, r, z - 1] = jnp.where(e, even, odd)
        zu[1, r, z - 1] = jnp.where(e, odd, even)
        return carry

    for r in range(count):
        inner(r, pack_spin)
    lax.fori_loop(0, count * planes, pack_bonds, 0)
    lax.fori_loop(0, count * last, pack_lower, 0)
    for r in range(count):
        for c in (0, 1):
            zd[c, r, 0] = jnp.ones((k, width), jnp.float32)

    if near:

        @pl.when(g == 0)
        def _():
            pl.semaphore_wait(wrap_sem, 1)
            for r in range(count):
                opening(r, 0).start()

    def pull(c, r, z, start, chunk=chunk):
        o = 1 - c
        part = pl.ds(start, chunk)
        e = parity(r, z, chunk)
        bx, br, by = xo[c, r, z, part, :], xr[c, r, z, part, :], yi[r, z, part, :]
        bo, bu, bd = yo[c, r, z, part, :], zu[c, r, z, part, :], zd[c, r, z, part, :]
        pulled = []
        for d in range(3):
            mid = sp[o, r, d, z + 1, pl.ds(PAD + start, chunk), :]
            nxt = sp[o, r, d, z + 1, pl.ds(PAD + start + 1, chunk), :]
            prv = sp[o, r, d, z + 1, pl.ds(PAD + start - 1, chunk), :]
            outer = jnp.where(e, nxt, prv) if c == 0 else jnp.where(e, prv, nxt)
            total = bx * pltpu.roll(mid, width - 1, 1) + br * pltpu.roll(mid, 1, 1)
            total = total + by * mid + bo * outer
            total = total + bu * sp[o, r, d, z + 2, pl.ds(PAD + start, chunk), :]
            total = total + bd * sp[o, r, d, z, pl.ds(PAD + start, chunk), :]
            pulled.append(total)
        return pulled

    def relax(c, r, z, lifting=False):
        for start in range(0, k, chunk):
            pulled = pull(c, r, z, start)
            current = [sp[c, r, d, z + 1, pl.ds(PAD + start, chunk), :] for d in range(3)]
            for d, value in enumerate(reflect(current, pulled)):
                put_spin(c, r, d, z, start, value)
                if lifting:
                    lift(c, r, d, start, value)

    def heat(c, r, z, lifting=False, rows_of=(0, k)):
        size = min(chunk, rows_of[1] - rows_of[0])
        for start in range(*rows_of, size):
            part = pl.ds(start, size)
            pulled = pull(c, r, z, start, size)
            trial = [ut[c, r, d, z, part, :] for d in range(3)]
            renewed = heat_bath(pulled, beta_ref[r], lv[c, r, z, part, :], trial)
            for d, value in enumerate(renewed):
                put_spin(c, r, d, z, start, value)
                if lifting:
                    lift(c, r, d, start, value)
            if c == 1:
                terms = dot3(renewed, pulled)
                eacc[r] = eacc[r] + sum(terms[j : j + 8] for j in range(0, size, 8))

    def pack_heat(r, z):
        for start in range(0, k, chunk):
            part = pl.ds(start, chunk)
            e = parity(r, z, chunk)
            even, odd = halves(level_in, (r, z), start, chunk)
            lv[0, r, z, part, :] = jnp.where(e, odd, even)
            lv[1, r, z, part, :] = jnp.where(e, even, odd)
            angles = halves(angle_in, (r, z), start, chunk)
            heights = halves(height_in, (r, z), start, chunk)
            trials = []
            for angle, height in zip(angles, heights):
                side = jnp.sqrt(jnp.maximum(1.0 - height * height, 0.0))
                cosine, sine = cos_sin(angle)
                trials.append((side * cosine, side * sine, height))
            for d in range(3):
                ut[0, r, d, z, part, :] = jnp.where(e, trials[1][d], trials[0][d])
                ut[1, r, d, z, part, :] = jnp.where(e, trials[0][d], trials[1][d])

    def take_halo(x, r, side):
        halo(x, r, 1 - side).wait_recv()
        if side == 0:
            sent(x - 1, r)

    def take_opening(r, side):
        opening(r, 1 - side).wait_recv()
        vector = from_square(orecv[r, 1 - side, 0], orecv[r, 1 - side, 1])
        if side == 0:
            even, odd = halves(cbelow, (), 0, k)
            bond = jnp.where(parity(r, 0, k), odd, even)
            vector = [bond * v for v in vector]
        for d in range(3):
            sp[1, r, d, planes + 1 if side else 0, pl.ds(PAD, k), :] = vector[d]

    def settle(c, z, start, stop):
        size = stop - start
        part, packed = pl.ds(start, size), pl.ds(PAD + start, size)
        for r in range(0, count, 2):
            taking = flag(bits_ref, r, size, width)
            for d in range(3):
                low = sp[c, r, d, z + 1, packed, :]
                top = sp[c, r + 1, d, z + 1, packed, :]
                evened[r, c * planes + z, d, part, :] = jnp.where(taking, top, low)
                evened[r + 1, c * planes + z, d, part, :] = jnp.where(taking, low, top)

    final = parts(HALVES - 1, count - 1)

    def pieces(c, z):
        return final if c == 1 and z in (0, last) else [(0, k)]

    def ship(c, z, side, part=0, many=1):
        start, stop = pieces(c, z)[part]
        rows_of = pl.ds(start, stop - start)
        here = pl.ds(c * planes + z, many)
        early = c == 0 and 0 < z < last
        return pltpu.make_async_remote_copy(
            src_ref=evened.at[count - 1 if side == 0 else 0, here, :, rows_of, :],
            dst_ref=rbuf.at[side, here, :, rows_of, :],
            send_sem=xsend.at[side],
            recv_sem=xrecv.at[0 if early else 1, side],
            device_id={"temp": t + 1 if side == 0 else t - 1},
            device_id_type=MESH,
        )

    def both_ways(action):
        along(1, lambda: action(0))
        along(-1, lambda: action(1))

    def send_off(c, z, part=0):
        settle(c, z, *pieces(c, z)[part])
        both_ways(lambda side: ship(c, z, side, part).start())

    def send_inner(c):
        for z in range(1, last):
            settle(c, z, 0, k)
        if planes > 2:
            both_ways(lambda side: ship(c, 1, side, many=planes - 2).start())

    def whole(side, size, sem):
        ref = rbuf.at[side, pl.ds(0, size)]
        pltpu.make_async_copy(ref, ref, sem).wait()

    def arrived(early):
        size = planes - 2 if early else planes + 2
        if size:
            both_ways(lambda side: whole(1 - side, size, xrecv.at[0 if early else 1, 1 - side]))

    def work(x):
        return functools.partial(relax if x < relaxing else heat, x % 2)

    ahead = g < n - 1
    eacc[...] = jnp.zeros_like(eacc)
    relaxing = 2 * OR_SWEEPS
    for r in range(count):
        inner(r, work(0))
    for load in loads[first + 3 :]:
        load.wait()
    if near:
        along(1, lambda: pl.semaphore_wait(temp_sem, m - 1 - t))
    along(1, lambda: tell(0).start())
    along(-1, lambda: tell(1).start())
    across().wait_recv()
    if shares_of > 1:
        for d in range(1, m):
            pass_on(d).start()

    def first_step(i, carry):
        r = jnp.where(g == 0, lax.rem(i, count), i // 2)
        side = jnp.where(g == 0, jnp.where(i < count, 1, 0), 1 - lax.rem(i, 2))
        pl.when(i == jnp.where(g == 0, count, 1))(lambda: passed_on(3))

        @pl.when(side == 1)
        def _():
            take_opening(r, 1)
            work(0)(r, last, lifting=True)
            halo(1, r, 1).start()

        @pl.when(side == 0)
        def _():
            take_opening(r, 0)
            work(0)(r, 0)
            halo(1, r, 0).start()

        return carry

    lax.fori_loop(0, 2 * count, first_step, 0)
    for x in range(HALVES - 1):
        for r in range(count):
            for side, z in ((0, 0), (1, last)) if x else ():
                take_halo(x, r, side)
                work(x)(r, z, lifting=side == 1)
                if side == 0 and len(parts(x + 1, r)) == 1:
                    pl.when(ahead)(lambda: halo(x + 1, r, 0).start())
            for part in range(len(parts(x + 1, r)) if x else 0):
                if len(parts(x + 1, r)) > 1:
                    pl.when(ahead)(lambda: halo(x + 1, r, 0, part).start())
                halo(x + 1, r, 1, part).start()
                pl.when(~ahead)(lambda: halo(x + 1, r, 0, part).start())
            if r == count - 1 and x == relaxing:
                for z in (0, last):
                    send_off(0, z)
            for z in range(planes):
                if z % relaxing == x:
                    pack_heat(r, z)
            inner(r, work(x + 1))
        if x >= relaxing - 1:
            send_inner(x + 1 - relaxing)

    x = HALVES - 1
    for r in range(count):
        if r == count - 1:
            arrived(True)
            along(1, lambda: tell(1).wait_recv())
            along(-1, lambda: tell(0).wait_recv())
        for part, rows_of in enumerate(parts(x, r)):
            for side, z in ((1, last), (0, 0)):
                halo(x, r, 1 - side, part).wait_recv()
                if part == 0 and side == 1:
                    sent(x - 1, r)
                work(x)(r, z, rows_of=rows_of)
                if r == count - 1:
                    send_off(1, z, part)
    for r in range(count):
        ebuf[n + g, r : r + 1] = jnp.sum(eacc[r], axis=0, keepdims=True)

    def share(dt, source, there):
        return pltpu.make_async_remote_copy(
            src_ref=ebuf.at[n + source],
            dst_ref=ebuf.at[(1 - dt) * n + source],
            send_sem=esend,
            recv_sem=erecv,
            device_id=peer(dt, there),
            device_id_type=MESH,
        )

    def spread(dt):
        for d in range(1 if dt == 0 else 0, n):
            share(dt, g, lax.rem(g + d, n)).start()

    temps = 1 + has_below.astype(jnp.int32) + has_above.astype(jnp.int32)

    def shares(sem):
        for groups in range(1, 4):
            size = groups * n - 1

            @pl.when(temps == groups)
            def _():
                if size:
                    ref = ebuf.at[pl.ds(0, size)]
                    pltpu.make_async_copy(ref, ref, sem).wait()

    for dt in (0, 1, -1):
        along(dt, lambda dt=dt: spread(dt))
    for r in range(count):
        sent(x, r)
    across().wait_send()
    passed_on(2)
    along(1, lambda: tell(0).wait_send())
    along(-1, lambda: tell(1).wait_send())
    both_ways(lambda side: whole(side, 2 * planes, xsend.at[side]))
    arrived(False)
    shares(esend)
    shares(erecv)


def finish_kernel(
    dims,
    evened,
    rbuf,
    trecv,
    ebuf,
    out_hbm,
    eout_hbm,
    stage,
    eout_ref,
    out_sem,
    eout_sem,
):
    count, planes, rows, width, n, m = dims
    k = rows // 2
    g = lax.axis_index("gz")
    t = lax.axis_index("temp")
    below, above = (t > 0).astype(jnp.int32), (t < m - 1).astype(jnp.int32)

    def number(side, row):
        return trecv[side, row : row + 1]

    def own_order(r):
        return number(2, r)

    def own_bit(r):
        return number(2, count + r)

    def mask(value, size):
        return jnp.broadcast_to(value, (size, width)) > 0.5

    def plan(r):
        if r == 0:
            met = jnp.full((1, width), below, jnp.int32) != 0
            return rbuf.at[0], jnp.where(met, number(0, 1), 0.0), jnp.where(met, number(0, 0), 0.0)
        if r == count - 1:
            met = jnp.full((1, width), above, jnp.int32) != 0
            return rbuf.at[1], jnp.where(met, own_bit(r), 0.0), jnp.where(met, number(1, 0), 0.0)
        other = r + 1 if r % 2 else r - 1
        return evened.at[other], own_bit(min(r, other)), own_order(other)

    lane = lax.broadcasted_iota(jnp.int32, (k, width), 1)
    plans = [plan(r) for r in range(count)]
    orders = [
        jnp.where(take > 0.5, order, own_order(r)).astype(jnp.int32)
        for r, (_, take, order) in enumerate(plans)
    ]
    def unpack(z):
        for r in range(count):
            other, take, _ = plans[r]
            taking = mask(take, k)
            e = ((lane + (jnp.broadcast_to(orders[r], (k, width)) + (g * planes + z))) & 1) != 0
            for d in range(3):
                first, second = [
                    jnp.where(taking, other[i, d], evened[r, i, d]) for i in (z, planes + z)
                ]
                stage[r, d, z, pl.ds(0, k, stride=2), :] = jnp.where(e, second, first)
                stage[r, d, z, pl.ds(1, k, stride=2), :] = jnp.where(e, first, second)
            copy = pltpu.make_async_copy(
                stage.at[r, :, z], out_hbm.at[r, :, z], out_sem
            )
            copy.start()

    for z in range(planes // 2):
        unpack(z)
    sites = float(width * rows * planes * n)

    def total(slot, r):
        summed = ebuf[slot * n, r : r + 1]
        for j in range(1, n):
            summed = summed + ebuf[slot * n + j, r : r + 1]
        return jnp.broadcast_to(jnp.sum(-summed, axis=1, keepdims=True) / sites, (1, width))

    energy = []
    for r in range(0, count, 2):
        taking = own_bit(r) > 0.5
        low, top = total(1, r), total(1, r + 1)
        energy += [jnp.where(taking, top, low), jnp.where(taking, low, top)]
    for r in range(count):
        other, take, _ = plans[r]
        if r == 0:
            swapped = number(0, 2) > 0.5
            partner = jnp.where(swapped, total(0, count - 2), total(0, count - 1))
        elif r == count - 1:
            swapped = number(1, 2) > 0.5
            partner = jnp.where(swapped, total(2, 1), total(2, 0))
        else:
            partner = energy[r + 1 if r % 2 else r - 1]
        eout_ref[r] = jnp.max(jnp.where(take > 0.5, partner, energy[r]))
    told = pltpu.make_async_copy(eout_ref, eout_hbm, eout_sem)
    told.start()
    for z in range(planes // 2, planes):
        unpack(z)
    told.wait()
    pltpu.make_async_copy(stage, out_hbm, out_sem).wait()


def on_device(n, m, spin, coup, beta, order, level, height, angle, bits):
    count, _, planes, rows, width = spin.shape
    k = rows // 2
    f32 = jnp.float32
    hbm = pl.BlockSpec(memory_space=pltpu.HBM)
    vmem = pl.BlockSpec(memory_space=pltpu.VMEM)
    dma = pltpu.SemaphoreType.DMA
    bonds = pltpu.VMEM((2, count, planes, k, width), f32)
    dims = (count, planes, rows, width, n, m)
    handed = pl.pallas_call(
        functools.partial(sweep_kernel, dims),
        out_shape=(
            pltpu.VMEM((count, 2 * planes, 3, k, width), f32),
            pltpu.VMEM((2, 2 * planes, 3, k, width), f32),
            pltpu.VMEM((3, max(8, 2 * count), width), f32),
            pltpu.VMEM((3 * n, count, width), f32),
        ),
        in_specs=[hbm] * 8,
        out_specs=(vmem,) * 4,
        scratch_shapes=[
            pltpu.VMEM(spin.shape, f32),
            pltpu.VMEM(coup.shape, f32),
            pltpu.VMEM(level.shape, f32),
            pltpu.VMEM(level.shape, f32),
            pltpu.VMEM(level.shape, f32),
            pltpu.VMEM((2, count, 3, k, width), f32),
            pltpu.VMEM((count, 2, 2, k, width), f32),
            pltpu.VMEM((count, 2, 2, k, width), f32),
            pltpu.VMEM((rows, width), f32),
            pltpu.VMEM((2, count, 3, planes + 2, k + 2 * PAD, width), f32),
            bonds,
            bonds,
            pltpu.VMEM((count, planes, k, width), f32),
            bonds,
            bonds,
            bonds,
            bonds,
            pltpu.VMEM((2, count, 3, planes, k, width), f32),
            pltpu.VMEM((count, 8, width), f32),
            pltpu.VMEM((2, max(8, 2 * count), width), f32),
            pltpu.SMEM((count,), f32),
            pltpu.SMEM((count,), jnp.int32),
            pltpu.SMEM((count,), jnp.int32),
            dma((2 * count + 4,)),
            dma((2, count)),
            dma((4 * count + 4,)),
            dma(()),
            dma(()),
            dma((2,)),
            dma((2,)),
            dma((2,)),
            dma((2, 2)),
            dma((4,)),
            pltpu.SemaphoreType.REGULAR,
            pltpu.SemaphoreType.REGULAR,
        ],
        compiler_params=pltpu.CompilerParams(
            collective_id=0, has_side_effects=True, vmem_limit_bytes=58 * 1024 * 1024
        ),
    )(spin, coup, beta, order, level, height, angle, bits)
    return pl.pallas_call(
        functools.partial(finish_kernel, dims),
        out_shape=(
            jax.ShapeDtypeStruct(spin.shape, f32),
            jax.ShapeDtypeStruct((count,), f32),
        ),
        in_specs=[vmem] * 4,
        out_specs=(hbm, hbm),
        scratch_shapes=[
            pltpu.VMEM(spin.shape, f32),
            pltpu.SMEM((count,), f32),
            dma(()),
            dma(()),
        ],
        compiler_params=pltpu.CompilerParams(vmem_limit_bytes=16 * 1024 * 1024),
    )(*handed)


def solution(mesh):
    n, m = mesh.shape["gz"], mesh.shape["temp"]
    return jax.shard_map(
        functools.partial(on_device, n, m),
        mesh=mesh,
        in_specs=(
            P(("group", "temp"), None, "gz", None, None),
            P(None, ("group", "gz"), None, None),
            P(("group", "temp")),
            P(("group", "temp")),
            P(("group", "temp"), "gz", None, None),
            P(("group", "temp"), "gz", None, None),
            P(("group", "temp"), "gz", None, None),
            P(("group", "temp")),
        ),
        out_specs=(P(("group", "temp"), None, "gz", None, None), P(("group", "temp"))),
        check_vma=False,
    )
```
